8 devices in a mesh: dp: 2 (over z, y), sp: 4 (over x, core).
Axes of the slice: x: 2, y: 2, z: 1, core: 2. Of those that a mesh axis runs over, the one named last changes fastest.
Arguments:
- x: bfloat16 [4, 4096], P('dp'), parts along dimension 0
- lens: int32 [4], P('dp'), parts along dimension 0
- wq: bfloat16 [2, 4096, 4096], replicated
- wk: bfloat16 [2, 4096, 4096], replicated
- wv: bfloat16 [2, 4096, 4096], replicated
- wo: bfloat16 [2, 4096, 4096], P(None, 'sp')
- w1: bfloat16 [2, 4096, 16384], P(None, None, 'sp')
- w2: bfloat16 [2, 16384, 4096], P(None, 'sp')
- g1: bfloat16 [2, 4096], replicated
- g2: bfloat16 [2, 4096], replicated
- kc: bfloat16 [2, 4, 2048, 32, 128], P(None, 'dp', 'sp'), parts along dimension 1
- vc: bfloat16 [2, 4, 2048, 32, 128], P(None, 'dp', 'sp'), parts along dimension 1
Outputs:
- output 1: bfloat16 [4, 4096], P('dp'), parts along dimension 0
- output 2: bfloat16 [2, 4, 2048, 32, 128], P(None, 'dp', 'sp'), parts along dimension 1
- output 3: bfloat16 [2, 4, 2048, 32, 128], P(None, 'dp', 'sp'), parts along dimension 1
There are 2 independent parts. The reference program is written for one: setup_inputs(seed, part) draws one part's arguments, and reference() takes and returns one part's arrays. A program takes and returns all parts, laid end to end along the dimension named above; an argument that names none is the same for every part.
All inputs are finite; a program needn't handle non-finite values.
Results may differ from the reference program's by a relative error of at most 0.00913119.
Values are sent between devices in bfloat16 or wider.
A program may use at most 1.75 GiB of HBM per device.

```python
import math
import jax
import jax.numpy as jnp
from jax import lax

B = 2
S_DEV = 512
SEQ = 4
D = 4096
HEADS = 32
KV_HEADS = 32
HEAD = 128
LAYERS = 2
S = S_DEV * SEQ
G = HEADS // KV_HEADS
FF = 4 * D
BLOCK = min(S_DEV, 1024)
EPS = 1e-6


def _rms(h, g):
    r = lax.rsqrt(jnp.mean(h * h, axis=-1, keepdims=True) + EPS)
    return (h * r * g.astype(jnp.float32)).astype(jnp.bfloat16)


def _mm(a, w):
    return jnp.dot(a, w, preferred_element_type=jnp.float32)


def _cache(key, t):
    k = jax.random.split(key, 7)
    ph = jax.random.uniform(k[0], (B, 3), jnp.float32)
    fr = jax.random.uniform(k[1], (B, 3), jnp.float32, 1.0, 3.0)
    wave = jnp.sin(2.0 * math.pi * (fr[:, None, :] * t[None, :, None] + ph[:, None, :]))
    kdir = jax.random.normal(k[2], (B, 1, KV_HEADS, HEAD), jnp.float32)
    u1 = jax.random.normal(k[3], (B, 1, KV_HEADS, HEAD), jnp.float32)
    u2 = jax.random.normal(k[4], (B, 1, KV_HEADS, HEAD), jnp.float32)
    kc = jax.random.normal(k[5], (B, S, KV_HEADS, HEAD), jnp.float32) + wave[:, :, 0, None, None] * kdir
    vc = (0.5 * jax.random.normal(k[6], (B, S, KV_HEADS, HEAD), jnp.float32)
          + wave[:, :, 1, None, None] * u1 + wave[:, :, 2, None, None] * u2)
    return kc.astype(jnp.bfloat16), vc.astype(jnp.bfloat16)


def _lengths(key):
    draws = jax.random.randint(key, (B,), 0, 256, dtype=jnp.int32)
    scaled = draws * (S - 1) // 255
    lens = scaled * draws // 255 + 1
    return lens.at[0].set(S).astype(jnp.int32)


def setup_inputs(seed: int = 0, part: int = 0) -> dict:
    key = jax.random.key(seed)
    ks = jax.random.split(key, 8)
    kp = jax.random.split(jax.random.fold_in(key, part), 3)
    gamma = (math.log(S) - 1.0) / math.sqrt(HEAD)
    wk = jax.random.normal(ks[0], (LAYERS, D, KV_HEADS, 1, HEAD), jnp.float32) * D ** -0.5
    wq = gamma * wk + jax.random.normal(ks[1], (LAYERS, D, KV_HEADS, G, HEAD), jnp.float32) * D ** -0.5
    wv = jax.random.normal(ks[2], (LAYERS, D, KV_HEADS * HEAD), jnp.float32) * D ** -0.5
    wo = jax.random.normal(ks[3], (LAYERS, HEADS * HEAD, D), jnp.float32) * (HEADS * HEAD) ** -0.5
    w1 = jax.random.normal(ks[4], (LAYERS, D, FF), jnp.float32) * D ** -0.5
    w2 = jax.random.normal(ks[5], (LAYERS, FF, D), jnp.float32) * FF ** -0.5
    g1 = 1.0 + 0.1 * jax.random.normal(ks[6], (LAYERS, D), jnp.float32)
    g2 = 1.0 + 0.1 * jax.random.normal(ks[7], (LAYERS, D), jnp.float32)
    t = jnp.arange(S, dtype=jnp.float32) / S
    ck = jax.random.split(kp[2], LAYERS)
    caches = [_cache(ck[i], t) for i in range(LAYERS)]
    bf = jnp.bfloat16
    return {
        'x': jax.random.normal(kp[0], (B, D), jnp.float32).astype(bf),
        'lens': _lengths(kp[1]),
        'wq': wq.reshape(LAYERS, D, HEADS * HEAD).astype(bf),
        'wk': wk.reshape(LAYERS, D, KV_HEADS * HEAD).astype(bf),
        'wv': wv.astype(bf),
        'wo': wo.astype(bf),
        'w1': w1.astype(bf),
        'w2': w2.astype(bf),
        'g1': g1.astype(bf),
        'g2': g2.astype(bf),
        'kc': jnp.stack([c[0] for c in caches]),
        'vc': jnp.stack([c[1] for c in caches]),
    }


def _attend(q, kc, vc, lens):
    qf = q.astype(jnp.float32)

    def body(carry, i):
        m, l, o = carry
        k = lax.dynamic_slice_in_dim(kc, i * BLOCK, BLOCK, axis=1).astype(jnp.float32)
        v = lax.dynamic_slice_in_dim(vc, i * BLOCK, BLOCK, axis=1).astype(jnp.float32)
        s = jnp.einsum('bkgd,bskd->bkgs', qf, k) * HEAD ** -0.5
        posn = i * BLOCK + jnp.arange(BLOCK)
        s = jnp.where((posn[None, :] < lens[:, None])[:, None, None, :], s, -jnp.inf)
        mn = jnp.maximum(m, jnp.max(s, axis=-1))
        c = jnp.exp(m - mn)
        p = jnp.exp(s - mn[..., None])
        o = o * c[..., None] + jnp.einsum('bkgs,bskd->bkgd', p, v)
        return (mn, l * c + jnp.sum(p, axis=-1), o), None

    init = (jnp.full((B, KV_HEADS, G), -jnp.inf, jnp.float32),
            jnp.zeros((B, KV_HEADS, G), jnp.float32),
            jnp.zeros((B, KV_HEADS, G, HEAD), jnp.float32))
    (m, l, o), _ = lax.scan(body, init, jnp.arange(S // BLOCK))
    return o / l[..., None]


def reference(x, lens, wq, wk, wv, wo, w1, w2, g1, g2, kc, vc):
    posn = jnp.arange(S)
    write = (posn[None, :] == (lens - 1)[:, None])[:, :, None, None]

    def layer(h, w):
        wq_, wk_, wv_, wo_, w1_, w2_, g1_, g2_, kc_, vc_ = w
        xn = _rms(h, g1_)
        q = _mm(xn, wq_).astype(jnp.bfloat16).reshape(B, KV_HEADS, G, HEAD)
        k = _mm(xn, wk_).astype(jnp.bfloat16).reshape(B, 1, KV_HEADS, HEAD)
        v = _mm(xn, wv_).astype(jnp.bfloat16).reshape(B, 1, KV_HEADS, HEAD)
        kn = jnp.where(write, k, kc_)
        vn = jnp.where(write, v, vc_)
        o = _attend(q, kn, vn, lens).astype(jnp.bfloat16).reshape(B, HEADS * HEAD)
        h = h + _mm(o, wo_)
        u = jax.nn.gelu(_mm(_rms(h, g2_), w1_)).astype(jnp.bfloat16)
        h = h + _mm(u, w2_)
        return h, (kn, vn)

    h, (kn, vn) = lax.scan(layer, x.astype(jnp.float32), (wq, wk, wv, wo, w1, w2, g1, g2, kc, vc))
    return h.astype(jnp.bfloat16), kn, vn
```

```python
import functools

import jax
import jax.numpy as jnp
from jax import lax
from jax.experimental import pallas as pl
from jax.experimental.pallas import tpu as pltpu
from jax.sharding import PartitionSpec as P

EPS = 1e-6
MESH = pl.DeviceIdType.MESH
VM = pl.BlockSpec(memory_space=pltpu.VMEM)
ANY = pl.BlockSpec(memory_space=pl.ANY)
SM = pl.BlockSpec(memory_space=pltpu.SMEM)
F32, BF16 = jnp.float32, jnp.bfloat16
CH = 128
NB = 512


def _rms(h, g):
    r = lax.rsqrt(jnp.mean(h * h, axis=-1, keepdims=True) + EPS)
    return (h * r * g.astype(F32)).astype(BF16)


def _gelu(z):
    return 0.5 * z * (1.0 + jnp.tanh(0.7978845608028654 * (z + 0.044715 * z * z * z)))


def _dot(a, w):
    return jnp.dot(a, w, preferred_element_type=F32)


def _ids():
    dp, sp = lax.axis_index('dp'), lax.axis_index('sp')
    return dp, sp, lax.rem(sp, 2), dp * 4 + sp


def _barrier(me):
    sem = pltpu.get_barrier_semaphore()
    for k in range(1, 8):
        d = lax.rem(me + k, 8)
        pl.semaphore_signal(sem, inc=1, device_id=(d // 4, lax.rem(d, 4)), device_id_type=MESH)
    pl.semaphore_wait(sem, 7)


def _exchange(me, src, dst, ssem, rsem):
    out = []
    for k in range(1, 8):
        d = lax.rem(me + k, 8)
        c = pltpu.make_async_remote_copy(src(d), dst, ssem.at[k], rsem.at[k],
                                         device_id=(d // 4, lax.rem(d, 4)), device_id_type=MESH)
        c.start()
        out.append(c)
    return out


def _qkv_copies(l, me, ws, wbuf, wsem, slot, s0):
    out = []
    for i in range(3):
        for kh in range(2):
            n = 2 * i + kh
            out.append(pltpu.make_async_copy(
                ws[i].at[l, pl.ds(kh * 2048, 2048), pl.ds(pl.multiple_of(me * NB, NB), NB)],
                wbuf.at[slot + n], wsem.at[s0 + n]))
    return out


def _half_cols(t, q, c):
    half = (1 - c) if t < 2 else c
    return half * 2048 + q * 1024 + (t % 2) * NB


def _mlp_copies(l, dp, c, wo, w1, w2, wbuf, wsem):
    out = []
    for t in range(4):
        for q in range(2):
            n = 2 * t + q
            col = pl.multiple_of(_half_cols(t, q, c), NB)
            out.append(pltpu.make_async_copy(
                wo.at[l, pl.ds(pl.multiple_of(dp * 512, 512), 512), pl.ds(col, NB)],
                wbuf.at[n // 4, pl.ds((n % 4) * 512, 512)], wsem.at[n]))
    for j in range(4):
        for kh in range(2):
            n = 2 * j + kh
            out.append(pltpu.make_async_copy(
                w1.at[l, pl.ds(kh * 2048, 2048), pl.ds(pl.multiple_of(dp * 2048 + j * NB, NB), NB)],
                wbuf.at[2 + n], wsem.at[8 + n]))
    for t in range(4):
        for q in range(2):
            n = 2 * t + q
            col = pl.multiple_of(_half_cols(t, q, c), NB)
            out.append(pltpu.make_async_copy(
                w2.at[l, pl.ds(pl.multiple_of(dp * 2048, 2048), 2048), pl.ds(col, NB)],
                wbuf.at[10 + n], wsem.at[16 + n]))
    return out


def _allreduce(block, dp, sp, c, me, buf, sems, h_ref):
    psend, pown, precv, chips, tot = buf
    s1, r1, s2, r2, s3, r3 = sems
    partner = (dp, sp + 1 - 2 * c)
    for t in range(2):
        v = jnp.concatenate([block(t, 0)[0:4], block(t, 1)[0:4]], axis=0)
        psend[:, t * NB:(t + 1) * NB] = v
    one = pltpu.make_async_remote_copy(psend, precv, s1, r1, device_id=partner, device_id_type=MESH)
    one.start()
    for t in range(2):
        v = jnp.concatenate([block(t + 2, 0)[0:4], block(t + 2, 1)[0:4]], axis=0)
        pown[:, t * NB:(t + 1) * NB] = v
    one.wait()
    chip = dp * 2 + sp // 2
    chips[chip] = pown[...] + precv[...]
    two = []
    for k in range(1, 4):
        d = lax.rem(chip + k, 4)
        cp = pltpu.make_async_remote_copy(chips.at[chip], chips.at[chip], s2.at[k], r2.at[k],
                                          device_id=(d // 2, lax.rem(d, 2) * 2 + c), device_id_type=MESH)
        cp.start()
        two.append(cp)
    for cp in two:
        cp.wait()
    tot[c] = ((chips[0] + chips[1]) + chips[2]) + chips[3]
    three = pltpu.make_async_remote_copy(tot.at[c], tot.at[c], s3, r3, device_id=partner, device_id_type=MESH)
    three.start()
    three.wait()
    for half in range(2):
        for q in range(2):
            lo = half * 2048 + q * 1024
            h_ref[0:4, lo:lo + 1024] += tot[half, q * 4:q * 4 + 4, :]


def _qkv_stage(me, xn, wbuf, copies, slot, sendA, recvA, ssem, rsem, qkv_ref):
    res = []
    for i in range(3):
        copies[2 * i].wait()
        z = _dot(xn[:, :2048], wbuf[slot + 2 * i])
        copies[2 * i + 1].wait()
        z = z + _dot(xn[:, 2048:], wbuf[slot + 2 * i + 1])
        res.append(z)
    for g in range(2):
        rows = [r[2 * g:2 * g + 2] for r in res] + [jnp.zeros((2, NB), F32)]
        sendA[g] = jnp.concatenate(rows, axis=0).astype(BF16)
    cps = _exchange(me, lambda d: sendA.at[d // 4], recvA.at[me], ssem, rsem)
    recvA[me] = sendA[me // 4]
    for cp in cps:
        cp.wait()
    qkv_ref[...] = recvA[...]


def _first(x_ref, wq, wk, wv, g1, h_ref, qkv_ref, wbuf, xo, sendA, recvA, wsem, xs, xr, sa, ra):
    dp, sp, c, me = _ids()
    cq = _qkv_copies(0, me, (wq, wk, wv), wbuf, wsem, 0, 0)
    for cp in cq:
        cp.start()
    _barrier(me)
    ex = pltpu.make_async_remote_copy(x_ref, xo, xs, xr, device_id=(1 - dp, sp), device_id_type=MESH)
    ex.start()
    ex.wait()
    mine, other = x_ref[...].astype(F32), xo[...].astype(F32)
    h_ref[0:2, :] = jnp.where(dp == 0, mine, other)
    h_ref[2:4, :] = jnp.where(dp == 0, other, mine)
    h_ref[4:8, :] = jnp.zeros((4, h_ref.shape[1]), F32)
    xn = _rms(h_ref[...], g1[0:1, :])
    _qkv_stage(me, xn, wbuf, cq, 0, sendA, recvA, sa, ra, qkv_ref)


def _layer(l, last, *refs):
    if last:
        (op_ref, hin, wo, w1, w2, g2, y_ref, h_ref, *sc) = refs
    else:
        (op_ref, hin, wo, w1, w2, g2, wq, wk, wv, g1, h_ref, qkv_ref, *sc) = refs
    wbuf, recvB, att, u, psend, pown, precv, chips, tot = sc[:9]
    wsem, sb, rb, s1, r1, s2, r2, s3, r3 = sc[9:18]
    dp, sp, c, me = _ids()
    cm = _mlp_copies(l, dp, c, wo, w1, w2, wbuf, wsem)
    cq = []
    if not last:
        sendA, recvA, sa, ra = sc[18:]
        cq = _qkv_copies(l + 1, me, (wq, wk, wv), wbuf, wsem, 18, 24)
    for cp in cm + cq:
        cp.start()
    _barrier(me)
    cps = _exchange(me, lambda d: op_ref.at[2 * lax.rem(d, 4) + d // 4], recvB.at[me], sb, rb)
    recvB[me] = op_ref[2 * sp + dp]
    h_ref[...] = hin[...]
    att[...] = jnp.zeros_like(att)
    for cp in cps:
        cp.wait()
    for g in range(2):
        ms = [recvB[4 * g + i, 1][:, 0:1] for i in range(4)]
        m = functools.reduce(jnp.maximum, ms)
        o = jnp.zeros((8, 128), F32)
        den = jnp.zeros((8, 1), F32)
        for i in range(4):
            e = jnp.exp(ms[i] - m)
            o = o + recvB[4 * g + i, 0] * e
            den = den + recvB[4 * g + i, 1][:, 64:65] * e
        a = o / den
        for b in range(2):
            for j in range(4):
                att[2 * g + b:2 * g + b + 1, j * 128:(j + 1) * 128] = a[4 * b + j:4 * b + j + 1]
    av = att[...].astype(BF16)

    def wo_block(t, q):
        n = 2 * t + q
        cm[n].wait()
        return _dot(av, wbuf[n // 4, (n % 4) * 512:(n % 4) * 512 + 512, :])

    def bufs(i):
        return [psend.at[i], pown.at[i], precv.at[i], chips.at[i], tot.at[i]]

    def sems(i):
        return [s1.at[i], r1.at[i], s2.at[i], r2.at[i], s3.at[i], r3.at[i]]

    _allreduce(wo_block, dp, sp, c, me, bufs(0), sems(0), h_ref)
    xn = _rms(h_ref[...], g2[l:l + 1, :])
    for j in range(4):
        cm[8 + 2 * j].wait()
        z = _dot(xn[:, :2048], wbuf[2 + 2 * j])
        cm[9 + 2 * j].wait()
        z = z + _dot(xn[:, 2048:], wbuf[3 + 2 * j])
        u[:, j * NB:(j + 1) * NB] = _gelu(z).astype(BF16)
    uv = u[...]

    def w2_block(t, q):
        n = 2 * t + q
        cm[16 + n].wait()
        return _dot(uv, wbuf[10 + n])

    _allreduce(w2_block, dp, sp, c, me, bufs(1), sems(1), h_ref)
    if last:
        hv = h_ref[...]
        y_ref[...] = jnp.where(dp == 0, hv[0:2], hv[2:4]).astype(BF16)
    else:
        xn = _rms(h_ref[...], g1[l + 1:l + 2, :])
        _qkv_stage(me, xn, wbuf, cq, 18, sendA, recvA, sa, ra, qkv_ref)


def _attn(l, *refs):
    if l == 0:
        lens, qkv, kc, vc, ko, vo, op_ref, *sc = refs
    else:
        lens, qkv, kc, vc, _, _, ko, vo, op_ref, *sc = refs
    kb, vb, tr, s_ref, m_ref, l_ref, o_ref, ki, vi, kos, vos = sc
    nb, npos, nh, dh = kb.shape
    per = npos // CH
    n = nb * per
    base = lax.axis_index('sp') * npos

    def rd(src, buf, sem, i):
        b, p = i // per, pl.multiple_of(lax.rem(i, per) * CH, CH)
        return pltpu.make_async_copy(src.at[l, b, pl.ds(p, CH)], buf.at[b, pl.ds(p, CH)], sem.at[i])

    def wr(dst, buf, sem, i):
        b, p = i // per, pl.multiple_of(lax.rem(i, per) * CH, CH)
        return pltpu.make_async_copy(buf.at[b, pl.ds(p, CH)], dst.at[l, b, pl.ds(p, CH)], sem.at[i])

    for i in range(n):
        rd(kc, kb, ki, i).start()
    for i in range(n):
        rd(vc, vb, vi, i).start()
    for src in range(8):
        v = qkv[src].astype(F32)
        for j in range(4):
            tr[src * 4 + j] = v[:, j * dh:(j + 1) * dh]
    m_ref[...] = jnp.full(m_ref.shape, -jnp.inf, F32)
    l_ref[...] = jnp.zeros_like(l_ref)
    o_ref[...] = jnp.zeros_like(o_ref)

    def patch(buf, row, b, p0):
        lp = lens[b] - 1 - base

        @pl.when((lp >= p0) & (lp < p0 + CH))
        def _():
            buf[b, lp] = tr[:, row + b, :].astype(BF16)

    row = lax.broadcasted_iota(jnp.int32, (nh, CH * nh), 0)
    col = lax.broadcasted_iota(jnp.int32, (nh, CH * nh), 1)
    same = lax.rem(col, nh) == row

    def kstep(i, _):
        b = i // per
        p0 = pl.multiple_of(lax.rem(i, per) * CH, CH)
        rd(kc, kb, ki, i).wait()
        patch(kb, 2, b, p0)
        q = tr[:, b, :].astype(BF16)
        kk = kb[b, pl.ds(p0, CH)].reshape(CH * nh, dh)
        s = lax.dot_general(q, kk, (((1,), (1,)), ((), ())), preferred_element_type=F32) * dh ** -0.5
        lim = (lens[b] - base - p0) * nh
        s = jnp.where(same & (col < lim), s, -jnp.inf)
        s_ref[i] = s
        m_ref[b] = jnp.maximum(m_ref[b], jnp.max(s, axis=1, keepdims=True))
        wr(ko, kb, kos, i).start()
        return 0

    def vstep(i, _):
        b = i // per
        p0 = pl.multiple_of(lax.rem(i, per) * CH, CH)
        rd(vc, vb, vi, i).wait()
        patch(vb, 4, b, p0)
        m = m_ref[b][:, 0:1]
        m = jnp.where(m == -jnp.inf, 0.0, m)
        p = jnp.exp(s_ref[i] - m)
        l_ref[b] += jnp.sum(p, axis=1, keepdims=True)
        vv = vb[b, pl.ds(p0, CH)].reshape(CH * nh, dh)
        o_ref[b] += _dot(p.astype(BF16), vv)
        wr(vo, vb, vos, i).start()
        return 0

    lax.fori_loop(0, n, kstep, 0)
    lax.fori_loop(0, n, vstep, 0)
    lane = lax.broadcasted_iota(jnp.int32, (nh, dh), 1)
    for b in range(nb):
        ov = o_ref[b]
        ml = jnp.where(lane < 64, m_ref[b], l_ref[b])
        for r in range(8):
            op_ref[r, 0, b * 4:b * 4 + 4, :] = ov[4 * r:4 * r + 4]
            op_ref[r, 1, b * 4:b * 4 + 4, :] = ml[4 * r:4 * r + 4]
    for i in range(n):
        wr(ko, kb, kos, i).wait()
    for i in range(n):
        wr(vo, vb, vos, i).wait()


def solution(mesh):
    kspec = P(None, 'dp', 'sp', None, None)
    DMA = pltpu.SemaphoreType.DMA

    def local(x, lens, wq, wk, wv, wo, w1, w2, g1, g2, kc, vc):
        nl, nb, npos, nh, dh = kc.shape
        d = x.shape[1]
        h_sh = jax.ShapeDtypeStruct((8, d), F32)
        qkv_sh = jax.ShapeDtypeStruct((8, 8, NB), BF16)
        qkv_sc = [pltpu.VMEM((2, 8, NB), BF16), pltpu.VMEM((8, 8, NB), BF16)]
        cparams = lambda i, mib: pltpu.CompilerParams(
            collective_id=i, has_side_effects=True, vmem_limit_bytes=mib * 2 ** 20)

        h, qkv = pl.pallas_call(
            _first, out_shape=(h_sh, qkv_sh),
            in_specs=[VM, ANY, ANY, ANY, VM], out_specs=(VM, VM),
            scratch_shapes=[pltpu.VMEM((6, 2048, NB), BF16), pltpu.VMEM((2, d), BF16), *qkv_sc,
                            DMA((6,)), DMA, DMA, DMA((8,)), DMA((8,))],
            compiler_params=cparams(0, 40), name='first')(x, wq, wk, wv, g1)

        def attn(l, qkv, ko, vo):
            n = nb * npos // CH
            c_sh = jax.ShapeDtypeStruct(kc.shape, kc.dtype)
            args = [lens, qkv, kc, vc] + ([] if l == 0 else [ko, vo])
            return pl.pallas_call(
                functools.partial(_attn, l),
                out_shape=(c_sh, c_sh, jax.ShapeDtypeStruct((8, 2, 8, dh), F32)),
                in_specs=[SM, VM, ANY, ANY] + ([] if l == 0 else [ANY, ANY]),
                out_specs=(ANY, ANY, VM),
                scratch_shapes=[pltpu.VMEM((nb, npos, nh, dh), BF16), pltpu.VMEM((nb, npos, nh, dh), BF16),
                                pltpu.VMEM((nh, 8, dh), F32), pltpu.VMEM((n, nh, CH * nh), F32),
                                pltpu.VMEM((nb, nh, dh), F32), pltpu.VMEM((nb, nh, dh), F32),
                                pltpu.VMEM((nb, nh, dh), F32), DMA((n,)), DMA((n,)), DMA((n,)), DMA((n,))],
                input_output_aliases={} if l == 0 else {4: 0, 5: 1},
                compiler_params=pltpu.CompilerParams(vmem_limit_bytes=48 * 2 ** 20), name='attn')(*args)

        def layer(l, op, h, last):
            nw = 18 if last else 24
            sc = [pltpu.VMEM((nw, 2048, NB), BF16), pltpu.VMEM((8, 2, 8, dh), F32),
                  pltpu.VMEM((8, 512), F32), pltpu.VMEM((8, 2048), BF16),
                  pltpu.VMEM((2, 8, 1024), F32), pltpu.VMEM((2, 8, 1024), F32), pltpu.VMEM((2, 8, 1024), F32),
                  pltpu.VMEM((2, 4, 8, 1024), F32), pltpu.VMEM((2, 2, 8, 1024), F32),
                  DMA((30,)), DMA((8,)), DMA((8,)),
                  DMA((2,)), DMA((2,)), DMA((2, 4)), DMA((2, 4)), DMA((2,)), DMA((2,))]
            args = [op, h, wo, w1, w2, g2]
            specs = [VM, VM, ANY, ANY, ANY, VM]
            if last:
                sc = [pltpu.VMEM((8, d), F32)] + sc
                outs, out_specs = jax.ShapeDtypeStruct((nb, d), BF16), VM
            else:
                args += [wq, wk, wv, g1]
                specs += [ANY, ANY, ANY, VM]
                sc += qkv_sc + [DMA((8,)), DMA((8,))]
                outs, out_specs = (h_sh, qkv_sh), (VM, VM)
            return pl.pallas_call(
                functools.partial(_layer, l, last), out_shape=outs, in_specs=specs, out_specs=out_specs,
                scratch_shapes=sc, compiler_params=cparams(1 + l, 60), name='layer')(*args)

        ko = vo = None
        for l in range(nl):
            ko, vo, op = attn(l, qkv, ko, vo)
            if l < nl - 1:
                h, qkv = layer(l, op, h, False)
            else:
                y = layer(l, op, h, True)
        return y, ko, vo

    return jax.shard_map(
        local, mesh=mesh,
        in_specs=(P('dp', None), P('dp'), P(), P(), P(), P(None, 'sp', None), P(None, None, 'sp'),
                  P(None, 'sp', None), P(), P(), kspec, kspec),
        out_specs=(P('dp', None), kspec, kspec), check_vma=False)
```

```python
import functools

import jax
import jax.numpy as jnp
from jax import lax
from jax.experimental import pallas as pl
from jax.experimental.pallas import tpu as pltpu
from jax.sharding import PartitionSpec as P

EPS = 1e-6
MESH = pl.DeviceIdType.MESH
VM = pl.BlockSpec(memory_space=pltpu.VMEM)
ANY = pl.BlockSpec(memory_space=pltpu.HBM)
SM = pl.BlockSpec(memory_space=pltpu.SMEM)
F32, BF16 = jnp.float32, jnp.bfloat16
CH = 128
NB = 512
LM = 39


def _rms(h, g):
    r = lax.rsqrt(jnp.mean(h * h, axis=-1, keepdims=True) + EPS)
    return (h * r * g.astype(F32)).astype(BF16)


def _gelu(z):
    return 0.5 * z * (1.0 + jnp.tanh(0.7978845608028654 * (z + 0.044715 * z * z * z)))


def _dot(a, w):
    return jnp.dot(a, w, preferred_element_type=F32)


def _ids():
    dp, sp = lax.axis_index('dp'), lax.axis_index('sp')
    return dp, sp, lax.rem(sp, 2), dp * 4 + sp


def _barrier(me):
    sem = pltpu.get_barrier_semaphore()
    for k in range(1, 8):
        d = lax.rem(me + k, 8)
        pl.semaphore_signal(sem, inc=1, device_id=(d // 4, lax.rem(d, 4)), device_id_type=MESH)
    pl.semaphore_wait(sem, 7)


def _exchange(me, src, dst, ssem, rsem):
    out = []
    for k in range(1, 8):
        d = lax.rem(me + k, 8)
        c = pltpu.make_async_remote_copy(src(d), dst, ssem.at[k], rsem.at[k],
                                         device_id=(d // 4, lax.rem(d, 4)), device_id_type=MESH)
        c.start()
        out.append(c)
    return out


def _qkv_copies(l, me, ws, wbuf, wsem, slot, s0):
    out = []
    for i in range(3):
        for kh in range(2):
            n = 2 * i + kh
            out.append(pltpu.make_async_copy(
                ws[i].at[l, pl.ds(kh * 2048, 2048), pl.ds(pl.multiple_of(me * NB, NB), NB)],
                wbuf.at[slot + n], wsem.at[s0 + n]))
    return out


def _half_cols(t, q, c):
    half = (1 - c) if t < 2 else c
    return half * 2048 + q * 1024 + (t % 2) * NB


def _mlp_copies(l, dp, c, wo, w1, w2, wbuf, wsem):
    out = []
    for t in range(4):
        for q in range(2):
            n = 2 * t + q
            col = pl.multiple_of(_half_cols(t, q, c), NB)
            out.append(pltpu.make_async_copy(
                wo.at[l, pl.ds(pl.multiple_of(dp * 512, 512), 512), pl.ds(col, NB)],
                wbuf.at[n // 4, pl.ds((n % 4) * 512, 512)], wsem.at[n]))
    for j in range(4):
        for kh in range(2):
            n = 2 * j + kh
            out.append(pltpu.make_async_copy(
                w1.at[l, pl.ds(kh * 2048, 2048), pl.ds(pl.multiple_of(dp * 2048 + j * NB, NB), NB)],
                wbuf.at[2 + n], wsem.at[8 + n]))
    for t in range(4):
        for q in range(2):
            n = 2 * t + q
            col = pl.multiple_of(_half_cols(t, q, c), NB)
            out.append(pltpu.make_async_copy(
                w2.at[l, pl.ds(pl.multiple_of(dp * 2048, 2048), 2048), pl.ds(col, NB)],
                wbuf.at[10 + n], wsem.at[16 + n]))
    return out


def _allreduce(block, dp, sp, c, me, buf, sems, h_ref):
    psend, pown, precv, chips, tot = buf
    s1, r1, s2, r2, s3, r3 = sems
    partner = (dp, sp + 1 - 2 * c)
    for t in range(2):
        v = jnp.concatenate([block(t, 0)[0:4], block(t, 1)[0:4]], axis=0)
        psend[:, t * NB:(t + 1) * NB] = v
    one = pltpu.make_async_remote_copy(psend, precv, s1, r1, device_id=partner, device_id_type=MESH)
    one.start()
    for t in range(2):
        v = jnp.concatenate([block(t + 2, 0)[0:4], block(t + 2, 1)[0:4]], axis=0)
        pown[:, t * NB:(t + 1) * NB] = v
    one.wait()
    chip = dp * 2 + sp // 2
    chips[chip] = pown[...] + precv[...]
    two = []
    for k in range(1, 4):
        d = lax.rem(chip + k, 4)
        cp = pltpu.make_async_remote_copy(chips.at[chip], chips.at[chip], s2.at[k], r2.at[k],
                                          device_id=(d // 2, lax.rem(d, 2) * 2 + c), device_id_type=MESH)
        cp.start()
        two.append(cp)
    for cp in two:
        cp.wait()
    tot[c] = ((chips[0] + chips[1]) + chips[2]) + chips[3]
    three = pltpu.make_async_remote_copy(tot.at[c], tot.at[c], s3, r3, device_id=partner, device_id_type=MESH)
    three.start()
    three.wait()
    for half in range(2):
        for q in range(2):
            lo = half * 2048 + q * 1024
            h_ref[0:4, lo:lo + 1024] += tot[half, q * 4:q * 4 + 4, :]


def _qkv_stage(me, xn, wbuf, copies, slot, sendA, recvA, ssem, rsem, qkv_ref):
    res = []
    for i in range(3):
        copies[2 * i].wait()
        z = _dot(xn[:, :2048], wbuf[slot + 2 * i])
        copies[2 * i + 1].wait()
        z = z + _dot(xn[:, 2048:], wbuf[slot + 2 * i + 1])
        res.append(z)
    for g in range(2):
        rows = [r[2 * g:2 * g + 2] for r in res] + [jnp.zeros((2, NB), F32)]
        sendA[g] = jnp.concatenate(rows, axis=0).astype(BF16)
    cps = _exchange(me, lambda d: sendA.at[d // 4], recvA.at[me], ssem, rsem)
    recvA[me] = sendA[me // 4]
    for cp in cps:
        cp.wait()
    qkv_ref[...] = recvA[...]


def _cache_copies(l, kc, vc, kb, vb, sem):
    return [pltpu.make_async_copy(src.at[l, b], dst.at[b], sem.at[i, b])
            for i, (src, dst) in enumerate(((kc, kb), (vc, vb))) for b in range(kb.shape[0])]


def _first(x, wq, wk, wv, g1h, kc, vc, h_ref, qkv_ref, kb, vb,
           wbuf, xm, xo, g1, sendA, recvA, wsem, xs, xr, sa, ra, gs, ks):
    dp, sp, c, me = _ids()
    cs = [pltpu.make_async_copy(x, xm, gs.at[0]), pltpu.make_async_copy(g1h, g1, gs.at[1])]
    cq = _qkv_copies(0, me, (wq, wk, wv), wbuf, wsem, 0, 0)
    ck = _cache_copies(0, kc, vc, kb, vb, ks)
    for cp in cs + cq + ck:
        cp.start()
    _barrier(me)
    cs[0].wait()
    ex = pltpu.make_async_remote_copy(xm, xo, xs, xr, device_id=(1 - dp, sp), device_id_type=MESH)
    ex.start()
    cs[1].wait()
    ex.wait()
    mine, other = xm[...].astype(F32), xo[...].astype(F32)
    h_ref[0:2, :] = jnp.where(dp == 0, mine, other)
    h_ref[2:4, :] = jnp.where(dp == 0, other, mine)
    h_ref[4:8, :] = jnp.zeros((4, h_ref.shape[1]), F32)
    xn = _rms(h_ref[...], g1[0:1, :])
    _qkv_stage(me, xn, wbuf, cq, 0, sendA, recvA, sa, ra, qkv_ref)
    for cp in ck:
        cp.wait()


def _layer(l, last, *refs):
    if last:
        (op_ref, hin, wo, w1, w2, g2h, y_ref, h_ref, *sc) = refs
    else:
        (op_ref, hin, wo, w1, w2, g2h, wq, wk, wv, g1h, kc, vc, h_ref, qkv_ref, kb, vb, *sc) = refs
    g2, gs, wbuf, recvB, att, u, psend, pown, precv, chips, tot = sc[:11]
    wsem, sb, rb, s1, r1, s2, r2, s3, r3 = sc[11:20]
    dp, sp, c, me = _ids()
    cm = _mlp_copies(l, dp, c, wo, w1, w2, wbuf, wsem)
    cg = [pltpu.make_async_copy(g2h, g2, gs.at[0])]
    ck = []
    if not last:
        g1, sendA, recvA, sa, ra, ks = sc[20:]
        cg.append(pltpu.make_async_copy(g1h, g1, gs.at[1]))
        cq = _qkv_copies(l + 1, me, (wq, wk, wv), wbuf, wsem, 2, 24)
        ck = _cache_copies(l + 1, kc, vc, kb, vb, ks)
    for cp in cg + cm + ck:
        cp.start()
    _barrier(me)
    cps = _exchange(me, lambda d: op_ref.at[2 * lax.rem(d, 4) + d // 4], recvB.at[me], sb, rb)
    recvB[me] = op_ref[2 * sp + dp]
    h_ref[...] = hin[...]
    att[...] = jnp.zeros_like(att)
    for cp in cg + cps:
        cp.wait()
    for g in range(2):
        ms = [recvB[4 * g + i, 1][:, 0:1] for i in range(4)]
        m = functools.reduce(jnp.maximum, ms)
        o = jnp.zeros((8, 128), F32)
        den = jnp.zeros((8, 1), F32)
        for i in range(4):
            e = jnp.exp(ms[i] - m)
            o = o + recvB[4 * g + i, 0] * e
            den = den + recvB[4 * g + i, 1][:, 64:65] * e
        a = o / den
        for b in range(2):
            for j in range(4):
                att[2 * g + b:2 * g + b + 1, j * 128:(j + 1) * 128] = a[4 * b + j:4 * b + j + 1]
    av = att[...].astype(BF16)

    def wo_block(t, q):
        n = 2 * t + q
        cm[n].wait()
        return _dot(av, wbuf[n // 4, (n % 4) * 512:(n % 4) * 512 + 512, :])

    def bufs(i):
        return [psend.at[i], pown.at[i], precv.at[i], chips.at[i], tot.at[i]]

    def sems(i):
        return [s1.at[i], r1.at[i], s2.at[i], r2.at[i], s3.at[i], r3.at[i]]

    _allreduce(wo_block, dp, sp, c, me, bufs(0), sems(0), h_ref)
    xn = _rms(h_ref[...], g2[l:l + 1, :])
    for j in range(4):
        cm[8 + 2 * j].wait()
        z = _dot(xn[:, :2048], wbuf[2 + 2 * j])
        cm[9 + 2 * j].wait()
        z = z + _dot(xn[:, 2048:], wbuf[3 + 2 * j])
        u[:, j * NB:(j + 1) * NB] = _gelu(z).astype(BF16)
    uv = u[...]
    if not last:
        for cp in cq:
            cp.start()

    def w2_block(t, q):
        n = 2 * t + q
        cm[16 + n].wait()
        return _dot(uv, wbuf[10 + n])

    _allreduce(w2_block, dp, sp, c, me, bufs(1), sems(1), h_ref)
    if last:
        hv = h_ref[...]
        y_ref[...] = jnp.where(dp == 0, hv[0:2], hv[2:4]).astype(BF16)
    else:
        xn = _rms(h_ref[...], g1[l + 1:l + 2, :])
        _qkv_stage(me, xn, wbuf, cq, 2, sendA, recvA, sa, ra, qkv_ref)
        for cp in ck:
            cp.wait()


def _attn(l, *refs):
    if l == 0:
        lensh, qkv, kin, vin, ko, vo, op_ref, kb, vb, *sc = refs
    else:
        lensh, qkv, kin, vin, _, _, ko, vo, op_ref, kb, vb, *sc = refs
    lens, tr, s_ref, m_ref, l_ref, o_ref, ls, kos, vos = sc
    nb, npos, nh, dh = kb.shape
    per = npos // CH
    n = nb * per
    base = lax.axis_index('sp') * npos
    cl = pltpu.make_async_copy(lensh, lens, ls)
    cl.start()

    def wr(dst, buf, sem, i):
        b, p = i // per, pl.multiple_of(lax.rem(i, per) * CH, CH)
        return pltpu.make_async_copy(buf.at[b, pl.ds(p, CH)], dst.at[l, b, pl.ds(p, CH)], sem.at[i])

    for src in range(8):
        v = qkv[src].astype(F32)
        for j in range(4):
            tr[src * 4 + j] = v[:, j * dh:(j + 1) * dh]
    m_ref[...] = jnp.full(m_ref.shape, -jnp.inf, F32)
    l_ref[...] = jnp.zeros_like(l_ref)
    o_ref[...] = jnp.zeros_like(o_ref)
    cl.wait()
    for b in range(nb):
        lp = lens[b] - 1 - base

        @pl.when((lp >= 0) & (lp < npos))
        def _():
            kb[b, lp] = tr[:, 2 + b, :].astype(BF16)
            vb[b, lp] = tr[:, 4 + b, :].astype(BF16)

    row = lax.broadcasted_iota(jnp.int32, (nh, CH * nh), 0)
    col = lax.broadcasted_iota(jnp.int32, (nh, CH * nh), 1)
    same = lax.rem(col, nh) == row

    def kstep(i, _):
        b = i // per
        p0 = pl.multiple_of(lax.rem(i, per) * CH, CH)
        q = tr[:, b, :].astype(BF16)
        kk = kb[b, pl.ds(p0, CH)].reshape(CH * nh, dh)
        s = lax.dot_general(q, kk, (((1,), (1,)), ((), ())), preferred_element_type=F32) * dh ** -0.5
        lim = (lens[b] - base - p0) * nh
        s = jnp.where(same & (col < lim), s, -jnp.inf)
        s_ref[i] = s
        m_ref[b] = jnp.maximum(m_ref[b], jnp.max(s, axis=1, keepdims=True))
        wr(ko, kb, kos, i).start()
        wr(vo, vb, vos, i).start()
        return 0

    def vstep(i, _):
        b = i // per
        p0 = pl.multiple_of(lax.rem(i, per) * CH, CH)
        m = m_ref[b][:, 0:1]
        m = jnp.where(m == -jnp.inf, 0.0, m)
        p = jnp.exp(s_ref[i] - m)
        l_ref[b] += jnp.sum(p, axis=1, keepdims=True)
        vv = vb[b, pl.ds(p0, CH)].reshape(CH * nh, dh)
        o_ref[b] += _dot(p.astype(BF16), vv)
        return 0

    lax.fori_loop(0, n, kstep, 0)
    lax.fori_loop(0, n, vstep, 0)
    lane = lax.broadcasted_iota(jnp.int32, (nh, dh), 1)
    for b in range(nb):
        ov = o_ref[b]
        ml = jnp.where(lane < 64, m_ref[b], l_ref[b])
        for r in range(8):
            op_ref[r, 0, b * 4:b * 4 + 4, :] = ov[4 * r:4 * r + 4]
            op_ref[r, 1, b * 4:b * 4 + 4, :] = ml[4 * r:4 * r + 4]
    for i in range(n):
        wr(ko, kb, kos, i).wait()
        wr(vo, vb, vos, i).wait()


def solution(mesh):
    kspec = P(None, 'dp', 'sp', None, None)
    DMA = pltpu.SemaphoreType.DMA

    def local(x, lens, wq, wk, wv, wo, w1, w2, g1, g2, kc, vc):
        nl, nb, npos, nh, dh = kc.shape
        d = x.shape[1]
        V = lambda *sh_dt: pltpu.VMEM(*sh_dt)
        hbm = lambda *xs: [pltpu.with_memory_space_constraint(a, pltpu.HBM) for a in xs]
        vm = lambda *xs: [pltpu.with_memory_space_constraint(a, pltpu.VMEM) for a in xs]
        h_sh, qkv_sh = V((8, d), F32), V((8, 8, NB), BF16)
        c_vm = V((nb, npos, nh, dh), BF16)
        qkv_sc = [V((2, 8, NB), BF16), V((8, 8, NB), BF16)]
        cparams = lambda i, mib: pltpu.CompilerParams(
            collective_id=i, has_side_effects=True, vmem_limit_bytes=mib * 2 ** 20)

        h, qkv, kb, vb = pl.pallas_call(
            _first, out_shape=(h_sh, qkv_sh, c_vm, c_vm),
            in_specs=[ANY] * 7, out_specs=(VM,) * 4,
            scratch_shapes=[V((6, 2048, NB), BF16), V((2, d), BF16), V((2, d), BF16), V((nl, d), BF16), *qkv_sc,
                            DMA((6,)), DMA, DMA, DMA((8,)), DMA((8,)), DMA((2,)), DMA((2, nb))],
            compiler_params=cparams(0, 16), name='first')(*hbm(x, wq, wk, wv, g1, kc, vc))

        def attn(l, qkv, kb, vb, ko, vo):
            n = nb * npos // CH
            c_sh = jax.ShapeDtypeStruct(kc.shape, kc.dtype)
            args = hbm(lens) + vm(qkv, kb, vb) + ([] if l == 0 else hbm(ko, vo))
            al = {2: 3, 3: 4}
            if l > 0:
                al.update({4: 0, 5: 1})
            return pl.pallas_call(
                functools.partial(_attn, l),
                out_shape=(c_sh, c_sh, V((8, 2, 8, dh), F32), c_vm, c_vm),
                in_specs=[ANY, VM, VM, VM] + ([] if l == 0 else [ANY, ANY]),
                out_specs=(ANY, ANY, VM, VM, VM),
                scratch_shapes=[pltpu.SMEM((nb,), jnp.int32), V((nh, 8, dh), F32), V((n, nh, CH * nh), F32),
                                V((nb, nh, dh), F32), V((nb, nh, dh), F32), V((nb, nh, dh), F32),
                                DMA, DMA((n,)), DMA((n,))],
                input_output_aliases=al,
                compiler_params=pltpu.CompilerParams(vmem_limit_bytes=14 * 2 ** 20), name='attn')(*args)[:3]

        def layer(l, op, h, last):
            sc = [V((nl, d), BF16), DMA((2,)), V((18, 2048, NB), BF16), V((8, 2, 8, dh), F32),
                  V((8, 512), F32), V((8, 2048), BF16),
                  V((2, 8, 1024), F32), V((2, 8, 1024), F32), V((2, 8, 1024), F32),
                  V((2, 4, 8, 1024), F32), V((2, 2, 8, 1024), F32),
                  DMA((30,)), DMA((8,)), DMA((8,)),
                  DMA((2,)), DMA((2,)), DMA((2, 4)), DMA((2, 4)), DMA((2,)), DMA((2,))]
            args = vm(op, h) + hbm(wo, w1, w2, g2)
            specs = [VM, VM, ANY, ANY, ANY, ANY]
            if last:
                sc = [V((8, d), F32)] + sc
                outs, out_specs, mib = jax.ShapeDtypeStruct((nb, d), BF16), VM, 39
            else:
                args += hbm(wq, wk, wv, g1, kc, vc)
                specs += [ANY] * 6
                sc += [V((nl, d), BF16), *qkv_sc, DMA((8,)), DMA((8,)), DMA((2, nb))]
                outs, out_specs, mib = (h_sh, qkv_sh, c_vm, c_vm), (VM,) * 4, LM
            return pl.pallas_call(
                functools.partial(_layer, l, last), out_shape=outs, in_specs=specs, out_specs=out_specs,
                scratch_shapes=sc, compiler_params=cparams(1 + l, mib), name='layer')(*args)

        ko = vo = None
        for l in range(nl):
            ko, vo, op = attn(l, qkv, kb, vb, ko, vo)
            if l < nl - 1:
                h, qkv, kb, vb = layer(l, op, h, False)
            else:
                y = layer(l, op, h, True)
        return y, ko, vo

    return jax.shard_map(
        local, mesh=mesh,
        in_specs=(P('dp', None), P('dp'), P(), P(), P(), P(None, 'sp', None), P(None, None, 'sp'),
                  P(None, 'sp', None), P(), P(), kspec, kspec),
        out_specs=(P('dp', None), kspec, kspec), check_vma=False)
```

```python
import functools

import jax
import jax.numpy as jnp
from jax import lax
from jax.experimental import pallas as pl
from jax.experimental.pallas import tpu as pltpu
from jax.sharding import PartitionSpec as P

EPS = 1e-6
MESH = pl.DeviceIdType.MESH
VM = pl.BlockSpec(memory_space=pltpu.VMEM)
ANY = pl.BlockSpec(memory_space=pltpu.HBM)
SM = pl.BlockSpec(memory_space=pltpu.SMEM)
F32, BF16 = jnp.float32, jnp.bfloat16
CH = 128
NB = 512
LM = 39


def _rms(h, g):
    r = lax.rsqrt(jnp.mean(h * h, axis=-1, keepdims=True) + EPS)
    return (h * r * g.astype(F32)).astype(BF16)


def _gelu(z):
    return 0.5 * z * (1.0 + jnp.tanh(0.7978845608028654 * (z + 0.044715 * z * z * z)))


def _dot(a, w):
    return jnp.dot(a, w, preferred_element_type=F32)


def _ids():
    dp, sp = lax.axis_index('dp'), lax.axis_index('sp')
    return dp, sp, lax.rem(sp, 2), dp * 4 + sp


def _barrier(me):
    sem = pltpu.get_barrier_semaphore()
    for k in range(1, 8):
        d = lax.rem(me + k, 8)
        pl.semaphore_signal(sem, inc=1, device_id=(d // 4, lax.rem(d, 4)), device_id_type=MESH)
    pl.semaphore_wait(sem, 7)


def _exchange(me, src, dst, ssem, rsem):
    out = []
    for k in range(1, 8):
        d = lax.rem(me + k, 8)
        c = pltpu.make_async_remote_copy(src(d), dst, ssem.at[k], rsem.at[k],
                                         device_id=(d // 4, lax.rem(d, 4)), device_id_type=MESH)
        c.start()
        out.append(c)
    return out


def _qkv_copies(l, me, ws, wbuf, wsem, slot, s0):
    out = []
    for i in range(3):
        for kh in range(2):
            n = 2 * i + kh
            out.append(pltpu.make_async_copy(
                ws[i].at[l, pl.ds(kh * 2048, 2048), pl.ds(pl.multiple_of(me * NB, NB), NB)],
                wbuf.at[slot + n], wsem.at[s0 + n]))
    return out


def _half_cols(t, q, c):
    half = (1 - c) if t < 2 else c
    return half * 2048 + q * 1024 + (t % 2) * NB


def _mlp_copies(l, dp, c, wo, w1, w2, wbuf, wsem):
    out = []
    for t in range(4):
        for q in range(2):
            n = 2 * t + q
            col = pl.multiple_of(_half_cols(t, q, c), NB)
            out.append(pltpu.make_async_copy(
                wo.at[l, pl.ds(pl.multiple_of(dp * 512, 512), 512), pl.ds(col, NB)],
                wbuf.at[n // 4, pl.ds((n % 4) * 512, 512)], wsem.at[n]))
    for j in range(4):
        for kh in range(2):
            n = 2 * j + kh
            out.append(pltpu.make_async_copy(
                w1.at[l, pl.ds(kh * 2048, 2048), pl.ds(pl.multiple_of(dp * 2048 + j * NB, NB), NB)],
                wbuf.at[2 + n], wsem.at[8 + n]))
    for t in range(4):
        for q in range(2):
            n = 2 * t + q
            col = pl.multiple_of(_half_cols(t, q, c), NB)
            out.append(pltpu.make_async_copy(
                w2.at[l, pl.ds(pl.multiple_of(dp * 2048, 2048), 2048), pl.ds(col, NB)],
                wbuf.at[10 + n], wsem.at[16 + n]))
    return out


def _allreduce(block, dp, sp, c, me, buf, sems, h_ref):
    psend, pown, precv, chips, tot = buf
    s1, r1, s2, r2, s3, r3 = sems
    partner = (dp, sp + 1 - 2 * c)
    for t in range(2):
        v = jnp.concatenate([block(t, 0)[0:4], block(t, 1)[0:4]], axis=0)
        psend[:, t * NB:(t + 1) * NB] = v
    one = pltpu.make_async_remote_copy(psend, precv, s1, r1, device_id=partner, device_id_type=MESH)
    one.start()
    for t in range(2):
        v = jnp.concatenate([block(t + 2, 0)[0:4], block(t + 2, 1)[0:4]], axis=0)
        pown[:, t * NB:(t + 1) * NB] = v
    one.wait()
    chip = dp * 2 + sp // 2
    chips[chip] = pown[...] + precv[...]
    two = []
    for k in range(1, 4):
        d = lax.rem(chip + k, 4)
        cp = pltpu.make_async_remote_copy(chips.at[chip], chips.at[chip], s2.at[k], r2.at[k],
                                          device_id=(d // 2, lax.rem(d, 2) * 2 + c), device_id_type=MESH)
        cp.start()
        two.append(cp)
    for cp in two:
        cp.wait()
    tot[c] = ((chips[0] + chips[1]) + chips[2]) + chips[3]
    three = pltpu.make_async_remote_copy(tot.at[c], tot.at[c], s3, r3, device_id=partner, device_id_type=MESH)
    three.start()
    three.wait()
    for half in range(2):
        for q in range(2):
            lo = half * 2048 + q * 1024
            h_ref[0:4, lo:lo + 1024] += tot[half, q * 4:q * 4 + 4, :]


def _qkv_stage(me, xn, wbuf, copies, slot, sendA, recvA, ssem, rsem, qkv_ref):
    res = []
    for i in range(3):
        copies[2 * i].wait()
        z = _dot(xn[:, :2048], wbuf[slot + 2 * i])
        copies[2 * i + 1].wait()
        z = z + _dot(xn[:, 2048:], wbuf[slot + 2 * i + 1])
        res.append(z)
    for g in range(2):
        rows = [r[2 * g:2 * g + 2] for r in res] + [jnp.zeros((2, NB), F32)]
        sendA[g] = jnp.concatenate(rows, axis=0).astype(BF16)
    cps = _exchange(me, lambda d: sendA.at[d // 4], recvA.at[me], ssem, rsem)
    recvA[me] = sendA[me // 4]
    for cp in cps:
        cp.wait()
    qkv_ref[...] = recvA[...]


def _cache_copies(l, kc, vc, kb, vb, sem):
    return [pltpu.make_async_copy(src.at[l, b], dst.at[b], sem.at[i, b])
            for i, (src, dst) in enumerate(((kc, kb), (vc, vb))) for b in range(kb.shape[0])]


def _first(xm, wq, wk, wv, g1, kc, vc, h_ref, qkv_ref, kb, vb,
           wbuf, xo, sendA, recvA, wsem, xs, xr, sa, ra, ks):
    dp, sp, c, me = _ids()
    cq = _qkv_copies(0, me, (wq, wk, wv), wbuf, wsem, 0, 0)
    ck = _cache_copies(0, kc, vc, kb, vb, ks)
    for cp in cq:
        cp.start()
    _barrier(me)
    ex = pltpu.make_async_remote_copy(xm, xo, xs, xr, device_id=(1 - dp, sp), device_id_type=MESH)
    ex.start()
    ex.wait()
    mine, other = xm[...].astype(F32), xo[...].astype(F32)
    h_ref[0:2, :] = jnp.where(dp == 0, mine, other)
    h_ref[2:4, :] = jnp.where(dp == 0, other, mine)
    h_ref[4:8, :] = jnp.zeros((4, h_ref.shape[1]), F32)
    xn = _rms(h_ref[...], g1[0:1, :])
    for cp in ck:
        cp.start()
    _qkv_stage(me, xn, wbuf, cq, 0, sendA, recvA, sa, ra, qkv_ref)
    for cp in ck:
        cp.wait()


def _layer(l, last, *refs):
    if last:
        (op_ref, hin, wo, w1, w2, g2, y_ref, h_ref, *sc) = refs
    else:
        (op_ref, hin, wo, w1, w2, g2, wq, wk, wv, g1, kc, vc, h_ref, qkv_ref, kb, vb, *sc) = refs
    wbuf, recvB, att, u, psend, pown, precv, chips, tot = sc[:9]
    wsem, sb, rb, s1, r1, s2, r2, s3, r3 = sc[9:18]
    dp, sp, c, me = _ids()
    cm = _mlp_copies(l, dp, c, wo, w1, w2, wbuf, wsem)
    ck = []
    if not last:
        sendA, recvA, sa, ra, ks = sc[18:]
        cq = _qkv_copies(l + 1, me, (wq, wk, wv), wbuf, wsem, 2, 24)
        ck = _cache_copies(l + 1, kc, vc, kb, vb, ks)
    for cp in cm + ck:
        cp.start()
    _barrier(me)
    cps = _exchange(me, lambda d: op_ref.at[2 * lax.rem(d, 4) + d // 4], recvB.at[me], sb, rb)
    recvB[me] = op_ref[2 * sp + dp]
    h_ref[...] = hin[...]
    att[...] = jnp.zeros_like(att)
    for cp in cps:
        cp.wait()
    for g in range(2):
        ms = [recvB[4 * g + i, 1][:, 0:1] for i in range(4)]
        m = functools.reduce(jnp.maximum, ms)
        o = jnp.zeros((8, 128), F32)
        den = jnp.zeros((8, 1), F32)
        for i in range(4):
            e = jnp.exp(ms[i] - m)
            o = o + recvB[4 * g + i, 0] * e
            den = den + recvB[4 * g + i, 1][:, 64:65] * e
        a = o / den
        for b in range(2):
            for j in range(4):
                att[2 * g + b:2 * g + b + 1, j * 128:(j + 1) * 128] = a[4 * b + j:4 * b + j + 1]
    av = att[...].astype(BF16)

    def wo_block(t, q):
        n = 2 * t + q
        cm[n].wait()
        return _dot(av, wbuf[n // 4, (n % 4) * 512:(n % 4) * 512 + 512, :])

    def bufs(i):
        return [psend.at[i], pown.at[i], precv.at[i], chips.at[i], tot.at[i]]

    def sems(i):
        return [s1.at[i], r1.at[i], s2.at[i], r2.at[i], s3.at[i], r3.at[i]]

    _allreduce(wo_block, dp, sp, c, me, bufs(0), sems(0), h_ref)
    xn = _rms(h_ref[...], g2[l:l + 1, :])
    for j in range(4):
        cm[8 + 2 * j].wait()
        z = _dot(xn[:, :2048], wbuf[2 + 2 * j])
        cm[9 + 2 * j].wait()
        z = z + _dot(xn[:, 2048:], wbuf[3 + 2 * j])
        u[:, j * NB:(j + 1) * NB] = _gelu(z).astype(BF16)
    uv = u[...]
    if not last:
        for cp in cq:
            cp.start()

    def w2_block(t, q):
        n = 2 * t + q
        cm[16 + n].wait()
        return _dot(uv, wbuf[10 + n])

    _allreduce(w2_block, dp, sp, c, me, bufs(1), sems(1), h_ref)
    if last:
        hv = h_ref[...]
        y_ref[...] = jnp.where(dp == 0, hv[0:2], hv[2:4]).astype(BF16)
    else:
        xn = _rms(h_ref[...], g1[l + 1:l + 2, :])
        _qkv_stage(me, xn, wbuf, cq, 2, sendA, recvA, sa, ra, qkv_ref)
        for cp in ck:
            cp.wait()


def _attn(l, *refs):
    if l == 0:
        lensh, qkv, kin, vin, ko, vo, op_ref, kb, vb, *sc = refs
    else:
        lensh, qkv, kin, vin, _, _, ko, vo, op_ref, kb, vb, *sc = refs
    lens, tr, s_ref, m_ref, l_ref, o_ref, ls, kos, vos = sc
    nb, npos, nh, dh = kb.shape
    per = npos // CH
    n = nb * per
    base = lax.axis_index('sp') * npos
    cl = pltpu.make_async_copy(lensh, lens, ls)
    cl.start()

    def wr(dst, buf, sem, i):
        b, p = i // per, pl.multiple_of(lax.rem(i, per) * CH, CH)
        return pltpu.make_async_copy(buf.at[b, pl.ds(p, CH)], dst.at[l, b, pl.ds(p, CH)], sem.at[i])

    for src in range(8):
        v = qkv[src].astype(F32)
        for j in range(4):
            tr[src * 4 + j] = v[:, j * dh:(j + 1) * dh]
    m_ref[...] = jnp.full(m_ref.shape, -jnp.inf, F32)
    l_ref[...] = jnp.zeros_like(l_ref)
    o_ref[...] = jnp.zeros_like(o_ref)
    cl.wait()
    for b in range(nb):
        lp = lens[b] - 1 - base

        @pl.when((lp >= 0) & (lp < npos))
        def _():
            kb[b, lp] = tr[:, 2 + b, :].astype(BF16)
            vb[b, lp] = tr[:, 4 + b, :].astype(BF16)

    row = lax.broadcasted_iota(jnp.int32, (nh, CH * nh), 0)
    col = lax.broadcasted_iota(jnp.int32, (nh, CH * nh), 1)
    same = lax.rem(col, nh) == row

    def kstep(i, _):
        b = i // per
        p0 = pl.multiple_of(lax.rem(i, per) * CH, CH)
        q = tr[:, b, :].astype(BF16)
        kk = kb[b, pl.ds(p0, CH)].reshape(CH * nh, dh)
        s = lax.dot_general(q, kk, (((1,), (1,)), ((), ())), preferred_element_type=F32) * dh ** -0.5
        lim = (lens[b] - base - p0) * nh
        s = jnp.where(same & (col < lim), s, -jnp.inf)
        s_ref[i] = s
        m_ref[b] = jnp.maximum(m_ref[b], jnp.max(s, axis=1, keepdims=True))
        wr(ko, kb, kos, i).start()
        wr(vo, vb, vos, i).start()
        return 0

    def vstep(i, _):
        b = i // per
        p0 = pl.multiple_of(lax.rem(i, per) * CH, CH)
        m = m_ref[b][:, 0:1]
        m = jnp.where(m == -jnp.inf, 0.0, m)
        p = jnp.exp(s_ref[i] - m)
        l_ref[b] += jnp.sum(p, axis=1, keepdims=True)
        vv = vb[b, pl.ds(p0, CH)].reshape(CH * nh, dh)
        o_ref[b] += _dot(p.astype(BF16), vv)
        return 0

    lax.fori_loop(0, n, kstep, 0)
    lax.fori_loop(0, n, vstep, 0)
    lane = lax.broadcasted_iota(jnp.int32, (nh, dh), 1)
    for b in range(nb):
        ov = o_ref[b]
        ml = jnp.where(lane < 64, m_ref[b], l_ref[b])
        for r in range(8):
            op_ref[r, 0, b * 4:b * 4 + 4, :] = ov[4 * r:4 * r + 4]
            op_ref[r, 1, b * 4:b * 4 + 4, :] = ml[4 * r:4 * r + 4]
    for i in range(n):
        wr(ko, kb, kos, i).wait()
        wr(vo, vb, vos, i).wait()


def solution(mesh):
    kspec = P(None, 'dp', 'sp', None, None)
    DMA = pltpu.SemaphoreType.DMA

    def local(x, lens, wq, wk, wv, wo, w1, w2, g1, g2, kc, vc):
        nl, nb, npos, nh, dh = kc.shape
        d = x.shape[1]
        V = lambda *sh_dt: pltpu.VMEM(*sh_dt)
        hbm = lambda *xs: [pltpu.with_memory_space_constraint(a, pltpu.HBM) for a in xs]
        vm = lambda *xs: [pltpu.with_memory_space_constraint(a, pltpu.VMEM) for a in xs]
        h_sh, qkv_sh = V((8, d), F32), V((8, 8, NB), BF16)
        c_vm = V((nb, npos, nh, dh), BF16)
        qkv_sc = [V((2, 8, NB), BF16), V((8, 8, NB), BF16)]
        cparams = lambda i, mib: pltpu.CompilerParams(
            collective_id=i, has_side_effects=True, vmem_limit_bytes=mib * 2 ** 20)

        h, qkv, kb, vb = pl.pallas_call(
            _first, out_shape=(h_sh, qkv_sh, c_vm, c_vm),
            in_specs=[VM, ANY, ANY, ANY, VM, ANY, ANY], out_specs=(VM,) * 4,
            scratch_shapes=[V((6, 2048, NB), BF16), V((2, d), BF16), *qkv_sc,
                            DMA((6,)), DMA, DMA, DMA((8,)), DMA((8,)), DMA((2, nb))],
            compiler_params=cparams(0, 16), name='first')(*(vm(x) + hbm(wq, wk, wv) + vm(g1) + hbm(kc, vc)))

        def attn(l, qkv, kb, vb, ko, vo):
            n = nb * npos // CH
            c_sh = jax.ShapeDtypeStruct(kc.shape, kc.dtype)
            args = hbm(lens) + vm(qkv, kb, vb) + ([] if l == 0 else hbm(ko, vo))
            al = {2: 3, 3: 4}
            if l > 0:
                al.update({4: 0, 5: 1})
            return pl.pallas_call(
                functools.partial(_attn, l),
                out_shape=(c_sh, c_sh, V((8, 2, 8, dh), F32), c_vm, c_vm),
                in_specs=[ANY, VM, VM, VM] + ([] if l == 0 else [ANY, ANY]),
                out_specs=(ANY, ANY, VM, VM, VM),
                scratch_shapes=[pltpu.SMEM((nb,), jnp.int32), V((nh, 8, dh), F32), V((n, nh, CH * nh), F32),
                                V((nb, nh, dh), F32), V((nb, nh, dh), F32), V((nb, nh, dh), F32),
                                DMA, DMA((n,)), DMA((n,))],
                input_output_aliases=al,
                compiler_params=pltpu.CompilerParams(vmem_limit_bytes=14 * 2 ** 20), name='attn')(*args)[:3]

        def layer(l, op, h, last):
            sc = [V((18, 2048, NB), BF16), V((8, 2, 8, dh), F32),
                  V((8, 512), F32), V((8, 2048), BF16),
                  V((2, 8, 1024), F32), V((2, 8, 1024), F32), V((2, 8, 1024), F32),
                  V((2, 4, 8, 1024), F32), V((2, 2, 8, 1024), F32),
                  DMA((30,)), DMA((8,)), DMA((8,)),
                  DMA((2,)), DMA((2,)), DMA((2, 4)), DMA((2, 4)), DMA((2,)), DMA((2,))]
            args = vm(op, h) + hbm(wo, w1, w2) + vm(g2)
            specs = [VM, VM, ANY, ANY, ANY, VM]
            if last:
                sc = [V((8, d), F32)] + sc
                outs, out_specs, mib = jax.ShapeDtypeStruct((nb, d), BF16), VM, 39
            else:
                args += hbm(wq, wk, wv) + vm(g1) + hbm(kc, vc)
                specs += [ANY, ANY, ANY, VM, ANY, ANY]
                sc += [*qkv_sc, DMA((8,)), DMA((8,)), DMA((2, nb))]
                outs, out_specs, mib = (h_sh, qkv_sh, c_vm, c_vm), (VM,) * 4, LM
            return pl.pallas_call(
                functools.partial(_layer, l, last), out_shape=outs, in_specs=specs, out_specs=out_specs,
                scratch_shapes=sc, compiler_params=cparams(1 + l, mib), name='layer')(*args)

        ko = vo = None
        for l in range(nl):
            ko, vo, op = attn(l, qkv, kb, vb, ko, vo)
            if l < nl - 1:
                h, qkv, kb, vb = layer(l, op, h, False)
            else:
                y = layer(l, op, h, True)
        return y, ko, vo

    return jax.shard_map(
        local, mesh=mesh,
        in_specs=(P('dp', None), P('dp'), P(), P(), P(), P(None, 'sp', None), P(None, None, 'sp'),
                  P(None, 'sp', None), P(), P(), kspec, kspec),
        out_specs=(P('dp', None), kspec, kspec), check_vma=False)
```

```python
import functools

import jax
import jax.numpy as jnp
from jax import lax
from jax.experimental import pallas as pl
from jax.experimental.pallas import tpu as pltpu
from jax.sharding import PartitionSpec as P

EPS = 1e-6
MESH = pl.DeviceIdType.MESH
VM = pl.BlockSpec(memory_space=pltpu.VMEM)
ANY = pl.BlockSpec(memory_space=pltpu.HBM)
SM = pl.BlockSpec(memory_space=pltpu.SMEM)
F32, BF16 = jnp.float32, jnp.bfloat16
CH = 128
NB = 512
LM = 39


def _rms(h, g):
    r = lax.rsqrt(jnp.mean(h * h, axis=-1, keepdims=True) + EPS)
    return (h * r * g.astype(F32)).astype(BF16)


def _gelu(z):
    return 0.5 * z * (1.0 + jnp.tanh(0.7978845608028654 * (z + 0.044715 * z * z * z)))


def _dot(a, w):
    return jnp.dot(a, w, preferred_element_type=F32)


def _ids():
    dp, sp = lax.axis_index('dp'), lax.axis_index('sp')
    return dp, sp, lax.rem(sp, 2), dp * 4 + sp


def _hello(me):
    sem = pltpu.get_barrier_semaphore()
    for k in range(1, 8):
        d = lax.rem(me + k, 8)
        pl.semaphore_signal(sem, inc=1, device_id=(d // 4, lax.rem(d, 4)), device_id_type=MESH)


def _barrier():
    pl.semaphore_wait(pltpu.get_barrier_semaphore(), 7)


def _exchange(me, src, dst, ssem, rsem):
    out = []
    for k in range(1, 8):
        d = lax.rem(me + k, 8)
        c = pltpu.make_async_remote_copy(src(d), dst, ssem.at[k], rsem.at[k],
                                         device_id=(d // 4, lax.rem(d, 4)), device_id_type=MESH)
        c.start()
        out.append(c)
    return out


def _qkv_copies(l, me, ws, wbuf, wsem, slot, s0):
    out = []
    for i in range(3):
        for kh in range(2):
            n = 2 * i + kh
            out.append(pltpu.make_async_copy(
                ws[i].at[l, pl.ds(kh * 2048, 2048), pl.ds(pl.multiple_of(me * NB, NB), NB)],
                wbuf.at[slot + n], wsem.at[s0 + n]))
    return out


def _half_cols(t, q, c):
    half = (1 - c) if t < 2 else c
    return half * 2048 + q * 1024 + (t % 2) * NB


def _mlp_copies(l, dp, c, wo, w1, w2, wbuf, wsem):
    out = []
    for t in range(4):
        for q in range(2):
            n = 2 * t + q
            col = pl.multiple_of(_half_cols(t, q, c), NB)
            out.append(pltpu.make_async_copy(
                wo.at[l, pl.ds(pl.multiple_of(dp * 512, 512), 512), pl.ds(col, NB)],
                wbuf.at[n // 4, pl.ds((n % 4) * 512, 512)], wsem.at[n]))
    for j in range(4):
        for kh in range(2):
            n = 2 * j + kh
            out.append(pltpu.make_async_copy(
                w1.at[l, pl.ds(kh * 2048, 2048), pl.ds(pl.multiple_of(dp * 2048 + j * NB, NB), NB)],
                wbuf.at[2 + n], wsem.at[8 + n]))
    for t in range(4):
        for q in range(2):
            n = 2 * t + q
            col = pl.multiple_of(_half_cols(t, q, c), NB)
            out.append(pltpu.make_async_copy(
                w2.at[l, pl.ds(pl.multiple_of(dp * 2048, 2048), 2048), pl.ds(col, NB)],
                wbuf.at[10 + n], wsem.at[16 + n]))
    return out


def _allreduce(block, dp, sp, c, me, buf, sems, h_ref):
    psend, pown, precv, chips, tot = buf
    s1, r1, s2, r2, s3, r3 = sems
    partner = (dp, sp + 1 - 2 * c)
    for t in range(2):
        v = jnp.concatenate([block(t, 0)[0:4], block(t, 1)[0:4]], axis=0)
        psend[:, t * NB:(t + 1) * NB] = v
    one = pltpu.make_async_remote_copy(psend, precv, s1, r1, device_id=partner, device_id_type=MESH)
    one.start()
    for t in range(2):
        v = jnp.concatenate([block(t + 2, 0)[0:4], block(t + 2, 1)[0:4]], axis=0)
        pown[:, t * NB:(t + 1) * NB] = v
    one.wait()
    chip = dp * 2 + sp // 2
    chips[chip] = pown[...] + precv[...]
    two = []
    for k in range(1, 4):
        d = lax.rem(chip + k, 4)
        cp = pltpu.make_async_remote_copy(chips.at[chip], chips.at[chip], s2.at[k], r2.at[k],
                                          device_id=(d // 2, lax.rem(d, 2) * 2 + c), device_id_type=MESH)
        cp.start()
        two.append(cp)
    for cp in two:
        cp.wait()
    tot[c] = ((chips[0] + chips[1]) + chips[2]) + chips[3]
    three = pltpu.make_async_remote_copy(tot.at[c], tot.at[c], s3, r3, device_id=partner, device_id_type=MESH)
    three.start()
    three.wait()
    for half in range(2):
        for q in range(2):
            lo = half * 2048 + q * 1024
            h_ref[0:4, lo:lo + 1024] += tot[half, q * 4:q * 4 + 4, :]


def _qkv_stage(chase, me, xn, wbuf, copies, slot, sendA, recvA, ssem, rsem, qkv_ref):
    res = []
    step = 2 if chase else 6
    for i in range(3):
        if 2 * i % step == 0:
            for cp in copies[2 * i:2 * i + step]:
                cp.wait()
        z = _dot(xn[:, :2048], wbuf[slot + 2 * i])
        z = z + _dot(xn[:, 2048:], wbuf[slot + 2 * i + 1])
        res.append(z)
    for g in range(2):
        rows = [r[2 * g:2 * g + 2] for r in res] + [jnp.zeros((2, NB), F32)]
        sendA[g] = jnp.concatenate(rows, axis=0).astype(BF16)
    cps = _exchange(me, lambda d: sendA.at[d // 4], recvA.at[me], ssem, rsem)
    recvA[me] = sendA[me // 4]
    for cp in cps:
        cp.wait()
    qkv_ref[...] = recvA[...]


def _cache_copies(l, kc, vc, kb, vb, sem):
    return [pltpu.make_async_copy(src.at[l, b], dst.at[b], sem.at[i, b])
            for i, (src, dst) in enumerate(((kc, kb), (vc, vb))) for b in range(kb.shape[0])]


def _first(x, wq, wk, wv, g1h, kc, vc, h_ref, qkv_ref, kb, vb,
           wbuf, xm, xo, g1, sendA, recvA, wsem, xs, xr, sa, ra, gs, ks):
    dp, sp, c, me = _ids()
    cq = _qkv_copies(0, me, (wq, wk, wv), wbuf, wsem, 0, 0)
    ck = _cache_copies(0, kc, vc, kb, vb, ks)
    _hello(me)
    cs = [pltpu.make_async_copy(x, xm, gs.at[0]), pltpu.make_async_copy(g1h, g1, gs.at[1])]
    for cp in cs:
        cp.start()
    for cp in cs:
        cp.wait()
    for cp in cq:
        cp.start()
    _barrier()
    ex = pltpu.make_async_remote_copy(xm, xo, xs, xr, device_id=(1 - dp, sp), device_id_type=MESH)
    ex.start()
    ex.wait()
    mine, other = xm[...].astype(F32), xo[...].astype(F32)
    h_ref[0:2, :] = jnp.where(dp == 0, mine, other)
    h_ref[2:4, :] = jnp.where(dp == 0, other, mine)
    h_ref[4:8, :] = jnp.zeros((4, h_ref.shape[1]), F32)
    xn = _rms(h_ref[...], g1[0:1, :])
    for cp in ck:
        cp.start()
    _qkv_stage(True, me, xn, wbuf, cq, 0, sendA, recvA, sa, ra, qkv_ref)
    for cp in ck:
        cp.wait()


def _layer(l, last, *refs):
    if last:
        (op_ref, hin, wo, w1, w2, g2, y_ref, h_ref, *sc) = refs
    else:
        (op_ref, hin, wo, w1, w2, g2, wq, wk, wv, g1, kc, vc, h_ref, qkv_ref, kb, vb, *sc) = refs
    wbuf, recvB, att, u, psend, pown, precv, chips, tot = sc[:9]
    wsem, sb, rb, s1, r1, s2, r2, s3, r3 = sc[9:18]
    dp, sp, c, me = _ids()
    _hello(me)
    cm = _mlp_copies(l, dp, c, wo, w1, w2, wbuf, wsem)
    ck, cq = [], []
    if not last:
        sendA, recvA, sa, ra, ks = sc[18:]
        cq = _qkv_copies(l + 1, me, (wq, wk, wv), wbuf, wsem, 2, 24)
        ck = _cache_copies(l + 1, kc, vc, kb, vb, ks)
    for cp in cm[:16]:
        cp.start()
    h_ref[...] = hin[...]
    att[...] = jnp.zeros_like(att)
    recvB[me] = op_ref[2 * sp + dp]
    _barrier()
    cps = _exchange(me, lambda d: op_ref.at[2 * lax.rem(d, 4) + d // 4], recvB.at[me], sb, rb)
    for cp in cps:
        cp.wait()
    for cp in cm[16:]:
        cp.start()
    for g in range(2):
        ms = [recvB[4 * g + i, 1][:, 0:1] for i in range(4)]
        m = functools.reduce(jnp.maximum, ms)
        o = jnp.zeros((8, 128), F32)
        den = jnp.zeros((8, 1), F32)
        for i in range(4):
            e = jnp.exp(ms[i] - m)
            o = o + recvB[4 * g + i, 0] * e
            den = den + recvB[4 * g + i, 1][:, 64:65] * e
        a = o / den
        for b in range(2):
            for j in range(4):
                att[2 * g + b:2 * g + b + 1, j * 128:(j + 1) * 128] = a[4 * b + j:4 * b + j + 1]
    av = att[...].astype(BF16)
    for cp in cm[:8]:
        cp.wait()

    def wo_block(t, q):
        n = 2 * t + q
        return _dot(av, wbuf[n // 4, (n % 4) * 512:(n % 4) * 512 + 512, :])

    def bufs(i):
        return [psend.at[i], pown.at[i], precv.at[i], chips.at[i], tot.at[i]]

    def sems(i):
        return [s1.at[i], r1.at[i], s2.at[i], r2.at[i], s3.at[i], r3.at[i]]

    _allreduce(wo_block, dp, sp, c, me, bufs(0), sems(0), h_ref)
    for cp in ck:
        cp.start()
    xn = _rms(h_ref[...], g2[l:l + 1, :])
    for cp in cm[8:16]:
        cp.wait()
    for j in range(4):
        z = _dot(xn[:, :2048], wbuf[2 + 2 * j])
        z = z + _dot(xn[:, 2048:], wbuf[3 + 2 * j])
        u[:, j * NB:(j + 1) * NB] = _gelu(z).astype(BF16)
    uv = u[...]
    for cp in cm[16:]:
        cp.wait()
    for cp in cq:
        cp.start()

    def w2_block(t, q):
        n = 2 * t + q
        return _dot(uv, wbuf[10 + n])

    _allreduce(w2_block, dp, sp, c, me, bufs(1), sems(1), h_ref)
    if last:
        hv = h_ref[...]
        y_ref[...] = jnp.where(dp == 0, hv[0:2], hv[2:4]).astype(BF16)
    else:
        xn = _rms(h_ref[...], g1[l + 1:l + 2, :])
        _qkv_stage(False, me, xn, wbuf, cq, 2, sendA, recvA, sa, ra, qkv_ref)
        for cp in ck:
            cp.wait()


def _attn(l, *refs):
    if l == 0:
        lensh, qkv, kin, vin, ko, vo, op_ref, kb, vb, *sc = refs
    else:
        lensh, qkv, kin, vin, _, _, ko, vo, op_ref, kb, vb, *sc = refs
    lens, tr, q_ref, s_ref, m_ref, l_ref, o_ref, ls, kos, vos = sc
    nb, npos, nh, dh = kb.shape
    per = npos // CH
    n = nb * per
    base = lax.axis_index('sp') * npos
    cl = pltpu.make_async_copy(lensh, lens, ls)
    cl.start()

    def wr(dst, buf, sem, i):
        b, p = i // per, pl.multiple_of(lax.rem(i, per) * CH, CH)
        return pltpu.make_async_copy(buf.at[b, pl.ds(p, CH)], dst.at[l, b, pl.ds(p, CH)], sem.at[i])

    for src in range(8):
        v = qkv[src].astype(F32)
        for j in range(4):
            tr[src * 4 + j] = v[:, j * dh:(j + 1) * dh]
    m_ref[...] = jnp.full(m_ref.shape, -jnp.inf, F32)
    l_ref[...] = jnp.zeros_like(l_ref)
    o_ref[...] = jnp.zeros_like(o_ref)
    z = jnp.zeros((nh, dh), BF16)
    for b in range(nb):
        q = tr[:, b, :].astype(BF16)
        q_ref[b, 0:nh] = jnp.concatenate([q, z], axis=1)
        q_ref[b, nh:2 * nh] = jnp.concatenate([z, q], axis=1)
    cl.wait()
    for b in range(nb):
        lp = lens[b] - 1 - base

        @pl.when((lp >= 0) & (lp < npos))
        def _():
            kb[b, lp] = tr[:, 2 + b, :].astype(BF16)
            vb[b, lp] = tr[:, 4 + b, :].astype(BF16)

    hc = CH * nh // 2
    row = lax.broadcasted_iota(jnp.int32, (2 * nh, hc), 0)
    col = lax.broadcasted_iota(jnp.int32, (2 * nh, hc), 1)
    same = lax.rem(col, nh) == lax.rem(row, nh)
    at = col + (row // nh) * hc

    def pair(buf, b, p0):
        return jnp.concatenate([buf[b, pl.ds(p0, CH // 2)].reshape(hc, dh),
                                buf[b, pl.ds(p0 + CH // 2, CH // 2)].reshape(hc, dh)], axis=1)

    for i in range(n):
        wr(ko, kb, kos, i).start()
        wr(vo, vb, vos, i).start()

    def kstep(t, _):
        b = t * 4 // per
        for j in range(4):
            i = t * 4 + j
            p0 = pl.multiple_of(lax.rem(i, per) * CH, CH)
            s = lax.dot_general(q_ref[b], pair(kb, b, p0), (((1,), (1,)), ((), ())),
                                preferred_element_type=F32) * dh ** -0.5
            lim = (lens[b] - base - p0) * nh
            s = jnp.where(same & (at < lim), s, -jnp.inf)
            s_ref[i] = s
            m_ref[b] = jnp.maximum(m_ref[b], jnp.max(s, axis=1, keepdims=True))
        return 0

    def vstep(t, _):
        b = t * 4 // per
        m = m_ref[b][:, 0:1]
        lt, ot = l_ref[b], o_ref[b]
        for j in range(4):
            i = t * 4 + j
            p0 = pl.multiple_of(lax.rem(i, per) * CH, CH)
            p = jnp.exp(s_ref[i] - m)
            lt = lt + jnp.sum(p, axis=1, keepdims=True)
            ot = ot + _dot(p.astype(BF16), pair(vb, b, p0))
        l_ref[b] = lt
        o_ref[b] = ot
        return 0

    lax.fori_loop(0, n // 4, kstep, 0)
    mt = []
    for b in range(nb):
        m = jnp.maximum(m_ref[b, 0:nh], m_ref[b, nh:2 * nh])
        mt.append(m)
        m = jnp.where(m == -jnp.inf, 0.0, m)
        m_ref[b, 0:nh] = m
        m_ref[b, nh:2 * nh] = m
    lax.fori_loop(0, n // 4, vstep, 0)
    lane = lax.broadcasted_iota(jnp.int32, (nh, dh), 1)
    for b in range(nb):
        ov = o_ref[b, 0:nh, 0:dh] + o_ref[b, nh:2 * nh, dh:2 * dh]
        ml = jnp.where(lane < 64, mt[b], l_ref[b, 0:nh] + l_ref[b, nh:2 * nh])
        for r in range(8):
            op_ref[r, 0, b * 4:b * 4 + 4, :] = ov[4 * r:4 * r + 4]
            op_ref[r, 1, b * 4:b * 4 + 4, :] = ml[4 * r:4 * r + 4]
    for i in range(n):
        wr(ko, kb, kos, i).wait()
        wr(vo, vb, vos, i).wait()


def solution(mesh):
    kspec = P(None, 'dp', 'sp', None, None)
    DMA = pltpu.SemaphoreType.DMA

    def local(x, lens, wq, wk, wv, wo, w1, w2, g1, g2, kc, vc):
        nl, nb, npos, nh, dh = kc.shape
        d = x.shape[1]
        V = lambda *sh_dt: pltpu.VMEM(*sh_dt)
        hbm = lambda *xs: [pltpu.with_memory_space_constraint(a, pltpu.HBM) for a in xs]
        vm = lambda *xs: [pltpu.with_memory_space_constraint(a, pltpu.VMEM) for a in xs]
        h_sh, qkv_sh = V((8, d), F32), V((8, 8, NB), BF16)
        c_vm = V((nb, npos, nh, dh), BF16)
        qkv_sc = [V((2, 8, NB), BF16), V((8, 8, NB), BF16)]
        cparams = lambda i, mib: pltpu.CompilerParams(
            collective_id=i, has_side_effects=True, vmem_limit_bytes=mib * 2 ** 20)

        h, qkv, kb, vb = pl.pallas_call(
            _first, out_shape=(h_sh, qkv_sh, c_vm, c_vm),
            in_specs=[ANY] * 7, out_specs=(VM,) * 4,
            scratch_shapes=[V((6, 2048, NB), BF16), V((2, d), BF16), V((2, d), BF16), V((nl, d), BF16), *qkv_sc,
                            DMA((6,)), DMA, DMA, DMA((8,)), DMA((8,)), DMA((2,)), DMA((2, nb))],
            compiler_params=cparams(0, 16), name='first')(*hbm(x, wq, wk, wv, g1, kc, vc))

        def attn(l, qkv, kb, vb, ko, vo):
            n = nb * npos // CH
            c_sh = jax.ShapeDtypeStruct(kc.shape, kc.dtype)
            args = hbm(lens) + vm(qkv, kb, vb) + ([] if l == 0 else hbm(ko, vo))
            al = {2: 3, 3: 4}
            if l > 0:
                al.update({4: 0, 5: 1})
            return pl.pallas_call(
                functools.partial(_attn, l),
                out_shape=(c_sh, c_sh, V((8, 2, 8, dh), F32), c_vm, c_vm),
                in_specs=[ANY, VM, VM, VM] + ([] if l == 0 else [ANY, ANY]),
                out_specs=(ANY, ANY, VM, VM, VM),
                scratch_shapes=[pltpu.SMEM((nb,), jnp.int32), V((nh, 8, dh), F32), V((nb, 2 * nh, 2 * dh), BF16),
                                V((n, 2 * nh, CH * nh // 2), F32), V((nb, 2 * nh, dh), F32),
                                V((nb, 2 * nh, dh), F32), V((nb, 2 * nh, 2 * dh), F32),
                                DMA, DMA((n,)), DMA((n,))],
                input_output_aliases=al,
                compiler_params=pltpu.CompilerParams(vmem_limit_bytes=14 * 2 ** 20), name='attn')(*args)[:3]

        def layer(l, op, h, last):
            sc = [V((18, 2048, NB), BF16), V((8, 2, 8, dh), F32),
                  V((8, 512), F32), V((8, 2048), BF16),
                  V((2, 8, 1024), F32), V((2, 8, 1024), F32), V((2, 8, 1024), F32),
                  V((2, 4, 8, 1024), F32), V((2, 2, 8, 1024), F32),
                  DMA((30,)), DMA((8,)), DMA((8,)),
                  DMA((2,)), DMA((2,)), DMA((2, 4)), DMA((2, 4)), DMA((2,)), DMA((2,))]
            args = vm(op, h) + hbm(wo, w1, w2) + vm(g2)
            specs = [VM, VM, ANY, ANY, ANY, VM]
            if last:
                sc = [V((8, d), F32)] + sc
                outs, out_specs, mib = jax.ShapeDtypeStruct((nb, d), BF16), VM, 39
            else:
                args += hbm(wq, wk, wv) + vm(g1) + hbm(kc, vc)
                specs += [ANY, ANY, ANY, VM, ANY, ANY]
                sc += [*qkv_sc, DMA((8,)), DMA((8,)), DMA((2, nb))]
                outs, out_specs, mib = (h_sh, qkv_sh, c_vm, c_vm), (VM,) * 4, LM
            return pl.pallas_call(
                functools.partial(_layer, l, last), out_shape=outs, in_specs=specs, out_specs=out_specs,
                scratch_shapes=sc, compiler_params=cparams(1 + l, mib), name='layer')(*args)

        ko = vo = None
        for l in range(nl):
            ko, vo, op = attn(l, qkv, kb, vb, ko, vo)
            if l < nl - 1:
                h, qkv, kb, vb = layer(l, op, h, False)
            else:
                y = layer(l, op, h, True)
        return y, ko, vo

    return jax.shard_map(
        local, mesh=mesh,
        in_specs=(P('dp', None), P('dp'), P(), P(), P(), P(None, 'sp', None), P(None, None, 'sp'),
                  P(None, 'sp', None), P(), P(), kspec, kspec),
        out_specs=(P('dp', None), kspec, kspec), check_vma=False)
```

```python
import functools

import jax
import jax.numpy as jnp
from jax import lax
from jax.experimental import pallas as pl
from jax.experimental.pallas import tpu as pltpu
from jax.sharding import PartitionSpec as P

EPS = 1e-6
LOG2E = 1.4426950408889634
MESH = pl.DeviceIdType.MESH
VM = pl.BlockSpec(memory_space=pltpu.VMEM)
ANY = pl.BlockSpec(memory_space=pltpu.HBM)
SM = pl.BlockSpec(memory_space=pltpu.SMEM)
F32, BF16 = jnp.float32, jnp.bfloat16
CH = 128
NB = 512
LM = 39


def _rms(h, g):
    r = lax.rsqrt(jnp.mean(h * h, axis=-1, keepdims=True) + EPS)
    return (h * r * g.astype(F32)).astype(BF16)


def _gelu(z):
    return 0.5 * z * (1.0 + jnp.tanh(0.7978845608028654 * (z + 0.044715 * z * z * z)))


def _dot(a, w):
    return jnp.dot(a, w, preferred_element_type=F32)


def _ids():
    dp, sp = lax.axis_index('dp'), lax.axis_index('sp')
    return dp, sp, lax.rem(sp, 2), dp * 4 + sp


def _hello(me):
    sem = pltpu.get_barrier_semaphore()
    for k in range(1, 8):
        d = lax.rem(me + k, 8)
        pl.semaphore_signal(sem, inc=1, device_id=(d // 4, lax.rem(d, 4)), device_id_type=MESH)


def _barrier():
    pl.semaphore_wait(pltpu.get_barrier_semaphore(), 7)


def _exchange(dp, sp, c, src, dst, ssem, rsem):
    x = sp // 2
    devs = [(1 - dp, (1 - x) * 2 + 1 - c), (1 - dp, (1 - x) * 2 + c), (1 - dp, x * 2 + 1 - c), (1 - dp, sp),
            (dp, (1 - x) * 2 + 1 - c), (dp, (1 - x) * 2 + c), (dp, sp + 1 - 2 * c)]
    out = []
    for k, dev in enumerate(devs):
        cp = pltpu.make_async_remote_copy(src(*dev), dst, ssem.at[k], rsem.at[k], device_id=dev, device_id_type=MESH)
        cp.start()
        out.append(cp)
    return out


def _qkv_copies(l, me, ws, wbuf, wsem, slot, s0):
    out = []
    for i in range(3):
        for kh in range(2):
            n = 2 * i + kh
            out.append(pltpu.make_async_copy(
                ws[i].at[l, pl.ds(kh * 2048, 2048), pl.ds(pl.multiple_of(me * NB, NB), NB)],
                wbuf.at[slot + n], wsem.at[s0 + n]))
    return out


def _half_cols(t, q, c):
    half = (1 - c) if t < 2 else c
    return half * 2048 + q * 1024 + (t % 2) * NB


def _mlp_copies(l, dp, c, wo, w1, w2, wbuf, wsem):
    out = []
    for t in range(4):
        for q in range(2):
            n = 2 * t + q
            col = pl.multiple_of(_half_cols(t, q, c), NB)
            out.append(pltpu.make_async_copy(
                wo.at[l, pl.ds(pl.multiple_of(dp * 512, 512), 512), pl.ds(col, NB)],
                wbuf.at[n // 4, pl.ds((n % 4) * 512, 512)], wsem.at[n]))
    for j in range(4):
        for kh in range(2):
            n = 2 * j + kh
            out.append(pltpu.make_async_copy(
                w1.at[l, pl.ds(kh * 2048, 2048), pl.ds(pl.multiple_of(dp * 2048 + j * NB, NB), NB)],
                wbuf.at[2 + n], wsem.at[8 + n]))
    for t in range(4):
        for q in range(2):
            n = 2 * t + q
            col = pl.multiple_of(_half_cols(t, q, c), NB)
            out.append(pltpu.make_async_copy(
                w2.at[l, pl.ds(pl.multiple_of(dp * 2048, 2048), 2048), pl.ds(col, NB)],
                wbuf.at[10 + n], wsem.at[16 + n]))
    return out


def _allreduce(block, dp, sp, c, buf, sems, h_ref):
    psend, pown, precv, chips, tot = buf
    s1, r1, s2, r2, s3, r3 = sems
    x = sp // 2
    partner = (dp, sp + 1 - 2 * c)
    chip = dp * 2 + x
    devs = ((1 - dp, (1 - x) * 2 + c), (1 - dp, sp), (dp, (1 - x) * 2 + c))

    def both(t):
        return jnp.concatenate([block(t, 0)[0:4], block(t, 1)[0:4]], axis=0)

    def copy(src, dst, ss, rs, dev):
        return pltpu.make_async_remote_copy(src, dst, ss, rs, device_id=dev, device_id_type=MESH)

    one = [copy(psend.at[t], precv.at[t], s1.at[t], r1.at[t], partner) for t in range(2)]
    two = [[copy(chips.at[chip, t], chips.at[chip, t], s2.at[t, k], r2.at[t, k], dev)
            for k, dev in enumerate(devs)] for t in range(2)]
    three = [copy(tot.at[c, t], tot.at[c, t], s3.at[t], r3.at[t], partner) for t in range(2)]
    for t in range(2):
        psend[t] = both(t)
        one[t].start()
    for t in range(2):
        pown[t] = both(2 + t)
        one[t].wait()
        chips[chip, t] = pown[t] + precv[t]
        for cp in two[t]:
            cp.start()
    for t in range(2):
        for cp in two[t]:
            cp.wait()
        tot[c, t] = ((chips[0, t] + chips[1, t]) + chips[2, t]) + chips[3, t]
        three[t].start()
    def add(half, t):
        for q in range(2):
            cols = pl.ds(pl.multiple_of(half * 2048 + q * 1024 + t * NB, NB), NB)
            h_ref[0:4, cols] += tot[half, t, q * 4:q * 4 + 4, :]

    for t in range(2):
        add(c, t)
    for t in range(2):
        three[t].wait()
        add(1 - c, t)


def _qkv_stage(chase, dp, sp, c, me, xn, wbuf, copies, slot, sendA, recvA, ssem, rsem, qkv_ref):
    res = []
    step = 2 if chase else 6
    for i in range(3):
        if 2 * i % step == 0:
            for cp in copies[2 * i:2 * i + step]:
                cp.wait()
        z = _dot(xn[:, :2048], wbuf[slot + 2 * i])
        z = z + _dot(xn[:, 2048:], wbuf[slot + 2 * i + 1])
        res.append(z)
    for g in range(2):
        rows = [r[2 * g:2 * g + 2] for r in res] + [jnp.zeros((2, NB), F32)]
        sendA[g] = jnp.concatenate(rows, axis=0).astype(BF16)
    cps = _exchange(dp, sp, c, lambda p, s: sendA.at[p], recvA.at[me], ssem, rsem)
    recvA[me] = sendA[dp]
    for cp in cps:
        cp.wait()
    qkv_ref[...] = recvA[...]


def _cache_copies(l, kc, vc, kb, vb, sem):
    return [pltpu.make_async_copy(src.at[l, b], dst.at[b], sem.at[i, b])
            for i, (src, dst) in enumerate(((kc, kb), (vc, vb))) for b in range(kb.shape[0])]


def _first(x, wq, wk, wv, g1h, kc, vc, h_ref, qkv_ref, kb, vb,
           wbuf, xm, xo, g1, sendA, recvA, wsem, xs, xr, sa, ra, gs, ks):
    dp, sp, c, me = _ids()
    cq = _qkv_copies(0, me, (wq, wk, wv), wbuf, wsem, 0, 0)
    ck = _cache_copies(0, kc, vc, kb, vb, ks)
    _hello(me)
    cs = [pltpu.make_async_copy(x, xm, gs.at[0]), pltpu.make_async_copy(g1h, g1, gs.at[1])]
    for cp in cs + cq[:1]:
        cp.start()
    for cp in cs:
        cp.wait()
    for cp in cq[1:]:
        cp.start()
    _barrier()
    ex = pltpu.make_async_remote_copy(xm, xo, xs, xr, device_id=(1 - dp, sp), device_id_type=MESH)
    ex.start()
    ex.wait()
    mine, other = xm[...].astype(F32), xo[...].astype(F32)
    h_ref[0:2, :] = jnp.where(dp == 0, mine, other)
    h_ref[2:4, :] = jnp.where(dp == 0, other, mine)
    h_ref[4:8, :] = jnp.zeros((4, h_ref.shape[1]), F32)
    xn = _rms(h_ref[...], g1[0:1, :])
    for cp in ck:
        cp.start()
    _qkv_stage(True, dp, sp, c, me, xn, wbuf, cq, 0, sendA, recvA, sa, ra, qkv_ref)
    for cp in ck:
        cp.wait()


def _layer(l, last, *refs):
    if last:
        (op_ref, hin, wo, w1, w2, g2, y_ref, h_ref, *sc) = refs
    else:
        (op_ref, hin, wo, w1, w2, g2, wq, wk, wv, g1, kc, vc, h_ref, qkv_ref, kb, vb, *sc) = refs
    wbuf, recvB, att, u, psend, pown, precv, chips, tot = sc[:9]
    wsem, sb, rb, s1, r1, s2, r2, s3, r3 = sc[9:18]
    dp, sp, c, me = _ids()
    _hello(me)
    cm = _mlp_copies(l, dp, c, wo, w1, w2, wbuf, wsem)
    ck, cq = [], []
    if not last:
        sendA, recvA, sa, ra, ks = sc[18:]
        cq = _qkv_copies(l + 1, me, (wq, wk, wv), wbuf, wsem, 2, 24)
        ck = _cache_copies(l + 1, kc, vc, kb, vb, ks)
    for cp in cm[:16]:
        cp.start()
    h_ref[...] = hin[...]
    att[...] = jnp.zeros_like(att)
    recvB[me] = op_ref[2 * sp + dp]
    _barrier()
    cps = _exchange(dp, sp, c, lambda p, s: op_ref.at[2 * s + p], recvB.at[me], sb, rb)
    for cp in cps:
        cp.wait()
    for cp in cm[16:]:
        cp.start()
    for g in range(2):
        ms = [recvB[4 * g + i, 1][:, 0:1] for i in range(4)]
        m = functools.reduce(jnp.maximum, ms)
        o = jnp.zeros((8, 128), F32)
        den = jnp.zeros((8, 1), F32)
        for i in range(4):
            e = jnp.exp2(ms[i] - m)
            o = o + recvB[4 * g + i, 0] * e
            den = den + recvB[4 * g + i, 1][:, 64:65] * e
        a = o / den
        for b in range(2):
            for j in range(4):
                att[2 * g + b:2 * g + b + 1, j * 128:(j + 1) * 128] = a[4 * b + j:4 * b + j + 1]
    av = att[...].astype(BF16)
    for cp in cm[:8]:
        cp.wait()

    def wo_block(t, q):
        n = 2 * t + q
        return _dot(av, wbuf[n // 4, (n % 4) * 512:(n % 4) * 512 + 512, :])

    def bufs(i):
        return [psend.at[i], pown.at[i], precv.at[i], chips.at[i], tot.at[i]]

    def sems(i):
        return [s1.at[i], r1.at[i], s2.at[i], r2.at[i], s3.at[i], r3.at[i]]

    _allreduce(wo_block, dp, sp, c, bufs(0), sems(0), h_ref)
    for cp in ck:
        cp.start()
    xn = _rms(h_ref[...], g2[l:l + 1, :])
    for cp in cm[8:16]:
        cp.wait()
    for j in range(4):
        z = _dot(xn[:, :2048], wbuf[2 + 2 * j])
        z = z + _dot(xn[:, 2048:], wbuf[3 + 2 * j])
        u[:, j * NB:(j + 1) * NB] = _gelu(z).astype(BF16)
    uv = u[...]
    for cp in cm[16:]:
        cp.wait()
    for cp in cq:
        cp.start()

    def w2_block(t, q):
        n = 2 * t + q
        return _dot(uv, wbuf[10 + n])

    _allreduce(w2_block, dp, sp, c, bufs(1), sems(1), h_ref)
    if last:
        hv = h_ref[...]
        y_ref[...] = jnp.where(dp == 0, hv[0:2], hv[2:4]).astype(BF16)
    else:
        xn = _rms(h_ref[...], g1[l + 1:l + 2, :])
        _qkv_stage(False, dp, sp, c, me, xn, wbuf, cq, 2, sendA, recvA, sa, ra, qkv_ref)
        for cp in ck:
            cp.wait()


def _attn(l, *refs):
    if l == 0:
        lensh, qkv, kin, vin, ko, vo, op_ref, kb, vb, *sc = refs
    else:
        lensh, qkv, kin, vin, _, _, ko, vo, op_ref, kb, vb, *sc = refs
    tr, q_ref, s_ref, m_ref, l_ref, o_ref, kos, vos = sc
    nb, npos, nh, dh = kb.shape
    per = npos // CH
    n = nb * per
    base = lax.axis_index('sp') * npos
    lv = lensh[...]
    lens = [jnp.max(lv[:, b:b + 1]) for b in range(nb)]

    def wr(dst, buf, sem, i):
        b, p = i // per, pl.multiple_of(lax.rem(i, per) * CH, CH)
        return pltpu.make_async_copy(buf.at[b, pl.ds(p, CH)], dst.at[l, b, pl.ds(p, CH)], sem.at[i])

    for src in range(8):
        v = qkv[src].astype(F32)
        for j in range(4):
            tr[src * 4 + j] = v[:, j * dh:(j + 1) * dh]
    m_ref[...] = jnp.full(m_ref.shape, -jnp.inf, F32)
    l_ref[...] = jnp.zeros_like(l_ref)
    o_ref[...] = jnp.zeros_like(o_ref)
    z = jnp.zeros((nh, dh), BF16)
    for b in range(nb):
        q = tr[:, b, :].astype(BF16)
        q_ref[b, 0:nh] = jnp.concatenate([q, z], axis=1)
        q_ref[b, nh:2 * nh] = jnp.concatenate([z, q], axis=1)
    for b in range(nb):
        lp = lens[b] - 1 - base

        @pl.when((lp >= 0) & (lp < npos))
        def _():
            kb[b, lp] = tr[:, 2 + b, :].astype(BF16)
            vb[b, lp] = tr[:, 4 + b, :].astype(BF16)

    hc = CH * nh // 2
    sl = lax.broadcasted_iota(jnp.int32, (8, dh), 0)
    ln = lax.broadcasted_iota(jnp.int32, (8, dh), 1)
    tile = lambda v: jnp.concatenate([v] * (hc // dh), axis=1)
    diag = tile(lax.rem(ln, nh) - sl)
    group = tile(lax.rem(ln, nh) // 8)
    col = lax.broadcasted_iota(jnp.int32, (8, hc), 1)
    ng = nh // 8
    sc = dh ** -0.5 * LOG2E

    def heads(v, op):
        k = nh
        while k < dh:
            v = op(v, pltpu.roll(v, k, 1))
            k *= 2
        return v

    def column(v, fill, op):
        return jnp.concatenate([op(jnp.where(ln == sl + 8 * r, v, fill), axis=1, keepdims=True)
                                for r in range(ng)], axis=0)

    def pair(buf, b, p0):
        return jnp.concatenate([buf[b, pl.ds(p0, CH // 2)].reshape(hc, dh),
                                buf[b, pl.ds(p0 + CH // 2, CH // 2)].reshape(hc, dh)], axis=1)

    for i in range(n):
        wr(ko, kb, kos, i).start()
        wr(vo, vb, vos, i).start()

    def pick(b):
        return functools.reduce(lambda v, i: jnp.where(b == i, lens[i], v), range(1, nb), lens[0])

    def kstep(b, _):
        m = m_ref[b]
        for j in range(per):
            s = lax.dot_general(q_ref[b], pair(kb, b, j * CH), (((1,), (1,)), ((), ())),
                                preferred_element_type=F32)
            lim = (pick(b) - base - j * CH) * nh
            for half in range(2):
                v = functools.reduce(jnp.maximum, [
                    jnp.where(diag == 8 * r, s[half * nh + 8 * r:half * nh + 8 * r + 8], -jnp.inf) for r in range(ng)])
                v = jnp.where(col < lim - half * hc, v, -jnp.inf)
                s_ref[b * per + j, half] = v
                for k in range(0, hc, dh):
                    m = jnp.maximum(m, v[:, k:k + dh])
        m_ref[b] = heads(m, jnp.maximum)
        return 0

    def vstep(b, _):
        m = m_ref[b]
        m = tile(jnp.where(m == -jnp.inf, 0.0, m))
        lt, ot = l_ref[b], o_ref[b]
        for j in range(per):
            rows = []
            for half in range(2):
                p = jnp.exp2((s_ref[b * per + j, half] - m) * sc)
                for k in range(0, hc, dh):
                    lt = lt + p[:, k:k + dh]
                rows += [jnp.where(group == r, p, 0.0) for r in range(ng)]
            ot = ot + _dot(jnp.concatenate(rows, axis=0).astype(BF16), pair(vb, b, j * CH))
        l_ref[b] = heads(lt, jnp.add)
        o_ref[b] = ot
        return 0

    lax.fori_loop(0, nb, kstep, 0)
    lax.fori_loop(0, nb, vstep, 0)
    lane = lax.broadcasted_iota(jnp.int32, (nh, dh), 1)
    for b in range(nb):
        ov = o_ref[b, 0:nh, 0:dh] + o_ref[b, nh:2 * nh, dh:2 * dh]
        mc = column(m_ref[b], -jnp.inf, jnp.max) * sc
        ml = jnp.where(lane < 64, mc, column(l_ref[b], 0.0, jnp.sum))
        for r in range(8):
            op_ref[r, 0, b * 4:b * 4 + 4, :] = ov[4 * r:4 * r + 4]
            op_ref[r, 1, b * 4:b * 4 + 4, :] = ml[4 * r:4 * r + 4]
    for i in range(n):
        wr(ko, kb, kos, i).wait()
        wr(vo, vb, vos, i).wait()


def solution(mesh):
    kspec = P(None, 'dp', 'sp', None, None)
    DMA = pltpu.SemaphoreType.DMA

    def local(x, lens, wq, wk, wv, wo, w1, w2, g1, g2, kc, vc):
        nl, nb, npos, nh, dh = kc.shape
        d = x.shape[1]
        V = lambda *sh_dt: pltpu.VMEM(*sh_dt)
        hbm = lambda *xs: [pltpu.with_memory_space_constraint(a, pltpu.HBM) for a in xs]
        vm = lambda *xs: [pltpu.with_memory_space_constraint(a, pltpu.VMEM) for a in xs]
        h_sh, qkv_sh = V((8, d), F32), V((8, 8, NB), BF16)
        c_vm = V((nb, npos, nh, dh), BF16)
        qkv_sc = [V((2, 8, NB), BF16), V((8, 8, NB), BF16)]
        cparams = lambda i, mib: pltpu.CompilerParams(
            collective_id=i, has_side_effects=True, vmem_limit_bytes=mib * 2 ** 20)

        h, qkv, kb, vb = pl.pallas_call(
            _first, out_shape=(h_sh, qkv_sh, c_vm, c_vm),
            in_specs=[ANY] * 7, out_specs=(VM,) * 4,
            scratch_shapes=[V((6, 2048, NB), BF16), V((2, d), BF16), V((2, d), BF16), V((nl, d), BF16), *qkv_sc,
                            DMA((6,)), DMA, DMA, DMA((8,)), DMA((8,)), DMA((2,)), DMA((2, nb))],
            compiler_params=cparams(0, 16), name='first')(*hbm(x, wq, wk, wv, g1, kc, vc))

        def attn(l, qkv, kb, vb, ko, vo):
            n = nb * npos // CH
            c_sh = jax.ShapeDtypeStruct(kc.shape, kc.dtype)
            args = vm(lens.reshape(1, nb), qkv, kb, vb) + ([] if l == 0 else hbm(ko, vo))
            al = {2: 3, 3: 4}
            if l > 0:
                al.update({4: 0, 5: 1})
            return pl.pallas_call(
                functools.partial(_attn, l),
                out_shape=(c_sh, c_sh, V((8, 2, 8, dh), F32), c_vm, c_vm),
                in_specs=[VM, VM, VM, VM] + ([] if l == 0 else [ANY, ANY]),
                out_specs=(ANY, ANY, VM, VM, VM),
                scratch_shapes=[V((nh, 8, dh), F32), V((nb, 2 * nh, 2 * dh), BF16),
                                V((n, 2, 8, CH * nh // 2), F32), V((nb, 8, dh), F32),
                                V((nb, 8, dh), F32), V((nb, 2 * nh, 2 * dh), F32),
                                DMA((n,)), DMA((n,))],
                input_output_aliases=al,
                compiler_params=pltpu.CompilerParams(vmem_limit_bytes=14 * 2 ** 20), name='attn')(*args)[:3]

        def layer(l, op, h, last):
            sc = [V((18, 2048, NB), BF16), V((8, 2, 8, dh), F32),
                  V((8, 512), F32), V((8, 2048), BF16),
                  V((2, 2, 8, NB), F32), V((2, 2, 8, NB), F32), V((2, 2, 8, NB), F32),
                  V((2, 4, 2, 8, NB), F32), V((2, 2, 2, 8, NB), F32),
                  DMA((30,)), DMA((8,)), DMA((8,)),
                  DMA((2, 2)), DMA((2, 2)), DMA((2, 2, 3)), DMA((2, 2, 3)), DMA((2, 2)), DMA((2, 2))]
            args = vm(op, h) + hbm(wo, w1, w2) + vm(g2)
            specs = [VM, VM, ANY, ANY, ANY, VM]
            if last:
                sc = [V((8, d), F32)] + sc
                outs, out_specs, mib = jax.ShapeDtypeStruct((nb, d), BF16), VM, 39
            else:
                args += hbm(wq, wk, wv) + vm(g1) + hbm(kc, vc)
                specs += [ANY, ANY, ANY, VM, ANY, ANY]
                sc += [*qkv_sc, DMA((8,)), DMA((8,)), DMA((2, nb))]
                outs, out_specs, mib = (h_sh, qkv_sh, c_vm, c_vm), (VM,) * 4, LM
            return pl.pallas_call(
                functools.partial(_layer, l, last), out_shape=outs, in_specs=specs, out_specs=out_specs,
                scratch_shapes=sc, compiler_params=cparams(1 + l, mib), name='layer')(*args)

        ko = vo = None
        for l in range(nl):
            ko, vo, op = attn(l, qkv, kb, vb, ko, vo)
            if l < nl - 1:
                h, qkv, kb, vb = layer(l, op, h, False)
            else:
                y = layer(l, op, h, True)
        return y, ko, vo

    return jax.shard_map(
        local, mesh=mesh,
        in_specs=(P('dp', None), P('dp'), P(), P(), P(), P(None, 'sp', None), P(None, None, 'sp'),
                  P(None, 'sp', None), P(), P(), kspec, kspec),
        out_specs=(P('dp', None), kspec, kspec), check_vma=False)
```

```python
import functools

import jax
import jax.numpy as jnp
from jax import lax
from jax.experimental import pallas as pl
from jax.experimental.pallas import tpu as pltpu
from jax.sharding import PartitionSpec as P

EPS = 1e-6
LOG2E = 1.4426950408889634
MESH = pl.DeviceIdType.MESH
VM = pl.BlockSpec(memory_space=pltpu.VMEM)
ANY = pl.BlockSpec(memory_space=pltpu.HBM)
SM = pl.BlockSpec(memory_space=pltpu.SMEM)
F32, BF16 = jnp.float32, jnp.bfloat16
CH = 128
NB = 512
LATE = 256
LM = 39


def _rms(h, g):
    r = lax.rsqrt(jnp.mean(h * h, axis=-1, keepdims=True) + EPS)
    return (h * r * g.astype(F32)).astype(BF16)


def _gelu(z):
    return 0.5 * z * (1.0 + jnp.tanh(0.7978845608028654 * (z + 0.044715 * z * z * z)))


def _dot(a, w):
    return jnp.dot(a, w, preferred_element_type=F32)


def _ids():
    dp, sp = lax.axis_index('dp'), lax.axis_index('sp')
    return dp, sp, lax.rem(sp, 2), dp * 4 + sp


def _hello(me):
    sem = pltpu.get_barrier_semaphore()
    for k in range(1, 8):
        d = lax.rem(me + k, 8)
        pl.semaphore_signal(sem, inc=1, device_id=(d // 4, lax.rem(d, 4)), device_id_type=MESH)


def _barrier():
    pl.semaphore_wait(pltpu.get_barrier_semaphore(), 7)


def _exchange(dp, sp, c, src, dst, ssem, rsem):
    x = sp // 2
    devs = [(1 - dp, (1 - x) * 2 + 1 - c), (1 - dp, (1 - x) * 2 + c), (1 - dp, x * 2 + 1 - c), (1 - dp, sp),
            (dp, (1 - x) * 2 + 1 - c), (dp, (1 - x) * 2 + c), (dp, sp + 1 - 2 * c)]
    out = []
    for k, dev in enumerate(devs):
        cp = pltpu.make_async_remote_copy(src(*dev), dst, ssem.at[k], rsem.at[k], device_id=dev, device_id_type=MESH)
        cp.start()
        out.append(cp)
    return out


def _qkv_copies(l, me, ws, wbuf, wsem, slot, s0):
    out = []
    for i in range(3):
        for kh in range(2):
            n = 2 * i + kh
            out.append(pltpu.make_async_copy(
                ws[i].at[l, pl.ds(kh * 2048, 2048), pl.ds(pl.multiple_of(me * NB, NB), NB)],
                wbuf.at[slot + n], wsem.at[s0 + n]))
    return out


def _half_cols(t, q, c):
    half = (1 - c) if t < 2 else c
    return half * 2048 + q * 1024 + (t % 2) * NB


def _mlp_copies(l, dp, c, wo, w1, w2, wbuf, wsem):
    out = []
    for t in range(4):
        for q in range(2):
            n = 2 * t + q
            col = pl.multiple_of(_half_cols(t, q, c), NB)
            out.append(pltpu.make_async_copy(
                wo.at[l, pl.ds(pl.multiple_of(dp * 512, 512), 512), pl.ds(col, NB)],
                wbuf.at[n // 4, pl.ds((n % 4) * 512, 512)], wsem.at[n]))
    for j in range(4):
        for kh in range(2):
            n = 2 * j + kh
            out.append(pltpu.make_async_copy(
                w1.at[l, pl.ds(kh * 2048, 2048), pl.ds(pl.multiple_of(dp * 2048 + j * NB, NB), NB)],
                wbuf.at[2 + n], wsem.at[8 + n]))
    for t in range(4):
        for q in range(2):
            n = 2 * t + q
            col = pl.multiple_of(_half_cols(t, q, c), NB)
            out.append(pltpu.make_async_copy(
                w2.at[l, pl.ds(pl.multiple_of(dp * 2048, 2048), 2048), pl.ds(col, NB)],
                wbuf.at[10 + n], wsem.at[16 + n]))
    return out


def _allreduce(block, dp, sp, c, buf, sems, h_ref):
    psend, pown, precv, chips, tot = buf
    s1, r1, s2, r2, s3, r3 = sems
    x = sp // 2
    partner = (dp, sp + 1 - 2 * c)
    chip = dp * 2 + x
    devs = ((1 - dp, (1 - x) * 2 + c), (1 - dp, sp), (dp, (1 - x) * 2 + c))

    def both(t):
        return jnp.concatenate([block(t, 0)[0:4], block(t, 1)[0:4]], axis=0)

    def copy(src, dst, ss, rs, dev):
        return pltpu.make_async_remote_copy(src, dst, ss, rs, device_id=dev, device_id_type=MESH)

    one = [copy(psend.at[t], precv.at[t], s1.at[t], r1.at[t], partner) for t in range(2)]
    two = [[copy(chips.at[chip, t], chips.at[chip, t], s2.at[t, k], r2.at[t, k], dev)
            for k, dev in enumerate(devs)] for t in range(2)]
    three = [copy(tot.at[c, t], tot.at[c, t], s3.at[t], r3.at[t], partner) for t in range(2)]
    for t in range(2):
        psend[t] = both(t)
        one[t].start()
    for t in range(2):
        pown[t] = both(2 + t)
        one[t].wait()
        chips[chip, t] = pown[t] + precv[t]
        for cp in two[t]:
            cp.start()
    for t in range(2):
        for cp in two[t]:
            cp.wait()
        tot[c, t] = ((chips[0, t] + chips[1, t]) + chips[2, t]) + chips[3, t]
        three[t].start()
    def add(half, t):
        for q in range(2):
            cols = pl.ds(pl.multiple_of(half * 2048 + q * 1024 + t * NB, NB), NB)
            h_ref[0:4, cols] += tot[half, t, q * 4:q * 4 + 4, :]

    for t in range(2):
        add(c, t)
    for t in range(2):
        three[t].wait()
        add(1 - c, t)


def _qkv_stage(chase, dp, sp, c, me, xn, wbuf, copies, slot, sendA, recvA, ssem, rsem, qkv_ref):
    res = []
    step = 2 if chase else 6
    for i in range(3):
        if 2 * i % step == 0:
            for cp in copies[2 * i:2 * i + step]:
                cp.wait()
        z = _dot(xn[:, :2048], wbuf[slot + 2 * i])
        z = z + _dot(xn[:, 2048:], wbuf[slot + 2 * i + 1])
        res.append(z)
    for g in range(2):
        rows = [r[2 * g:2 * g + 2] for r in res] + [jnp.zeros((2, NB), F32)]
        sendA[g] = jnp.concatenate(rows, axis=0).astype(BF16)
    cps = _exchange(dp, sp, c, lambda p, s: sendA.at[p], recvA.at[me], ssem, rsem)
    recvA[me] = sendA[dp]
    for cp in cps:
        cp.wait()
    qkv_ref[...] = recvA[...]


def _cache_copies(l, kc, vc, kb, vb, sem, late=0):
    nb, npos = kb.shape[:2]
    out = []
    for i, (src, dst) in enumerate(((kc, kb), (vc, vb))):
        for b in range(nb):
            n = npos - (late if i == 1 and b == nb - 1 else 0)
            out.append(pltpu.make_async_copy(src.at[l, b, pl.ds(0, n)], dst.at[b, pl.ds(0, n)], sem.at[i, b]))
    return out


def _first(x, wq, wk, wv, g1h, kc, vc, h_ref, qkv_ref, kb, vb,
           wbuf, xm, xo, g1, sendA, recvA, wsem, xs, xr, sa, ra, gs, ks):
    dp, sp, c, me = _ids()
    cq = _qkv_copies(0, me, (wq, wk, wv), wbuf, wsem, 0, 0)
    ck = _cache_copies(0, kc, vc, kb, vb, ks, LATE)
    _hello(me)
    cs = [pltpu.make_async_copy(x, xm, gs.at[0]), pltpu.make_async_copy(g1h, g1, gs.at[1])]
    for cp in cs + cq[:1]:
        cp.start()
    for cp in cs:
        cp.wait()
    for cp in cq[1:]:
        cp.start()
    _barrier()
    ex = pltpu.make_async_remote_copy(xm, xo, xs, xr, device_id=(1 - dp, sp), device_id_type=MESH)
    ex.start()
    ex.wait()
    mine, other = xm[...].astype(F32), xo[...].astype(F32)
    h_ref[0:2, :] = jnp.where(dp == 0, mine, other)
    h_ref[2:4, :] = jnp.where(dp == 0, other, mine)
    h_ref[4:8, :] = jnp.zeros((4, h_ref.shape[1]), F32)
    xn = _rms(h_ref[...], g1[0:1, :])
    for cp in ck:
        cp.start()
    _qkv_stage(True, dp, sp, c, me, xn, wbuf, cq, 0, sendA, recvA, sa, ra, qkv_ref)
    for cp in ck:
        cp.wait()


def _layer(l, last, *refs):
    if last:
        (op_ref, hin, wo, w1, w2, g2, y_ref, h_ref, *sc) = refs
    else:
        (op_ref, hin, wo, w1, w2, g2, wq, wk, wv, g1, kc, vc, h_ref, qkv_ref, kb, vb, *sc) = refs
    wbuf, recvB, att, u, psend, pown, precv, chips, tot = sc[:9]
    wsem, sb, rb, s1, r1, s2, r2, s3, r3 = sc[9:18]
    dp, sp, c, me = _ids()
    _hello(me)
    cm = _mlp_copies(l, dp, c, wo, w1, w2, wbuf, wsem)
    ck, cq = [], []
    if not last:
        sendA, recvA, sa, ra, ks = sc[18:]
        cq = _qkv_copies(l + 1, me, (wq, wk, wv), wbuf, wsem, 2, 24)
        ck = _cache_copies(l + 1, kc, vc, kb, vb, ks)
    for cp in cm[:16]:
        cp.start()
    h_ref[...] = hin[...]
    att[...] = jnp.zeros_like(att)
    recvB[me] = op_ref[2 * sp + dp]
    _barrier()
    cps = _exchange(dp, sp, c, lambda p, s: op_ref.at[2 * s + p], recvB.at[me], sb, rb)
    for cp in cps:
        cp.wait()
    for cp in cm[16:]:
        cp.start()
    for g in range(2):
        ms = [recvB[4 * g + i, 1][:, 0:1] for i in range(4)]
        m = functools.reduce(jnp.maximum, ms)
        o = jnp.zeros((8, 128), F32)
        den = jnp.zeros((8, 1), F32)
        for i in range(4):
            e = jnp.exp2(ms[i] - m)
            o = o + recvB[4 * g + i, 0] * e
            den = den + recvB[4 * g + i, 1][:, 64:65] * e
        a = o / den
        for b in range(2):
            for j in range(4):
                att[2 * g + b:2 * g + b + 1, j * 128:(j + 1) * 128] = a[4 * b + j:4 * b + j + 1]
    av = att[...].astype(BF16)
    for cp in cm[:8]:
        cp.wait()

    def wo_block(t, q):
        n = 2 * t + q
        return _dot(av, wbuf[n // 4, (n % 4) * 512:(n % 4) * 512 + 512, :])

    def bufs(i):
        return [psend.at[i], pown.at[i], precv.at[i], chips.at[i], tot.at[i]]

    def sems(i):
        return [s1.at[i], r1.at[i], s2.at[i], r2.at[i], s3.at[i], r3.at[i]]

    _allreduce(wo_block, dp, sp, c, bufs(0), sems(0), h_ref)
    for cp in ck:
        cp.start()
    xn = _rms(h_ref[...], g2[l:l + 1, :])
    for cp in cm[8:16]:
        cp.wait()
    for j in range(4):
        z = _dot(xn[:, :2048], wbuf[2 + 2 * j])
        z = z + _dot(xn[:, 2048:], wbuf[3 + 2 * j])
        u[:, j * NB:(j + 1) * NB] = _gelu(z).astype(BF16)
    uv = u[...]
    for cp in cm[16:]:
        cp.wait()
    for cp in cq:
        cp.start()

    def w2_block(t, q):
        n = 2 * t + q
        return _dot(uv, wbuf[10 + n])

    _allreduce(w2_block, dp, sp, c, bufs(1), sems(1), h_ref)
    if last:
        hv = h_ref[...]
        y_ref[...] = jnp.where(dp == 0, hv[0:2], hv[2:4]).astype(BF16)
    else:
        xn = _rms(h_ref[...], g1[l + 1:l + 2, :])
        _qkv_stage(False, dp, sp, c, me, xn, wbuf, cq, 2, sendA, recvA, sa, ra, qkv_ref)
        for cp in ck:
            cp.wait()


def _attn(l, *refs):
    if l == 0:
        lensh, qkv, kin, vin, vc, ko, vo, op_ref, kb, vb, *sc = refs
    else:
        lensh, qkv, kin, vin, _, _, ko, vo, op_ref, kb, vb, *sc = refs
    tr, q_ref, s_ref, m_ref, l_ref, o_ref, kos, vos, ls = sc
    nb, npos, nh, dh = kb.shape
    per = npos // CH
    n = nb * per
    base = lax.axis_index('sp') * npos
    nlast = npos - LATE
    if l == 0:
        late = pltpu.make_async_copy(vc.at[l, nb - 1, pl.ds(nlast, LATE)], vb.at[nb - 1, pl.ds(nlast, LATE)], ls)
        late.start()
    lv = lensh[...]
    lens = [jnp.max(lv[:, b:b + 1]) for b in range(nb)]

    def wr(dst, buf, sem, i):
        b, p = i // per, pl.multiple_of(lax.rem(i, per) * CH, CH)
        return pltpu.make_async_copy(buf.at[b, pl.ds(p, CH)], dst.at[l, b, pl.ds(p, CH)], sem.at[i])

    for src in range(8):
        v = qkv[src].astype(F32)
        for j in range(4):
            tr[src * 4 + j] = v[:, j * dh:(j + 1) * dh]
    m_ref[...] = jnp.full(m_ref.shape, -jnp.inf, F32)
    l_ref[...] = jnp.zeros_like(l_ref)
    o_ref[...] = jnp.zeros_like(o_ref)
    def patch(buf, row, b):
        lp = lens[b] - 1 - base

        @pl.when((lp >= 0) & (lp < npos))
        def _():
            buf[b, lp] = tr[:, row + b, :].astype(BF16)

    for b in range(nb):
        patch(kb, 2, b)
    for b in range(nb - 1):
        patch(vb, 4, b)
    z = jnp.zeros((nh, dh), BF16)
    for b in range(nb):
        q = tr[:, b, :].astype(BF16)
        q_ref[b, 0:nh] = jnp.concatenate([q, z], axis=1)
        q_ref[b, nh:2 * nh] = jnp.concatenate([z, q], axis=1)
    hc = CH * nh // 2
    sl = lax.broadcasted_iota(jnp.int32, (8, dh), 0)
    ln = lax.broadcasted_iota(jnp.int32, (8, dh), 1)
    tile = lambda v: jnp.concatenate([v] * (hc // dh), axis=1)
    diag = tile(lax.rem(ln, nh) - sl)
    group = tile(lax.rem(ln, nh) // 8)
    col = lax.broadcasted_iota(jnp.int32, (8, hc), 1)
    ng = nh // 8
    sc = dh ** -0.5 * LOG2E

    def heads(v, op):
        k = nh
        while k < dh:
            v = op(v, pltpu.roll(v, k, 1))
            k *= 2
        return v

    def column(v, fill, op):
        return jnp.concatenate([op(jnp.where(ln == sl + 8 * r, v, fill), axis=1, keepdims=True)
                                for r in range(ng)], axis=0)

    def pair(buf, b, p0):
        return jnp.concatenate([buf[b, pl.ds(p0, CH // 2)].reshape(hc, dh),
                                buf[b, pl.ds(p0 + CH // 2, CH // 2)].reshape(hc, dh)], axis=1)

    for i in range(n):
        wr(ko, kb, kos, i).start()
    for i in range(n - per):
        wr(vo, vb, vos, i).start()

    def pick(b):
        return functools.reduce(lambda v, i: jnp.where(b == i, lens[i], v), range(1, nb), lens[0])

    def kstep(b, _):
        m = m_ref[b]
        for j in range(per):
            s = lax.dot_general(q_ref[b], pair(kb, b, j * CH), (((1,), (1,)), ((), ())),
                                preferred_element_type=F32)
            lim = (pick(b) - base - j * CH) * nh
            for half in range(2):
                v = functools.reduce(jnp.maximum, [
                    jnp.where(diag == 8 * r, s[half * nh + 8 * r:half * nh + 8 * r + 8], -jnp.inf) for r in range(ng)])
                v = jnp.where(col < lim - half * hc, v, -jnp.inf)
                s_ref[b * per + j, half] = v
                for k in range(0, hc, dh):
                    m = jnp.maximum(m, v[:, k:k + dh])
        m_ref[b] = heads(m, jnp.maximum)
        return 0

    def vstep(b, _):
        m = m_ref[b]
        m = tile(jnp.where(m == -jnp.inf, 0.0, m))
        lt, ot = l_ref[b], o_ref[b]
        for j in range(per):
            rows = []
            for half in range(2):
                p = jnp.exp2((s_ref[b * per + j, half] - m) * sc)
                for k in range(0, hc, dh):
                    lt = lt + p[:, k:k + dh]
                rows += [jnp.where(group == r, p, 0.0) for r in range(ng)]
            ot = ot + _dot(jnp.concatenate(rows, axis=0).astype(BF16), pair(vb, b, j * CH))
        l_ref[b] = heads(lt, jnp.add)
        o_ref[b] = ot
        return 0

    lax.fori_loop(0, nb, kstep, 0)
    if l == 0:
        late.wait()
    patch(vb, 4, nb - 1)
    mc = [column(m_ref[b], -jnp.inf, jnp.max) * sc for b in range(nb)]
    for i in range(n - per, n):
        wr(vo, vb, vos, i).start()
    lax.fori_loop(0, nb, vstep, 0)
    lane = lax.broadcasted_iota(jnp.int32, (nh, dh), 1)
    for b in range(nb):
        ov = o_ref[b, 0:nh, 0:dh] + o_ref[b, nh:2 * nh, dh:2 * dh]
        ml = jnp.where(lane < 64, mc[b], column(l_ref[b], 0.0, jnp.sum))
        for r in range(8):
            op_ref[r, 0, b * 4:b * 4 + 4, :] = ov[4 * r:4 * r + 4]
            op_ref[r, 1, b * 4:b * 4 + 4, :] = ml[4 * r:4 * r + 4]
    for i in range(n):
        wr(ko, kb, kos, i).wait()
        wr(vo, vb, vos, i).wait()


def solution(mesh):
    kspec = P(None, 'dp', 'sp', None, None)
    DMA = pltpu.SemaphoreType.DMA

    def local(x, lens, wq, wk, wv, wo, w1, w2, g1, g2, kc, vc):
        nl, nb, npos, nh, dh = kc.shape
        d = x.shape[1]
        V = lambda *sh_dt: pltpu.VMEM(*sh_dt)
        hbm = lambda *xs: [pltpu.with_memory_space_constraint(a, pltpu.HBM) for a in xs]
        vm = lambda *xs: [pltpu.with_memory_space_constraint(a, pltpu.VMEM) for a in xs]
        h_sh, qkv_sh = V((8, d), F32), V((8, 8, NB), BF16)
        c_vm = V((nb, npos, nh, dh), BF16)
        qkv_sc = [V((2, 8, NB), BF16), V((8, 8, NB), BF16)]
        cparams = lambda i, mib: pltpu.CompilerParams(
            collective_id=i, has_side_effects=True, vmem_limit_bytes=mib * 2 ** 20)

        h, qkv, kb, vb = pl.pallas_call(
            _first, out_shape=(h_sh, qkv_sh, c_vm, c_vm),
            in_specs=[ANY] * 7, out_specs=(VM,) * 4,
            scratch_shapes=[V((6, 2048, NB), BF16), V((2, d), BF16), V((2, d), BF16), V((nl, d), BF16), *qkv_sc,
                            DMA((6,)), DMA, DMA, DMA((8,)), DMA((8,)), DMA((2,)), DMA((2, nb))],
            compiler_params=cparams(0, 16), name='first')(*hbm(x, wq, wk, wv, g1, kc, vc))

        def attn(l, qkv, kb, vb, ko, vo):
            n = nb * npos // CH
            c_sh = jax.ShapeDtypeStruct(kc.shape, kc.dtype)
            args = vm(lens.reshape(1, nb), qkv, kb, vb) + (hbm(vc) if l == 0 else hbm(ko, vo))
            al = {2: 3, 3: 4}
            if l > 0:
                al.update({4: 0, 5: 1})
            return pl.pallas_call(
                functools.partial(_attn, l),
                out_shape=(c_sh, c_sh, V((8, 2, 8, dh), F32), c_vm, c_vm),
                in_specs=[VM, VM, VM, VM] + ([ANY] if l == 0 else [ANY, ANY]),
                out_specs=(ANY, ANY, VM, VM, VM),
                scratch_shapes=[V((nh, 8, dh), F32), V((nb, 2 * nh, 2 * dh), BF16),
                                V((n, 2, 8, CH * nh // 2), F32), V((nb, 8, dh), F32),
                                V((nb, 8, dh), F32), V((nb, 2 * nh, 2 * dh), F32),
                                DMA((n,)), DMA((n,)), DMA],
                input_output_aliases=al,
                compiler_params=pltpu.CompilerParams(vmem_limit_bytes=14 * 2 ** 20), name='attn')(*args)[:3]

        def layer(l, op, h, last):
            sc = [V((18, 2048, NB), BF16), V((8, 2, 8, dh), F32),
                  V((8, 512), F32), V((8, 2048), BF16),
                  V((2, 2, 8, NB), F32), V((2, 2, 8, NB), F32), V((2, 2, 8, NB), F32),
                  V((2, 4, 2, 8, NB), F32), V((2, 2, 2, 8, NB), F32),
                  DMA((30,)), DMA((8,)), DMA((8,)),
                  DMA((2, 2)), DMA((2, 2)), DMA((2, 2, 3)), DMA((2, 2, 3)), DMA((2, 2)), DMA((2, 2))]
            args = vm(op, h) + hbm(wo, w1, w2) + vm(g2)
            specs = [VM, VM, ANY, ANY, ANY, VM]
            if last:
                sc = [V((8, d), F32)] + sc
                outs, out_specs, mib = jax.ShapeDtypeStruct((nb, d), BF16), VM, 39
            else:
                args += hbm(wq, wk, wv) + vm(g1) + hbm(kc, vc)
                specs += [ANY, ANY, ANY, VM, ANY, ANY]
                sc += [*qkv_sc, DMA((8,)), DMA((8,)), DMA((2, nb))]
                outs, out_specs, mib = (h_sh, qkv_sh, c_vm, c_vm), (VM,) * 4, LM
            return pl.pallas_call(
                functools.partial(_layer, l, last), out_shape=outs, in_specs=specs, out_specs=out_specs,
                scratch_shapes=sc, compiler_params=cparams(1 + l, mib), name='layer')(*args)

        ko = vo = None
        for l in range(nl):
            ko, vo, op = attn(l, qkv, kb, vb, ko, vo)
            if l < nl - 1:
                h, qkv, kb, vb = layer(l, op, h, False)
            else:
                y = layer(l, op, h, True)
        return y, ko, vo

    return jax.shard_map(
        local, mesh=mesh,
        in_specs=(P('dp', None), P('dp'), P(), P(), P(), P(None, 'sp', None), P(None, None, 'sp'),
                  P(None, 'sp', None), P(), P(), kspec, kspec),
        out_specs=(P('dp', None), kspec, kspec), check_vma=False)
```

```python
import functools

import jax
import jax.numpy as jnp
from jax import lax
from jax.experimental import pallas as pl
from jax.experimental.pallas import tpu as pltpu
from jax.sharding import PartitionSpec as P

EPS = 1e-6
LOG2E = 1.4426950408889634
MESH = pl.DeviceIdType.MESH
VM = pl.BlockSpec(memory_space=pltpu.VMEM)
ANY = pl.BlockSpec(memory_space=pltpu.HBM)
SM = pl.BlockSpec(memory_space=pltpu.SMEM)
F32, BF16 = jnp.float32, jnp.bfloat16
CH = 256
NB = 512
LATE = 256
LM = 39


def _rms(h, g):
    r = lax.rsqrt(jnp.mean(h * h, axis=-1, keepdims=True) + EPS)
    return (h * r * g.astype(F32)).astype(BF16)


def _gelu(z):
    return 0.5 * z * (1.0 + jnp.tanh(0.7978845608028654 * (z + 0.044715 * z * z * z)))


def _dot(a, w):
    return jnp.dot(a, w, preferred_element_type=F32)


def _ids():
    dp, sp = lax.axis_index('dp'), lax.axis_index('sp')
    return dp, sp, lax.rem(sp, 2), dp * 4 + sp


def _hello(me):
    sem = pltpu.get_barrier_semaphore()
    for k in range(1, 8):
        d = lax.rem(me + k, 8)
        pl.semaphore_signal(sem, inc=1, device_id=(d // 4, lax.rem(d, 4)), device_id_type=MESH)


def _barrier():
    pl.semaphore_wait(pltpu.get_barrier_semaphore(), 7)


def _exchange(dp, sp, c, src, dst, ssem, rsem):
    x = sp // 2
    devs = [(1 - dp, (1 - x) * 2 + 1 - c), (1 - dp, (1 - x) * 2 + c), (1 - dp, x * 2 + 1 - c), (1 - dp, sp),
            (dp, (1 - x) * 2 + 1 - c), (dp, (1 - x) * 2 + c), (dp, sp + 1 - 2 * c)]
    out = []
    for k, dev in enumerate(devs):
        cp = pltpu.make_async_remote_copy(src(*dev), dst, ssem.at[k], rsem.at[k], device_id=dev, device_id_type=MESH)
        cp.start()
        out.append(cp)
    return out


def _qkv_copies(l, me, ws, wbuf, wsem, slot, s0):
    out = []
    for i in range(3):
        for kh in range(2):
            n = 2 * i + kh
            out.append(pltpu.make_async_copy(
                ws[i].at[l, pl.ds(kh * 2048, 2048), pl.ds(pl.multiple_of(me * NB, NB), NB)],
                wbuf.at[slot + n], wsem.at[s0 + n]))
    return out


def _half_cols(t, q, c):
    half = (1 - c) if t < 2 else c
    return half * 2048 + q * 1024 + (t % 2) * NB


def _mlp_copies(l, dp, c, wo, w1, w2, wbuf, wsem):
    out = []
    for t in range(4):
        for q in range(2):
            n = 2 * t + q
            col = pl.multiple_of(_half_cols(t, q, c), NB)
            out.append(pltpu.make_async_copy(
                wo.at[l, pl.ds(pl.multiple_of(dp * 512, 512), 512), pl.ds(col, NB)],
                wbuf.at[n // 4, pl.ds((n % 4) * 512, 512)], wsem.at[n]))
    for j in range(4):
        for kh in range(2):
            n = 2 * j + kh
            out.append(pltpu.make_async_copy(
                w1.at[l, pl.ds(kh * 2048, 2048), pl.ds(pl.multiple_of(dp * 2048 + j * NB, NB), NB)],
                wbuf.at[2 + n], wsem.at[8 + n]))
    for t in range(4):
        for q in range(2):
            n = 2 * t + q
            col = pl.multiple_of(_half_cols(t, q, c), NB)
            out.append(pltpu.make_async_copy(
                w2.at[l, pl.ds(pl.multiple_of(dp * 2048, 2048), 2048), pl.ds(col, NB)],
                wbuf.at[10 + n], wsem.at[16 + n]))
    return out


def _allreduce(block, dp, sp, c, buf, sems, h_ref):
    psend, pown, precv, chips, tot = buf
    s1, r1, s2, r2, s3, r3 = sems
    x = sp // 2
    partner = (dp, sp + 1 - 2 * c)
    chip = dp * 2 + x
    devs = ((1 - dp, (1 - x) * 2 + c), (1 - dp, sp), (dp, (1 - x) * 2 + c))

    def both(t):
        return jnp.concatenate([block(t, 0)[0:4], block(t, 1)[0:4]], axis=0)

    def copy(src, dst, ss, rs, dev):
        return pltpu.make_async_remote_copy(src, dst, ss, rs, device_id=dev, device_id_type=MESH)

    one = [copy(psend.at[t], precv.at[t], s1.at[t], r1.at[t], partner) for t in range(2)]
    two = [[copy(chips.at[chip, t], chips.at[chip, t], s2.at[t, k], r2.at[t, k], dev)
            for k, dev in enumerate(devs)] for t in range(2)]
    three = [copy(tot.at[c, t], tot.at[c, t], s3.at[t], r3.at[t], partner) for t in range(2)]
    for t in range(2):
        psend[t] = both(t)
        one[t].start()
    for t in range(2):
        pown[t] = both(2 + t)
        one[t].wait()
        chips[chip, t] = pown[t] + precv[t]
        for cp in two[t]:
            cp.start()
    for t in range(2):
        for cp in two[t]:
            cp.wait()
        tot[c, t] = ((chips[0, t] + chips[1, t]) + chips[2, t]) + chips[3, t]
        three[t].start()
    def add(half, t):
        for q in range(2):
            cols = pl.ds(pl.multiple_of(half * 2048 + q * 1024 + t * NB, NB), NB)
            h_ref[0:4, cols] += tot[half, t, q * 4:q * 4 + 4, :]

    for t in range(2):
        add(c, t)
    for t in range(2):
        three[t].wait()
        add(1 - c, t)


def _qkv_stage(chase, dp, sp, c, me, xn, wbuf, copies, slot, sendA, recvA, ssem, rsem, qkv_ref):
    res = []
    step = 2 if chase else 6
    for i in range(3):
        if 2 * i % step == 0:
            for cp in copies[2 * i:2 * i + step]:
                cp.wait()
        z = _dot(xn[:, :2048], wbuf[slot + 2 * i])
        z = z + _dot(xn[:, 2048:], wbuf[slot + 2 * i + 1])
        res.append(z)
    for g in range(2):
        rows = [r[2 * g:2 * g + 2] for r in res] + [jnp.zeros((2, NB), F32)]
        sendA[g] = jnp.concatenate(rows, axis=0).astype(BF16)
    cps = _exchange(dp, sp, c, lambda p, s: sendA.at[p], recvA.at[me], ssem, rsem)
    recvA[me] = sendA[dp]
    for cp in cps:
        cp.wait()
    qkv_ref[...] = recvA[...]


def _cache_copies(l, kc, vc, kb, vb, sem, late=0):
    nb, npos = kb.shape[:2]
    out = []
    for i, (src, dst) in enumerate(((kc, kb), (vc, vb))):
        for b in range(nb):
            n = npos - (late if i == 1 and b == nb - 1 else 0)
            out.append(pltpu.make_async_copy(src.at[l, b, pl.ds(0, n)], dst.at[b, pl.ds(0, n)], sem.at[i, b]))
    return out


def _first(x, wq, wk, wv, g1h, kc, vc, h_ref, qkv_ref, kb, vb,
           wbuf, xm, xo, g1, sendA, recvA, wsem, xs, xr, sa, ra, gs, ks):
    dp, sp, c, me = _ids()
    cq = _qkv_copies(0, me, (wq, wk, wv), wbuf, wsem, 0, 0)
    ck = _cache_copies(0, kc, vc, kb, vb, ks, LATE)
    _hello(me)
    cs = [pltpu.make_async_copy(x, xm, gs.at[0]), pltpu.make_async_copy(g1h, g1, gs.at[1])]
    for cp in cs + cq[:1]:
        cp.start()
    for cp in cs:
        cp.wait()
    for cp in cq[1:]:
        cp.start()
    _barrier()
    ex = pltpu.make_async_remote_copy(xm, xo, xs, xr, device_id=(1 - dp, sp), device_id_type=MESH)
    ex.start()
    ex.wait()
    mine, other = xm[...].astype(F32), xo[...].astype(F32)
    h_ref[0:2, :] = jnp.where(dp == 0, mine, other)
    h_ref[2:4, :] = jnp.where(dp == 0, other, mine)
    h_ref[4:8, :] = jnp.zeros((4, h_ref.shape[1]), F32)
    xn = _rms(h_ref[...], g1[0:1, :])
    for cp in ck:
        cp.start()
    _qkv_stage(True, dp, sp, c, me, xn, wbuf, cq, 0, sendA, recvA, sa, ra, qkv_ref)
    for cp in ck:
        cp.wait()


def _layer(l, last, *refs):
    if last:
        (op_ref, hin, wo, w1, w2, g2, y_ref, h_ref, *sc) = refs
    else:
        (op_ref, hin, wo, w1, w2, g2, wq, wk, wv, g1, kc, vc, h_ref, qkv_ref, kb, vb, *sc) = refs
    wbuf, recvB, att, u, psend, pown, precv, chips, tot = sc[:9]
    wsem, sb, rb, s1, r1, s2, r2, s3, r3 = sc[9:18]
    dp, sp, c, me = _ids()
    _hello(me)
    cm = _mlp_copies(l, dp, c, wo, w1, w2, wbuf, wsem)
    ck, cq = [], []
    if not last:
        sendA, recvA, sa, ra, ks = sc[18:]
        cq = _qkv_copies(l + 1, me, (wq, wk, wv), wbuf, wsem, 2, 24)
        ck = _cache_copies(l + 1, kc, vc, kb, vb, ks)
    for cp in cm[:16]:
        cp.start()
    h_ref[...] = hin[...]
    att[...] = jnp.zeros_like(att)
    recvB[me] = op_ref[2 * sp + dp]
    _barrier()
    cps = _exchange(dp, sp, c, lambda p, s: op_ref.at[2 * s + p], recvB.at[me], sb, rb)
    for cp in cps:
        cp.wait()
    for cp in cm[16:]:
        cp.start()
    for g in range(2):
        ms = [recvB[4 * g + i, 1][:, 0:1] for i in range(4)]
        m = functools.reduce(jnp.maximum, ms)
        o = jnp.zeros((8, 128), F32)
        den = jnp.zeros((8, 1), F32)
        for i in range(4):
            e = jnp.exp2(ms[i] - m)
            o = o + recvB[4 * g + i, 0] * e
            den = den + recvB[4 * g + i, 1][:, 64:65] * e
        a = o / den
        for b in range(2):
            for j in range(4):
                att[2 * g + b:2 * g + b + 1, j * 128:(j + 1) * 128] = a[4 * b + j:4 * b + j + 1]
    av = att[...].astype(BF16)
    for cp in cm[:8]:
        cp.wait()

    def wo_block(t, q):
        n = 2 * t + q
        return _dot(av, wbuf[n // 4, (n % 4) * 512:(n % 4) * 512 + 512, :])

    def bufs(i):
        return [psend.at[i], pown.at[i], precv.at[i], chips.at[i], tot.at[i]]

    def sems(i):
        return [s1.at[i], r1.at[i], s2.at[i], r2.at[i], s3.at[i], r3.at[i]]

    _allreduce(wo_block, dp, sp, c, bufs(0), sems(0), h_ref)
    for cp in ck:
        cp.start()
    xn = _rms(h_ref[...], g2[l:l + 1, :])
    for cp in cm[8:16]:
        cp.wait()
    for j in range(4):
        z = _dot(xn[:, :2048], wbuf[2 + 2 * j])
        z = z + _dot(xn[:, 2048:], wbuf[3 + 2 * j])
        u[:, j * NB:(j + 1) * NB] = _gelu(z).astype(BF16)
    uv = u[...]
    for cp in cm[16:]:
        cp.wait()
    for cp in cq:
        cp.start()

    def w2_block(t, q):
        n = 2 * t + q
        return _dot(uv, wbuf[10 + n])

    _allreduce(w2_block, dp, sp, c, bufs(1), sems(1), h_ref)
    if last:
        hv = h_ref[...]
        y_ref[...] = jnp.where(dp == 0, hv[0:2], hv[2:4]).astype(BF16)
    else:
        xn = _rms(h_ref[...], g1[l + 1:l + 2, :])
        _qkv_stage(False, dp, sp, c, me, xn, wbuf, cq, 2, sendA, recvA, sa, ra, qkv_ref)
        for cp in ck:
            cp.wait()


def _attn(l, *refs):
    if l == 0:
        lensh, qkv, kin, vin, vc, ko, vo, op_ref, kb, vb, *sc = refs
    else:
        lensh, qkv, kin, vin, _, _, ko, vo, op_ref, kb, vb, *sc = refs
    tr, q_ref, s_ref, m_ref, l_ref, o_ref, kos, vos, ls = sc
    nb, npos, nh, dh = kb.shape
    per = npos // CH
    n = nb * per
    base = lax.axis_index('sp') * npos
    nlast = npos - LATE
    if l == 0:
        late = pltpu.make_async_copy(vc.at[l, nb - 1, pl.ds(nlast, LATE)], vb.at[nb - 1, pl.ds(nlast, LATE)], ls)
        late.start()
    lv = lensh[...]
    lens = [jnp.max(lv[:, b:b + 1]) for b in range(nb)]

    def wr(dst, buf, sem, i):
        b, p = i // per, pl.multiple_of(lax.rem(i, per) * CH, CH)
        return pltpu.make_async_copy(buf.at[b, pl.ds(p, CH)], dst.at[l, b, pl.ds(p, CH)], sem.at[i])

    own = [lens[b] - 1 - base for b in range(nb)]
    first_v = [(vo, vb, vos, i, 4) for i in range(n if l > 0 else n - per)]
    early = [(ko, kb, kos, i, 2) for i in range(n)] + first_v
    last_v = [(vo, vb, vos, i, 4) for i in range(len(first_v), n)]

    def send(jobs, patched):
        for dst, buf, sem, i, _ in jobs:
            p0 = i % per * CH
            here = (own[i // per] >= p0) & (own[i // per] < p0 + CH)

            @pl.when(here if patched else jnp.logical_not(here))
            def _():
                wr(dst, buf, sem, i).start()

    send(early, False)
    for src in range(8):
        v = qkv[src].astype(F32)
        for j in range(4):
            tr[src * 4 + j] = v[:, j * dh:(j + 1) * dh]
    m_ref[...] = jnp.full(m_ref.shape, -jnp.inf, F32)
    l_ref[...] = jnp.zeros_like(l_ref)
    o_ref[...] = jnp.zeros_like(o_ref)

    def patch(buf, row, b):
        lp = own[b]

        @pl.when((lp >= 0) & (lp < npos))
        def _():
            buf[b, lp] = tr[:, row + b, :].astype(BF16)

    for b in range(nb):
        patch(kb, 2, b)
    for b in range(nb if l > 0 else nb - 1):
        patch(vb, 4, b)
    z = jnp.zeros((nh, dh), BF16)
    for b in range(nb):
        q = tr[:, b, :].astype(BF16)
        q_ref[b, 0:nh] = jnp.concatenate([q, z], axis=1)
        q_ref[b, nh:2 * nh] = jnp.concatenate([z, q], axis=1)
    hc = CH * nh // 2
    sl = lax.broadcasted_iota(jnp.int32, (8, dh), 0)
    ln = lax.broadcasted_iota(jnp.int32, (8, dh), 1)
    tile = lambda v: jnp.concatenate([v] * (hc // dh), axis=1)
    diag = tile(lax.rem(ln, nh) - sl)
    group = tile(lax.rem(ln, nh) // 8)
    col = lax.broadcasted_iota(jnp.int32, (8, hc), 1)
    ng = nh // 8
    sc = dh ** -0.5 * LOG2E

    def heads(v, op):
        k = nh
        while k < dh:
            v = op(v, pltpu.roll(v, k, 1))
            k *= 2
        return v

    def column(v, fill, op):
        return jnp.concatenate([op(jnp.where(ln == sl + 8 * r, v, fill), axis=1, keepdims=True)
                                for r in range(ng)], axis=0)

    def pair(buf, b, p0):
        return jnp.concatenate([buf[b, pl.ds(p0, CH // 2)].reshape(hc, dh),
                                buf[b, pl.ds(p0 + CH // 2, CH // 2)].reshape(hc, dh)], axis=1)

    send(early, True)

    def pick(b):
        return functools.reduce(lambda v, i: jnp.where(b == i, lens[i], v), range(1, nb), lens[0])

    def kstep(b, _):
        m = m_ref[b]
        for j in range(per):
            s = lax.dot_general(q_ref[b], pair(kb, b, j * CH), (((1,), (1,)), ((), ())),
                                preferred_element_type=F32)
            lim = (pick(b) - base - j * CH) * nh
            for half in range(2):
                v = functools.reduce(jnp.maximum, [
                    jnp.where(diag == 8 * r, s[half * nh + 8 * r:half * nh + 8 * r + 8], -jnp.inf) for r in range(ng)])
                v = jnp.where(col < lim - half * hc, v, -jnp.inf)
                s_ref[b * per + j, half] = v
                for k in range(0, hc, dh):
                    m = jnp.maximum(m, v[:, k:k + dh])
        m_ref[b] = heads(m, jnp.maximum)
        return 0

    def vstep(b, _):
        m = m_ref[b]
        m = tile(jnp.where(m == -jnp.inf, 0.0, m))
        lt, ot = l_ref[b], o_ref[b]
        for j in range(per):
            rows = []
            for half in range(2):
                p = jnp.exp2((s_ref[b * per + j, half] - m) * sc)
                for k in range(0, hc, dh):
                    lt = lt + p[:, k:k + dh]
                rows += [jnp.where(group == r, p, 0.0) for r in range(ng)]
            ot = ot + _dot(jnp.concatenate(rows, axis=0).astype(BF16), pair(vb, b, j * CH))
        l_ref[b] = heads(lt, jnp.add)
        o_ref[b] = ot
        return 0

    lax.fori_loop(0, nb, kstep, 0)
    if l == 0:
        late.wait()
        send(last_v, False)
        patch(vb, 4, nb - 1)
    mc = [column(m_ref[b], -jnp.inf, jnp.max) * sc for b in range(nb)]
    send(last_v, True)
    lax.fori_loop(0, nb, vstep, 0)
    lane = lax.broadcasted_iota(jnp.int32, (nh, dh), 1)
    for b in range(nb):
        ov = o_ref[b, 0:nh, 0:dh] + o_ref[b, nh:2 * nh, dh:2 * dh]
        ml = jnp.where(lane < 64, mc[b], column(l_ref[b], 0.0, jnp.sum))
        for r in range(8):
            op_ref[r, 0, b * 4:b * 4 + 4, :] = ov[4 * r:4 * r + 4]
            op_ref[r, 1, b * 4:b * 4 + 4, :] = ml[4 * r:4 * r + 4]
    for i in range(n):
        wr(ko, kb, kos, i).wait()
        wr(vo, vb, vos, i).wait()


def solution(mesh):
    kspec = P(None, 'dp', 'sp', None, None)
    DMA = pltpu.SemaphoreType.DMA

    def local(x, lens, wq, wk, wv, wo, w1, w2, g1, g2, kc, vc):
        nl, nb, npos, nh, dh = kc.shape
        d = x.shape[1]
        V = lambda *sh_dt: pltpu.VMEM(*sh_dt)
        hbm = lambda *xs: [pltpu.with_memory_space_constraint(a, pltpu.HBM) for a in xs]
        vm = lambda *xs: [pltpu.with_memory_space_constraint(a, pltpu.VMEM) for a in xs]
        h_sh, qkv_sh = V((8, d), F32), V((8, 8, NB), BF16)
        c_vm = V((nb, npos, nh, dh), BF16)
        qkv_sc = [V((2, 8, NB), BF16), V((8, 8, NB), BF16)]
        cparams = lambda i, mib: pltpu.CompilerParams(
            collective_id=i, has_side_effects=True, vmem_limit_bytes=mib * 2 ** 20)

        h, qkv, kb, vb = pl.pallas_call(
            _first, out_shape=(h_sh, qkv_sh, c_vm, c_vm),
            in_specs=[ANY] * 7, out_specs=(VM,) * 4,
            scratch_shapes=[V((6, 2048, NB), BF16), V((2, d), BF16), V((2, d), BF16), V((nl, d), BF16), *qkv_sc,
                            DMA((6,)), DMA, DMA, DMA((8,)), DMA((8,)), DMA((2,)), DMA((2, nb))],
            compiler_params=cparams(0, 16), name='first')(*hbm(x, wq, wk, wv, g1, kc, vc))

        def attn(l, qkv, kb, vb, ko, vo):
            n = nb * npos // CH
            c_sh = jax.ShapeDtypeStruct(kc.shape, kc.dtype)
            args = vm(lens.reshape(1, nb), qkv, kb, vb) + (hbm(vc) if l == 0 else hbm(ko, vo))
            al = {2: 3, 3: 4}
            if l > 0:
                al.update({4: 0, 5: 1})
            return pl.pallas_call(
                functools.partial(_attn, l),
                out_shape=(c_sh, c_sh, V((8, 2, 8, dh), F32), c_vm, c_vm),
                in_specs=[VM, VM, VM, VM] + ([ANY] if l == 0 else [ANY, ANY]),
                out_specs=(ANY, ANY, VM, VM, VM),
                scratch_shapes=[V((nh, 8, dh), F32), V((nb, 2 * nh, 2 * dh), BF16),
                                V((n, 2, 8, CH * nh // 2), F32), V((nb, 8, dh), F32),
                                V((nb, 8, dh), F32), V((nb, 2 * nh, 2 * dh), F32),
                                DMA((n,)), DMA((n,)), DMA],
                input_output_aliases=al,
                compiler_params=pltpu.CompilerParams(vmem_limit_bytes=14 * 2 ** 20), name='attn')(*args)[:3]

        def layer(l, op, h, last):
            sc = [V((18, 2048, NB), BF16), V((8, 2, 8, dh), F32),
                  V((8, 512), F32), V((8, 2048), BF16),
                  V((2, 2, 8, NB), F32), V((2, 2, 8, NB), F32), V((2, 2, 8, NB), F32),
                  V((2, 4, 2, 8, NB), F32), V((2, 2, 2, 8, NB), F32),
                  DMA((30,)), DMA((8,)), DMA((8,)),
                  DMA((2, 2)), DMA((2, 2)), DMA((2, 2, 3)), DMA((2, 2, 3)), DMA((2, 2)), DMA((2, 2))]
            args = vm(op, h) + hbm(wo, w1, w2) + vm(g2)
            specs = [VM, VM, ANY, ANY, ANY, VM]
            if last:
                sc = [V((8, d), F32)] + sc
                outs, out_specs, mib = jax.ShapeDtypeStruct((nb, d), BF16), VM, 39
            else:
                args += hbm(wq, wk, wv) + vm(g1) + hbm(kc, vc)
                specs += [ANY, ANY, ANY, VM, ANY, ANY]
                sc += [*qkv_sc, DMA((8,)), DMA((8,)), DMA((2, nb))]
                outs, out_specs, mib = (h_sh, qkv_sh, c_vm, c_vm), (VM,) * 4, LM
            return pl.pallas_call(
                functools.partial(_layer, l, last), out_shape=outs, in_specs=specs, out_specs=out_specs,
                scratch_shapes=sc, compiler_params=cparams(1 + l, mib), name='layer')(*args)

        ko = vo = None
        for l in range(nl):
            ko, vo, op = attn(l, qkv, kb, vb, ko, vo)
            if l < nl - 1:
                h, qkv, kb, vb = layer(l, op, h, False)
            else:
                y = layer(l, op, h, True)
        return y, ko, vo

    return jax.shard_map(
        local, mesh=mesh,
        in_specs=(P('dp', None), P('dp'), P(), P(), P(), P(None, 'sp', None), P(None, None, 'sp'),
                  P(None, 'sp', None), P(), P(), kspec, kspec),
        out_specs=(P('dp', None), kspec, kspec), check_vma=False)
```

```python
import functools

import jax
import jax.numpy as jnp
from jax import lax
from jax.experimental import pallas as pl
from jax.experimental.pallas import tpu as pltpu
from jax.sharding import PartitionSpec as P

EPS = 1e-6
LOG2E = 1.4426950408889634
MESH = pl.DeviceIdType.MESH
VM = pl.BlockSpec(memory_space=pltpu.VMEM)
ANY = pl.BlockSpec(memory_space=pltpu.HBM)
SM = pl.BlockSpec(memory_space=pltpu.SMEM)
F32, BF16 = jnp.float32, jnp.bfloat16
CH = 256
NB = 512
LATE = 256
LM = 39


def _rms(h, g):
    r = lax.rsqrt(jnp.mean(h * h, axis=-1, keepdims=True) + EPS)
    return (h * r * g.astype(F32)).astype(BF16)


def _gelu(z):
    return 0.5 * z * (1.0 + jnp.tanh(0.7978845608028654 * (z + 0.044715 * z * z * z)))


def _dot(a, w):
    return jnp.dot(a, w, preferred_element_type=F32)


def _ids():
    dp, sp = lax.axis_index('dp'), lax.axis_index('sp')
    return dp, sp, lax.rem(sp, 2), dp * 4 + sp


def _hello(me):
    sem = pltpu.get_barrier_semaphore()
    for k in range(1, 8):
        d = lax.rem(me + k, 8)
        pl.semaphore_signal(sem, inc=1, device_id=(d // 4, lax.rem(d, 4)), device_id_type=MESH)


def _barrier():
    pl.semaphore_wait(pltpu.get_barrier_semaphore(), 7)


def _exchange(dp, sp, c, src, dst, ssem, rsem):
    x = sp // 2
    devs = [(1 - dp, (1 - x) * 2 + 1 - c), (1 - dp, (1 - x) * 2 + c), (1 - dp, x * 2 + 1 - c), (1 - dp, sp),
            (dp, (1 - x) * 2 + 1 - c), (dp, (1 - x) * 2 + c), (dp, sp + 1 - 2 * c)]
    out = []
    for k, dev in enumerate(devs):
        cp = pltpu.make_async_remote_copy(src(*dev), dst, ssem.at[k], rsem.at[k], device_id=dev, device_id_type=MESH)
        cp.start()
        out.append(cp)
    return out


def _qkv_copies(l, me, ws, wbuf, wsem, slot, s0):
    out = []
    for i in range(3):
        for kh in range(2):
            n = 2 * i + kh
            out.append(pltpu.make_async_copy(
                ws[i].at[l, pl.ds(kh * 2048, 2048), pl.ds(pl.multiple_of(me * NB, NB), NB)],
                wbuf.at[slot + n], wsem.at[s0 + n]))
    return out


def _half_cols(t, q, c):
    half = (1 - c) if t < 2 else c
    return half * 2048 + q * 1024 + (t % 2) * NB


def _mlp_copies(l, dp, c, wo, w1, w2, wbuf, wsem):
    out = []
    for t in range(4):
        for q in range(2):
            n = 2 * t + q
            col = pl.multiple_of(_half_cols(t, q, c), NB)
            out.append(pltpu.make_async_copy(
                wo.at[l, pl.ds(pl.multiple_of(dp * 512, 512), 512), pl.ds(col, NB)],
                wbuf.at[n // 4, pl.ds((n % 4) * 512, 512)], wsem.at[n]))
    for j in range(4):
        for kh in range(2):
            n = 2 * j + kh
            out.append(pltpu.make_async_copy(
                w1.at[l, pl.ds(kh * 2048, 2048), pl.ds(pl.multiple_of(dp * 2048 + j * NB, NB), NB)],
                wbuf.at[2 + n], wsem.at[8 + n]))
    for t in range(4):
        for q in range(2):
            n = 2 * t + q
            col = pl.multiple_of(_half_cols(t, q, c), NB)
            out.append(pltpu.make_async_copy(
                w2.at[l, pl.ds(pl.multiple_of(dp * 2048, 2048), 2048), pl.ds(col, NB)],
                wbuf.at[10 + n], wsem.at[16 + n]))
    return out


def _allreduce(block, dp, sp, c, buf, sems, h_ref, more=()):
    psend, pown, precv, chips, tot = buf
    s1, r1, s2, r2, s3, r3 = sems
    x = sp // 2
    partner = (dp, sp + 1 - 2 * c)
    chip = dp * 2 + x
    devs = ((1 - dp, (1 - x) * 2 + c), (1 - dp, sp), (dp, (1 - x) * 2 + c))

    def both(t):
        return jnp.concatenate([block(t, 0)[0:4], block(t, 1)[0:4]], axis=0)

    def copy(src, dst, ss, rs, dev):
        return pltpu.make_async_remote_copy(src, dst, ss, rs, device_id=dev, device_id_type=MESH)

    one = [copy(psend.at[t], precv.at[t], s1.at[t], r1.at[t], partner) for t in range(2)]
    two = [[copy(chips.at[chip, t], chips.at[chip, t], s2.at[t, k], r2.at[t, k], dev)
            for k, dev in enumerate(devs)] for t in range(2)]
    three = [copy(tot.at[c, t], tot.at[c, t], s3.at[t], r3.at[t], partner) for t in range(2)]
    for t in range(2):
        psend[t] = both(t)
        one[t].start()
    for t in range(2):
        pown[t] = both(2 + t)
        one[t].wait()
        chips[chip, t] = pown[t] + precv[t]
        for cp in two[t]:
            cp.start()
    for cp in more:
        cp.start()
    for t in range(2):
        for cp in two[t]:
            cp.wait()
        tot[c, t] = ((chips[0, t] + chips[1, t]) + chips[2, t]) + chips[3, t]
        three[t].start()
    def add(half, t):
        for q in range(2):
            cols = pl.ds(pl.multiple_of(half * 2048 + q * 1024 + t * NB, NB), NB)
            h_ref[0:4, cols] += tot[half, t, q * 4:q * 4 + 4, :]

    for t in range(2):
        add(c, t)
    for t in range(2):
        three[t].wait()
        add(1 - c, t)


def _qkv_stage(chase, dp, sp, c, me, xn, wbuf, copies, slot, sendA, recvA, ssem, rsem, qkv_ref):
    res = []
    step = 2 if chase else 6
    for i in range(3):
        if 2 * i % step == 0:
            for cp in copies[2 * i:2 * i + step]:
                cp.wait()
        z = _dot(xn[:, :2048], wbuf[slot + 2 * i])
        z = z + _dot(xn[:, 2048:], wbuf[slot + 2 * i + 1])
        res.append(z)
    for g in range(2):
        rows = [r[2 * g:2 * g + 2] for r in res] + [jnp.zeros((2, NB), F32)]
        sendA[g] = jnp.concatenate(rows, axis=0).astype(BF16)
    cps = _exchange(dp, sp, c, lambda p, s: sendA.at[p], recvA.at[me], ssem, rsem)
    recvA[me] = sendA[dp]
    for cp in cps:
        cp.wait()
    qkv_ref[...] = recvA[...]


def _cache_copies(l, kc, vc, kb, vb, sem, late=0):
    nb, npos = kb.shape[:2]
    out = []
    for i, (src, dst) in enumerate(((kc, kb), (vc, vb))):
        for b in range(nb):
            n = npos - (late if i == 1 and b == nb - 1 else 0)
            out.append(pltpu.make_async_copy(src.at[l, b, pl.ds(0, n)], dst.at[b, pl.ds(0, n)], sem.at[i, b]))
    return out


def _first(x, wq, wk, wv, g1h, kc, vc, h_ref, qkv_ref, kb, vb,
           wbuf, xm, xo, g1, sendA, recvA, wsem, xs, xr, sa, ra, gs, ks):
    dp, sp, c, me = _ids()
    cq = _qkv_copies(0, me, (wq, wk, wv), wbuf, wsem, 0, 0)
    ck = _cache_copies(0, kc, vc, kb, vb, ks, LATE)
    _hello(me)
    cs = [pltpu.make_async_copy(x, xm, gs.at[0]), pltpu.make_async_copy(g1h, g1, gs.at[1])]
    for cp in cs + cq[:1]:
        cp.start()
    for cp in cs:
        cp.wait()
    for cp in cq[1:]:
        cp.start()
    _barrier()
    ex = pltpu.make_async_remote_copy(xm, xo, xs, xr, device_id=(1 - dp, sp), device_id_type=MESH)
    ex.start()
    ex.wait()
    mine, other = xm[...].astype(F32), xo[...].astype(F32)
    h_ref[0:2, :] = jnp.where(dp == 0, mine, other)
    h_ref[2:4, :] = jnp.where(dp == 0, other, mine)
    h_ref[4:8, :] = jnp.zeros((4, h_ref.shape[1]), F32)
    xn = _rms(h_ref[...], g1[0:1, :])
    for cp in ck:
        cp.start()
    _qkv_stage(True, dp, sp, c, me, xn, wbuf, cq, 0, sendA, recvA, sa, ra, qkv_ref)
    for cp in ck:
        cp.wait()


def _layer(l, last, *refs):
    if last:
        (op_ref, hin, wo, w1, w2, g2, y_ref, h_ref, *sc) = refs
    else:
        (op_ref, hin, wo, w1, w2, g2, wq, wk, wv, g1, kc, vc, h_ref, qkv_ref, kb, vb, *sc) = refs
    wbuf, recvB, att, u, psend, pown, precv, chips, tot = sc[:9]
    wsem, sb, rb, s1, r1, s2, r2, s3, r3 = sc[9:18]
    dp, sp, c, me = _ids()
    _hello(me)
    cm = _mlp_copies(l, dp, c, wo, w1, w2, wbuf, wsem)
    ck, cq = [], []
    if not last:
        sendA, recvA, sa, ra, ks = sc[18:]
        cq = _qkv_copies(l + 1, me, (wq, wk, wv), wbuf, wsem, 2, 24)
        ck = _cache_copies(l + 1, kc, vc, kb, vb, ks)
    for cp in cm[:16]:
        cp.start()
    h_ref[...] = hin[...]
    att[...] = jnp.zeros_like(att)
    recvB[me] = op_ref[2 * sp + dp]
    _barrier()
    cps = _exchange(dp, sp, c, lambda p, s: op_ref.at[2 * s + p], recvB.at[me], sb, rb)
    for cp in cps:
        cp.wait()
    for cp in cm[16:]:
        cp.start()
    for g in range(2):
        ms = [recvB[4 * g + i, 1][:, 0:1] for i in range(4)]
        m = functools.reduce(jnp.maximum, ms)
        o = jnp.zeros((8, 128), F32)
        den = jnp.zeros((8, 1), F32)
        for i in range(4):
            e = jnp.exp2(ms[i] - m)
            o = o + recvB[4 * g + i, 0] * e
            den = den + recvB[4 * g + i, 1][:, 64:65] * e
        a = o / den
        for b in range(2):
            for j in range(4):
                att[2 * g + b:2 * g + b + 1, j * 128:(j + 1) * 128] = a[4 * b + j:4 * b + j + 1]
    av = att[...].astype(BF16)
    for cp in cm[:8]:
        cp.wait()

    def wo_block(t, q):
        n = 2 * t + q
        return _dot(av, wbuf[n // 4, (n % 4) * 512:(n % 4) * 512 + 512, :])

    def bufs(i):
        return [psend.at[i], pown.at[i], precv.at[i], chips.at[i], tot.at[i]]

    def sems(i):
        return [s1.at[i], r1.at[i], s2.at[i], r2.at[i], s3.at[i], r3.at[i]]

    _allreduce(wo_block, dp, sp, c, bufs(0), sems(0), h_ref)
    xn = _rms(h_ref[...], g2[l:l + 1, :])
    for cp in cm[8:16]:
        cp.wait()
    for j in range(4):
        z = _dot(xn[:, :2048], wbuf[2 + 2 * j])
        z = z + _dot(xn[:, 2048:], wbuf[3 + 2 * j])
        u[:, j * NB:(j + 1) * NB] = _gelu(z).astype(BF16)
    uv = u[...]
    for cp in cm[16:]:
        cp.wait()
    for cp in cq + ck:
        cp.start()

    def w2_block(t, q):
        n = 2 * t + q
        return _dot(uv, wbuf[10 + n])

    _allreduce(w2_block, dp, sp, c, bufs(1), sems(1), h_ref)
    if last:
        hv = h_ref[...]
        y_ref[...] = jnp.where(dp == 0, hv[0:2], hv[2:4]).astype(BF16)
    else:
        xn = _rms(h_ref[...], g1[l + 1:l + 2, :])
        _qkv_stage(False, dp, sp, c, me, xn, wbuf, cq, 2, sendA, recvA, sa, ra, qkv_ref)
        for cp in ck:
            cp.wait()


def _attn(l, *refs):
    if l == 0:
        lensh, qkv, kin, vin, vc, ko, vo, op_ref, kb, vb, *sc = refs
    else:
        lensh, qkv, kin, vin, _, _, ko, vo, op_ref, kb, vb, *sc = refs
    tr, q_ref, s_ref, m_ref, l_ref, o_ref, kos, vos, ls = sc
    nb, npos, nh, dh = kb.shape
    per = npos // CH
    n = nb * per
    base = lax.axis_index('sp') * npos
    nlast = npos - LATE
    if l == 0:
        late = pltpu.make_async_copy(vc.at[l, nb - 1, pl.ds(nlast, LATE)], vb.at[nb - 1, pl.ds(nlast, LATE)], ls)
        late.start()
    lv = lensh[...]
    lens = [jnp.max(lv[:, b:b + 1]) for b in range(nb)]

    def wr(dst, buf, sem, i):
        b, p = i // per, pl.multiple_of(lax.rem(i, per) * CH, CH)
        return pltpu.make_async_copy(buf.at[b, pl.ds(p, CH)], dst.at[l, b, pl.ds(p, CH)], sem.at[i])

    own = [lens[b] - 1 - base for b in range(nb)]
    first_v = [(vo, vb, vos, i, 4) for i in range(n if l > 0 else n - per)]
    early = [(ko, kb, kos, i, 2) for i in range(n)] + first_v
    last_v = [(vo, vb, vos, i, 4) for i in range(len(first_v), n)]

    def send(jobs, patched):
        for dst, buf, sem, i, _ in jobs:
            p0 = i % per * CH
            here = (own[i // per] >= p0) & (own[i // per] < p0 + CH)

            @pl.when(here if patched else jnp.logical_not(here))
            def _():
                wr(dst, buf, sem, i).start()

    send(early, False)
    for src in range(8):
        v = qkv[src].astype(F32)
        for j in range(4):
            tr[src * 4 + j] = v[:, j * dh:(j + 1) * dh]
    m_ref[...] = jnp.full(m_ref.shape, -jnp.inf, F32)
    l_ref[...] = jnp.zeros_like(l_ref)
    o_ref[...] = jnp.zeros_like(o_ref)

    def patch(buf, row, b):
        lp = own[b]

        @pl.when((lp >= 0) & (lp < npos))
        def _():
            buf[b, lp] = tr[:, row + b, :].astype(BF16)

    for b in range(nb):
        patch(kb, 2, b)
    for b in range(nb if l > 0 else nb - 1):
        patch(vb, 4, b)
    z = jnp.zeros((nh, dh), BF16)
    for b in range(nb):
        q = tr[:, b, :].astype(BF16)
        q_ref[b, 0:nh] = jnp.concatenate([q, z], axis=1)
        q_ref[b, nh:2 * nh] = jnp.concatenate([z, q], axis=1)
    hc = CH * nh // 2
    sl = lax.broadcasted_iota(jnp.int32, (8, dh), 0)
    ln = lax.broadcasted_iota(jnp.int32, (8, dh), 1)
    tile = lambda v: jnp.concatenate([v] * (hc // dh), axis=1)
    diag = tile(lax.rem(ln, nh) - sl)
    group = tile(lax.rem(ln, nh) // 8)
    col = lax.broadcasted_iota(jnp.int32, (8, hc), 1)
    ng = nh // 8
    sc = dh ** -0.5 * LOG2E

    def heads(v, op):
        k = nh
        while k < dh:
            v = op(v, pltpu.roll(v, k, 1))
            k *= 2
        return v

    def column(v, fill, op):
        return jnp.concatenate([op(jnp.where(ln == sl + 8 * r, v, fill), axis=1, keepdims=True)
                                for r in range(ng)], axis=0)

    def pair(buf, b, p0):
        return jnp.concatenate([buf[b, pl.ds(p0, CH // 2)].reshape(hc, dh),
                                buf[b, pl.ds(p0 + CH // 2, CH // 2)].reshape(hc, dh)], axis=1)

    send(early, True)

    def pick(b):
        return functools.reduce(lambda v, i: jnp.where(b == i, lens[i], v), range(1, nb), lens[0])

    def kstep(b, _):
        m = m_ref[b]
        for j in range(per):
            s = lax.dot_general(q_ref[b], pair(kb, b, j * CH), (((1,), (1,)), ((), ())),
                                preferred_element_type=F32)
            lim = (pick(b) - base - j * CH) * nh
            for half in range(2):
                v = functools.reduce(jnp.maximum, [
                    jnp.where(diag == 8 * r, s[half * nh + 8 * r:half * nh + 8 * r + 8], -jnp.inf) for r in range(ng)])
                v = jnp.where(col < lim - half * hc, v, -jnp.inf)
                s_ref[b * per + j, half] = v
                for k in range(0, hc, dh):
                    m = jnp.maximum(m, v[:, k:k + dh])
        m_ref[b] = heads(m, jnp.maximum)
        return 0

    def vstep(b, _):
        m = m_ref[b]
        m = tile(jnp.where(m == -jnp.inf, 0.0, m))
        lt, ot = l_ref[b], o_ref[b]
        for j in range(per):
            rows = []
            for half in range(2):
                p = jnp.exp2((s_ref[b * per + j, half] - m) * sc)
                for k in range(0, hc, dh):
                    lt = lt + p[:, k:k + dh]
                rows += [jnp.where(group == r, p, 0.0) for r in range(ng)]
            ot = ot + _dot(jnp.concatenate(rows, axis=0).astype(BF16), pair(vb, b, j * CH))
        l_ref[b] = heads(lt, jnp.add)
        o_ref[b] = ot
        return 0

    lax.fori_loop(0, nb, kstep, 0)
    if l == 0:
        late.wait()
        send(last_v, False)
        patch(vb, 4, nb - 1)
    mc = [column(m_ref[b], -jnp.inf, jnp.max) * sc for b in range(nb)]
    send(last_v, True)
    lax.fori_loop(0, nb, vstep, 0)
    lane = lax.broadcasted_iota(jnp.int32, (nh, dh), 1)
    for b in range(nb):
        ov = o_ref[b, 0:nh, 0:dh] + o_ref[b, nh:2 * nh, dh:2 * dh]
        ml = jnp.where(lane < 64, mc[b], column(l_ref[b], 0.0, jnp.sum))
        for r in range(8):
            op_ref[r, 0, b * 4:b * 4 + 4, :] = ov[4 * r:4 * r + 4]
            op_ref[r, 1, b * 4:b * 4 + 4, :] = ml[4 * r:4 * r + 4]
    for i in range(n):
        wr(ko, kb, kos, i).wait()
        wr(vo, vb, vos, i).wait()


def solution(mesh):
    kspec = P(None, 'dp', 'sp', None, None)
    DMA = pltpu.SemaphoreType.DMA

    def local(x, lens, wq, wk, wv, wo, w1, w2, g1, g2, kc, vc):
        nl, nb, npos, nh, dh = kc.shape
        d = x.shape[1]
        V = lambda *sh_dt: pltpu.VMEM(*sh_dt)
        hbm = lambda *xs: [pltpu.with_memory_space_constraint(a, pltpu.HBM) for a in xs]
        vm = lambda *xs: [pltpu.with_memory_space_constraint(a, pltpu.VMEM) for a in xs]
        h_sh, qkv_sh = V((8, d), F32), V((8, 8, NB), BF16)
        c_vm = V((nb, npos, nh, dh), BF16)
        qkv_sc = [V((2, 8, NB), BF16), V((8, 8, NB), BF16)]
        cparams = lambda i, mib: pltpu.CompilerParams(
            collective_id=i, has_side_effects=True, vmem_limit_bytes=mib * 2 ** 20)

        h, qkv, kb, vb = pl.pallas_call(
            _first, out_shape=(h_sh, qkv_sh, c_vm, c_vm),
            in_specs=[ANY] * 7, out_specs=(VM,) * 4,
            scratch_shapes=[V((6, 2048, NB), BF16), V((2, d), BF16), V((2, d), BF16), V((nl, d), BF16), *qkv_sc,
                            DMA((6,)), DMA, DMA, DMA((8,)), DMA((8,)), DMA((2,)), DMA((2, nb))],
            compiler_params=cparams(0, 16), name='first')(*hbm(x, wq, wk, wv, g1, kc, vc))

        def attn(l, qkv, kb, vb, ko, vo):
            n = nb * npos // CH
            c_sh = jax.ShapeDtypeStruct(kc.shape, kc.dtype)
            args = vm(lens.reshape(1, nb), qkv, kb, vb) + (hbm(vc) if l == 0 else hbm(ko, vo))
            al = {2: 3, 3: 4}
            if l > 0:
                al.update({4: 0, 5: 1})
            return pl.pallas_call(
                functools.partial(_attn, l),
                out_shape=(c_sh, c_sh, V((8, 2, 8, dh), F32), c_vm, c_vm),
                in_specs=[VM, VM, VM, VM] + ([ANY] if l == 0 else [ANY, ANY]),
                out_specs=(ANY, ANY, VM, VM, VM),
                scratch_shapes=[V((nh, 8, dh), F32), V((nb, 2 * nh, 2 * dh), BF16),
                                V((n, 2, 8, CH * nh // 2), F32), V((nb, 8, dh), F32),
                                V((nb, 8, dh), F32), V((nb, 2 * nh, 2 * dh), F32),
                                DMA((n,)), DMA((n,)), DMA],
                input_output_aliases=al,
                compiler_params=pltpu.CompilerParams(vmem_limit_bytes=14 * 2 ** 20), name='attn')(*args)[:3]

        def layer(l, op, h, last):
            sc = [V((18, 2048, NB), BF16), V((8, 2, 8, dh), F32),
                  V((8, 512), F32), V((8, 2048), BF16),
                  V((2, 2, 8, NB), F32), V((2, 2, 8, NB), F32), V((2, 2, 8, NB), F32),
                  V((2, 4, 2, 8, NB), F32), V((2, 2, 2, 8, NB), F32),
                  DMA((30,)), DMA((8,)), DMA((8,)),
                  DMA((2, 2)), DMA((2, 2)), DMA((2, 2, 3)), DMA((2, 2, 3)), DMA((2, 2)), DMA((2, 2))]
            args = vm(op, h) + hbm(wo, w1, w2) + vm(g2)
            specs = [VM, VM, ANY, ANY, ANY, VM]
            if last:
                sc = [V((8, d), F32)] + sc
                outs, out_specs, mib = jax.ShapeDtypeStruct((nb, d), BF16), VM, 39
            else:
                args += hbm(wq, wk, wv) + vm(g1) + hbm(kc, vc)
                specs += [ANY, ANY, ANY, VM, ANY, ANY]
                sc += [*qkv_sc, DMA((8,)), DMA((8,)), DMA((2, nb))]
                outs, out_specs, mib = (h_sh, qkv_sh, c_vm, c_vm), (VM,) * 4, LM
            return pl.pallas_call(
                functools.partial(_layer, l, last), out_shape=outs, in_specs=specs, out_specs=out_specs,
                scratch_shapes=sc, compiler_params=cparams(1 + l, mib), name='layer')(*args)

        ko = vo = None
        for l in range(nl):
            ko, vo, op = attn(l, qkv, kb, vb, ko, vo)
            if l < nl - 1:
                h, qkv, kb, vb = layer(l, op, h, False)
            else:
                y = layer(l, op, h, True)
        return y, ko, vo

    return jax.shard_map(
        local, mesh=mesh,
        in_specs=(P('dp', None), P('dp'), P(), P(), P(), P(None, 'sp', None), P(None, None, 'sp'),
                  P(None, 'sp', None), P(), P(), kspec, kspec),
        out_specs=(P('dp', None), kspec, kspec), check_vma=False)
```

```python
import functools

import jax
import jax.numpy as jnp
from jax import lax
from jax.experimental import pallas as pl
from jax.experimental.pallas import tpu as pltpu
from jax.sharding import PartitionSpec as P

EPS = 1e-6
LOG2E = 1.4426950408889634
MESH = pl.DeviceIdType.MESH
VM = pl.BlockSpec(memory_space=pltpu.VMEM)
ANY = pl.BlockSpec(memory_space=pltpu.HBM)
SM = pl.BlockSpec(memory_space=pltpu.SMEM)
F32, BF16 = jnp.float32, jnp.bfloat16
CH = 256
NB = 512
LATE = 256
LM = 39


def _rms(h, g):
    r = lax.rsqrt(jnp.mean(h * h, axis=-1, keepdims=True) + EPS)
    return (h * r * g.astype(F32)).astype(BF16)


def _gelu(z):
    return 0.5 * z * (1.0 + jnp.tanh(0.7978845608028654 * (z + 0.044715 * z * z * z)))


def _dot(a, w):
    return jnp.dot(a, w, preferred_element_type=F32)


def _ids():
    dp, sp = lax.axis_index('dp'), lax.axis_index('sp')
    return dp, sp, lax.rem(sp, 2), dp * 4 + sp


def _hello(me):
    sem = pltpu.get_barrier_semaphore()
    for k in range(1, 8):
        d = lax.rem(me + k, 8)
        pl.semaphore_signal(sem, inc=1, device_id=(d // 4, lax.rem(d, 4)), device_id_type=MESH)


def _barrier():
    pl.semaphore_wait(pltpu.get_barrier_semaphore(), 7)


def _exchange(dp, sp, c, src, dst, ssem, rsem):
    x = sp // 2
    devs = [(1 - dp, (1 - x) * 2 + 1 - c), (1 - dp, (1 - x) * 2 + c), (1 - dp, x * 2 + 1 - c), (1 - dp, sp),
            (dp, (1 - x) * 2 + 1 - c), (dp, (1 - x) * 2 + c), (dp, sp + 1 - 2 * c)]
    out = []
    for k, dev in enumerate(devs):
        cp = pltpu.make_async_remote_copy(src(*dev), dst, ssem.at[k], rsem.at[k], device_id=dev, device_id_type=MESH)
        cp.start()
        out.append(cp)
    return out


def _qkv_copies(l, me, ws, wbuf, wsem, slot, s0):
    out = []
    for i in range(3):
        for kh in range(2):
            n = 2 * i + kh
            out.append(pltpu.make_async_copy(
                ws[i].at[l, pl.ds(kh * 2048, 2048), pl.ds(pl.multiple_of(me * NB, NB), NB)],
                wbuf.at[slot + n], wsem.at[s0 + n]))
    return out


def _half_cols(t, q, c):
    half = (1 - c) if t < 2 else c
    return half * 2048 + q * 1024 + (t % 2) * NB


def _mlp_copies(l, dp, c, wo, w1, w2, wbuf, wsem):
    out = []
    for t in range(4):
        for q in range(2):
            n = 2 * t + q
            col = pl.multiple_of(_half_cols(t, q, c), NB)
            out.append(pltpu.make_async_copy(
                wo.at[l, pl.ds(pl.multiple_of(dp * 512, 512), 512), pl.ds(col, NB)],
                wbuf.at[n // 4, pl.ds((n % 4) * 512, 512)], wsem.at[n]))
    for j in range(4):
        for kh in range(2):
            n = 2 * j + kh
            out.append(pltpu.make_async_copy(
                w1.at[l, pl.ds(kh * 2048, 2048), pl.ds(pl.multiple_of(dp * 2048 + j * NB, NB), NB)],
                wbuf.at[2 + n], wsem.at[8 + n]))
    for t in range(4):
        for q in range(2):
            n = 2 * t + q
            col = pl.multiple_of(_half_cols(t, q, c), NB)
            out.append(pltpu.make_async_copy(
                w2.at[l, pl.ds(pl.multiple_of(dp * 2048, 2048), 2048), pl.ds(col, NB)],
                wbuf.at[10 + n], wsem.at[16 + n]))
    return out


def _allreduce(block, dp, sp, c, buf, sems, h_ref, more=()):
    psend, pown, precv, chips, tot = buf
    s1, r1, s2, r2, s3, r3 = sems
    x = sp // 2
    partner = (dp, sp + 1 - 2 * c)
    chip = dp * 2 + x
    devs = ((1 - dp, (1 - x) * 2 + c), (1 - dp, sp), (dp, (1 - x) * 2 + c))

    def both(t):
        return jnp.concatenate([block(t, 0)[0:4], block(t, 1)[0:4]], axis=0)

    def copy(src, dst, ss, rs, dev):
        return pltpu.make_async_remote_copy(src, dst, ss, rs, device_id=dev, device_id_type=MESH)

    one = [copy(psend.at[t], precv.at[t], s1.at[t], r1.at[t], partner) for t in range(2)]
    two = [[copy(chips.at[chip, t], chips.at[chip, t], s2.at[t, k], r2.at[t, k], dev)
            for k, dev in enumerate(devs)] for t in range(2)]
    three = [copy(tot.at[c, t], tot.at[c, t], s3.at[t], r3.at[t], partner) for t in range(2)]
    for t in range(2):
        psend[t] = both(t)
        one[t].start()
    for t in range(2):
        mine = both(2 + t)
        one[t].wait()
        chips[chip, t] = mine + precv[t]
        for cp in two[t]:
            cp.start()
    for cp in more:
        cp.start()
    for t in range(2):
        for cp in two[t]:
            cp.wait()
        tot[c, t] = ((chips[0, t] + chips[1, t]) + chips[2, t]) + chips[3, t]
        three[t].start()
    def add(half, t):
        for q in range(2):
            cols = pl.ds(pl.multiple_of(half * 2048 + q * 1024 + t * NB, NB), NB)
            h_ref[0:4, cols] += tot[half, t, q * 4:q * 4 + 4, :]

    for t in range(2):
        add(c, t)
    for t in range(2):
        three[t].wait()
        add(1 - c, t)


def _qkv_stage(chase, dp, sp, c, me, xn, wbuf, copies, slot, sendA, recvA, ssem, rsem, qkv_ref):
    res = []
    step = 2 if chase else 6
    for i in range(3):
        if 2 * i % step == 0:
            for cp in copies[2 * i:2 * i + step]:
                cp.wait()
        z = _dot(xn[:, :2048], wbuf[slot + 2 * i])
        z = z + _dot(xn[:, 2048:], wbuf[slot + 2 * i + 1])
        res.append(z)
    for g in range(2):
        rows = [r[2 * g:2 * g + 2] for r in res] + [jnp.zeros((2, NB), F32)]
        sendA[g] = jnp.concatenate(rows, axis=0).astype(BF16)
    cps = _exchange(dp, sp, c, lambda p, s: sendA.at[p], recvA.at[me], ssem, rsem)
    recvA[me] = sendA[dp]
    for cp in cps:
        cp.wait()
    qkv_ref[...] = recvA[...]


def _cache_copies(l, kc, vc, kb, vb, sem, late=0):
    nb, npos = kb.shape[:2]
    out = []
    for i, (src, dst) in enumerate(((kc, kb), (vc, vb))):
        for b in range(nb):
            n = npos - (late if i == 1 and b == nb - 1 else 0)
            out.append(pltpu.make_async_copy(src.at[l, b, pl.ds(0, n)], dst.at[b, pl.ds(0, n)], sem.at[i, b]))
    return out


def _first(x, wq, wk, wv, g1h, kc, vc, h_ref, qkv_ref, kb, vb,
           wbuf, xm, xo, g1, sendA, recvA, wsem, xs, xr, sa, ra, gs, ks):
    dp, sp, c, me = _ids()
    cq = _qkv_copies(0, me, (wq, wk, wv), wbuf, wsem, 0, 0)
    ck = _cache_copies(0, kc, vc, kb, vb, ks, LATE)
    _hello(me)
    cs = [pltpu.make_async_copy(x, xm, gs.at[0]), pltpu.make_async_copy(g1h, g1, gs.at[1])]
    for cp in cs + cq[:1]:
        cp.start()
    for cp in cs:
        cp.wait()
    for cp in cq[1:]:
        cp.start()
    _barrier()
    ex = pltpu.make_async_remote_copy(xm, xo, xs, xr, device_id=(1 - dp, sp), device_id_type=MESH)
    ex.start()
    ex.wait()
    mine, other = xm[...].astype(F32), xo[...].astype(F32)
    h_ref[0:2, :] = jnp.where(dp == 0, mine, other)
    h_ref[2:4, :] = jnp.where(dp == 0, other, mine)
    h_ref[4:8, :] = jnp.zeros((4, h_ref.shape[1]), F32)
    xn = _rms(h_ref[...], g1[0:1, :])
    for cp in ck:
        cp.start()
    _qkv_stage(True, dp, sp, c, me, xn, wbuf, cq, 0, sendA, recvA, sa, ra, qkv_ref)
    for cp in ck:
        cp.wait()


def _layer(l, last, *refs):
    if last:
        (op_ref, hin, wo, w1, w2, g2, y_ref, h_ref, *sc) = refs
    else:
        (op_ref, hin, wo, w1, w2, g2, wq, wk, wv, g1, kc, vc, h_ref, qkv_ref, kb, vb, *sc) = refs
    wbuf, recvB, att, u, psend, pown, precv, chips, tot = sc[:9]
    wsem, sb, rb, s1, r1, s2, r2, s3, r3 = sc[9:18]
    dp, sp, c, me = _ids()
    _hello(me)
    cm = _mlp_copies(l, dp, c, wo, w1, w2, wbuf, wsem)
    ck, cq = [], []
    if not last:
        sendA, recvA, sa, ra, ks = sc[18:]
        cq = _qkv_copies(l + 1, me, (wq, wk, wv), wbuf, wsem, 2, 24)
        ck = _cache_copies(l + 1, kc, vc, kb, vb, ks)
    for cp in cm[:16]:
        cp.start()
    h_ref[...] = hin[...]
    att[...] = jnp.zeros_like(att)
    recvB[me] = op_ref[2 * sp + dp]
    _barrier()
    cps = _exchange(dp, sp, c, lambda p, s: op_ref.at[2 * s + p], recvB.at[me], sb, rb)
    for cp in cps:
        cp.wait()
    for cp in cm[16:]:
        cp.start()
    for g in range(2):
        ms = [recvB[4 * g + i, 1][:, 0:1] for i in range(4)]
        m = functools.reduce(jnp.maximum, ms)
        o = jnp.zeros((8, 128), F32)
        den = jnp.zeros((8, 1), F32)
        for i in range(4):
            e = jnp.exp2(ms[i] - m)
            o = o + recvB[4 * g + i, 0] * e
            den = den + recvB[4 * g + i, 1][:, 64:65] * e
        a = o / den
        for b in range(2):
            for j in range(4):
                att[2 * g + b:2 * g + b + 1, j * 128:(j + 1) * 128] = a[4 * b + j:4 * b + j + 1]
    av = att[...].astype(BF16)
    for cp in cm[:8]:
        cp.wait()

    def wo_block(t, q):
        n = 2 * t + q
        return _dot(av, wbuf[n // 4, (n % 4) * 512:(n % 4) * 512 + 512, :])

    def bufs(i):
        return [psend.at[i], pown.at[i], precv.at[i], chips.at[i], tot.at[i]]

    def sems(i):
        return [s1.at[i], r1.at[i], s2.at[i], r2.at[i], s3.at[i], r3.at[i]]

    _allreduce(wo_block, dp, sp, c, bufs(0), sems(0), h_ref)
    xn = _rms(h_ref[...], g2[l:l + 1, :])
    for cp in cm[8:16]:
        cp.wait()
    for j in range(4):
        z = _dot(xn[:, :2048], wbuf[2 + 2 * j])
        z = z + _dot(xn[:, 2048:], wbuf[3 + 2 * j])
        u[:, j * NB:(j + 1) * NB] = _gelu(z).astype(BF16)
    uv = u[...]
    for cp in cm[16:]:
        cp.wait()
    for cp in cq + ck:
        cp.start()

    def w2_block(t, q):
        n = 2 * t + q
        return _dot(uv, wbuf[10 + n])

    _allreduce(w2_block, dp, sp, c, bufs(1), sems(1), h_ref)
    if last:
        hv = h_ref[...]
        y_ref[...] = jnp.where(dp == 0, hv[0:2], hv[2:4]).astype(BF16)
    else:
        xn = _rms(h_ref[...], g1[l + 1:l + 2, :])
        _qkv_stage(False, dp, sp, c, me, xn, wbuf, cq, 2, sendA, recvA, sa, ra, qkv_ref)
        for cp in ck:
            cp.wait()


def _attn(l, *refs):
    if l == 0:
        lensh, qkv, kin, vin, vc, ko, vo, op_ref, kb, vb, *sc = refs
    else:
        lensh, qkv, kin, vin, _, _, ko, vo, op_ref, kb, vb, *sc = refs
    tr, q_ref, s_ref, m_ref, l_ref, o_ref, kos, vos, ls = sc
    nb, npos, nh, dh = kb.shape
    per = npos // CH
    n = nb * per
    base = lax.axis_index('sp') * npos
    nlast = npos - LATE
    if l == 0:
        late = pltpu.make_async_copy(vc.at[l, nb - 1, pl.ds(nlast, LATE)], vb.at[nb - 1, pl.ds(nlast, LATE)], ls)
        late.start()
    lv = lensh[...]
    lens = [jnp.max(lv[:, b:b + 1]) for b in range(nb)]

    def wr(dst, buf, sem, i):
        b, p = i // per, pl.multiple_of(lax.rem(i, per) * CH, CH)
        return pltpu.make_async_copy(buf.at[b, pl.ds(p, CH)], dst.at[l, b, pl.ds(p, CH)], sem.at[i])

    own = [lens[b] - 1 - base for b in range(nb)]
    first_v = [(vo, vb, vos, i, 4) for i in range(n if l > 0 else n - per)]
    early = [(ko, kb, kos, i, 2) for i in range(n)] + first_v
    last_v = [(vo, vb, vos, i, 4) for i in range(len(first_v), n)]

    def send(jobs, patched):
        for dst, buf, sem, i, _ in jobs:
            p0 = i % per * CH
            here = (own[i // per] >= p0) & (own[i // per] < p0 + CH)

            @pl.when(here if patched else jnp.logical_not(here))
            def _():
                wr(dst, buf, sem, i).start()

    send(early, False)
    for src in range(8):
        v = qkv[src].astype(F32)
        for j in range(4):
            tr[src * 4 + j] = v[:, j * dh:(j + 1) * dh]
    m_ref[...] = jnp.full(m_ref.shape, -jnp.inf, F32)
    l_ref[...] = jnp.zeros_like(l_ref)
    o_ref[...] = jnp.zeros_like(o_ref)

    def patch(buf, row, b):
        lp = own[b]

        @pl.when((lp >= 0) & (lp < npos))
        def _():
            buf[b, lp] = tr[:, row + b, :].astype(BF16)

    for b in range(nb):
        patch(kb, 2, b)
    for b in range(nb if l > 0 else nb - 1):
        patch(vb, 4, b)
    z = jnp.zeros((nh, dh), BF16)
    for b in range(nb):
        q = tr[:, b, :].astype(BF16)
        q_ref[b, 0:nh] = jnp.concatenate([q, z], axis=1)
        q_ref[b, nh:2 * nh] = jnp.concatenate([z, q], axis=1)
    hc = CH * nh // 2
    sl = lax.broadcasted_iota(jnp.int32, (8, dh), 0)
    ln = lax.broadcasted_iota(jnp.int32, (8, dh), 1)
    tile = lambda v: jnp.concatenate([v] * (hc // dh), axis=1)
    diag = tile(lax.rem(ln, nh) - sl)
    group = tile(lax.rem(ln, nh) // 8)
    col = lax.broadcasted_iota(jnp.int32, (8, hc), 1)
    ng = nh // 8
    sc = dh ** -0.5 * LOG2E

    def heads(v, op):
        k = nh
        while k < dh:
            v = op(v, pltpu.roll(v, k, 1))
            k *= 2
        return v

    def column(v, fill, op):
        return jnp.concatenate([op(jnp.where(ln == sl + 8 * r, v, fill), axis=1, keepdims=True)
                                for r in range(ng)], axis=0)

    def pair(buf, b, p0):
        return jnp.concatenate([buf[b, pl.ds(p0, CH // 2)].reshape(hc, dh),
                                buf[b, pl.ds(p0 + CH // 2, CH // 2)].reshape(hc, dh)], axis=1)

    send(early, True)

    def pick(b):
        return functools.reduce(lambda v, i: jnp.where(b == i, lens[i], v), range(1, nb), lens[0])

    def kstep(b, _):
        m = m_ref[b]
        for j in range(per):
            s = lax.dot_general(q_ref[b], pair(kb, b, j * CH), (((1,), (1,)), ((), ())),
                                preferred_element_type=F32)
            lim = (pick(b) - base - j * CH) * nh
            for half in range(2):
                v = functools.reduce(jnp.maximum, [
                    jnp.where(diag == 8 * r, s[half * nh + 8 * r:half * nh + 8 * r + 8], -jnp.inf) for r in range(ng)])
                v = jnp.where(col < lim - half * hc, v, -jnp.inf)
                s_ref[b * per + j, half] = v
                for k in range(0, hc, dh):
                    m = jnp.maximum(m, v[:, k:k + dh])
        m_ref[b] = heads(m, jnp.maximum)
        return 0

    def vstep(b, _):
        m = m_ref[b]
        m = tile(jnp.where(m == -jnp.inf, 0.0, m))
        lt, ot = l_ref[b], o_ref[b]
        for j in range(per):
            rows = []
            for half in range(2):
                p = jnp.exp2((s_ref[b * per + j, half] - m) * sc)
                for k in range(0, hc, dh):
                    lt = lt + p[:, k:k + dh]
                rows += [jnp.where(group == r, p, 0.0) for r in range(ng)]
            ot = ot + _dot(jnp.concatenate(rows, axis=0).astype(BF16), pair(vb, b, j * CH))
        l_ref[b] = heads(lt, jnp.add)
        o_ref[b] = ot
        return 0

    lax.fori_loop(0, nb, kstep, 0)
    if l == 0:
        late.wait()
        send(last_v, False)
        patch(vb, 4, nb - 1)
    mc = [column(m_ref[b], -jnp.inf, jnp.max) * sc for b in range(nb)]
    send(last_v, True)
    lax.fori_loop(0, nb, vstep, 0)
    lane = lax.broadcasted_iota(jnp.int32, (nh, dh), 1)
    for b in range(nb):
        ov = o_ref[b, 0:nh, 0:dh] + o_ref[b, nh:2 * nh, dh:2 * dh]
        ml = jnp.where(lane < 64, mc[b], column(l_ref[b], 0.0, jnp.sum))
        for r in range(8):
            op_ref[r, 0, b * 4:b * 4 + 4, :] = ov[4 * r:4 * r + 4]
            op_ref[r, 1, b * 4:b * 4 + 4, :] = ml[4 * r:4 * r + 4]
    for i in range(n):
        wr(ko, kb, kos, i).wait()
        wr(vo, vb, vos, i).wait()


def solution(mesh):
    kspec = P(None, 'dp', 'sp', None, None)
    DMA = pltpu.SemaphoreType.DMA

    def local(x, lens, wq, wk, wv, wo, w1, w2, g1, g2, kc, vc):
        nl, nb, npos, nh, dh = kc.shape
        d = x.shape[1]
        V = lambda *sh_dt: pltpu.VMEM(*sh_dt)
        hbm = lambda *xs: [pltpu.with_memory_space_constraint(a, pltpu.HBM) for a in xs]
        vm = lambda *xs: [pltpu.with_memory_space_constraint(a, pltpu.VMEM) for a in xs]
        h_sh, qkv_sh = V((8, d), F32), V((8, 8, NB), BF16)
        c_vm = V((nb, npos, nh, dh), BF16)
        qkv_sc = [V((2, 8, NB), BF16), V((8, 8, NB), BF16)]
        cparams = lambda i, mib: pltpu.CompilerParams(
            collective_id=i, has_side_effects=True, vmem_limit_bytes=mib * 2 ** 20)

        h, qkv, kb, vb = pl.pallas_call(
            _first, out_shape=(h_sh, qkv_sh, c_vm, c_vm),
            in_specs=[ANY] * 7, out_specs=(VM,) * 4,
            scratch_shapes=[V((6, 2048, NB), BF16), V((2, d), BF16), V((2, d), BF16), V((nl, d), BF16), *qkv_sc,
                            DMA((6,)), DMA, DMA, DMA((8,)), DMA((8,)), DMA((2,)), DMA((2, nb))],
            compiler_params=cparams(0, 16), name='first')(*hbm(x, wq, wk, wv, g1, kc, vc))

        def attn(l, qkv, kb, vb, ko, vo):
            n = nb * npos // CH
            c_sh = jax.ShapeDtypeStruct(kc.shape, kc.dtype)
            args = vm(lens.reshape(1, nb), qkv, kb, vb) + (hbm(vc) if l == 0 else hbm(ko, vo))
            al = {2: 3, 3: 4}
            if l > 0:
                al.update({4: 0, 5: 1})
            return pl.pallas_call(
                functools.partial(_attn, l),
                out_shape=(c_sh, c_sh, V((8, 2, 8, dh), F32), c_vm, c_vm),
                in_specs=[VM, VM, VM, VM] + ([ANY] if l == 0 else [ANY, ANY]),
                out_specs=(ANY, ANY, VM, VM, VM),
                scratch_shapes=[V((nh, 8, dh), F32), V((nb, 2 * nh, 2 * dh), BF16),
                                V((n, 2, 8, CH * nh // 2), F32), V((nb, 8, dh), F32),
                                V((nb, 8, dh), F32), V((nb, 2 * nh, 2 * dh), F32),
                                DMA((n,)), DMA((n,)), DMA],
                input_output_aliases=al,
                compiler_params=pltpu.CompilerParams(vmem_limit_bytes=14 * 2 ** 20), name='attn')(*args)[:3]

        def layer(l, op, h, last):
            sc = [V((18, 2048, NB), BF16), V((8, 2, 8, dh), F32),
                  V((8, 512), F32), V((8, 2048), BF16),
                  V((2, 2, 8, NB), F32), V((2, 2, 8, NB), F32), V((2, 2, 8, NB), F32),
                  V((2, 4, 2, 8, NB), F32), V((2, 2, 2, 8, NB), F32),
                  DMA((30,)), DMA((8,)), DMA((8,)),
                  DMA((2, 2)), DMA((2, 2)), DMA((2, 2, 3)), DMA((2, 2, 3)), DMA((2, 2)), DMA((2, 2))]
            args = vm(op, h) + hbm(wo, w1, w2) + vm(g2)
            specs = [VM, VM, ANY, ANY, ANY, VM]
            if last:
                sc = [V((8, d), F32)] + sc
                outs, out_specs, mib = jax.ShapeDtypeStruct((nb, d), BF16), VM, 39
            else:
                args += hbm(wq, wk, wv) + vm(g1) + hbm(kc, vc)
                specs += [ANY, ANY, ANY, VM, ANY, ANY]
                sc += [*qkv_sc, DMA((8,)), DMA((8,)), DMA((2, nb))]
                outs, out_specs, mib = (h_sh, qkv_sh, c_vm, c_vm), (VM,) * 4, LM
            return pl.pallas_call(
                functools.partial(_layer, l, last), out_shape=outs, in_specs=specs, out_specs=out_specs,
                scratch_shapes=sc, compiler_params=cparams(1 + l, mib), name='layer')(*args)

        ko = vo = None
        for l in range(nl):
            ko, vo, op = attn(l, qkv, kb, vb, ko, vo)
            if l < nl - 1:
                h, qkv, kb, vb = layer(l, op, h, False)
            else:
                y = layer(l, op, h, True)
        return y, ko, vo

    return jax.shard_map(
        local, mesh=mesh,
        in_specs=(P('dp', None), P('dp'), P(), P(), P(), P(None, 'sp', None), P(None, None, 'sp'),
                  P(None, 'sp', None), P(), P(), kspec, kspec),
        out_specs=(P('dp', None), kspec, kspec), check_vma=False)
```
